256 devices in a mesh: seq: 32 (over z, x), tensor: 8 (over y, core).
Axes of the slice: x: 4, y: 4, z: 8, core: 2. Of those that a mesh axis runs over, the one named last changes fastest.
Arguments:
- hidden_in: bfloat16 [16, 5120], replicated, may hold values from -6 to 6
- united_down: bfloat16 [5120, 2112], P(None, 'tensor'), may hold values from -0.078125 to 0.078125
- q_gain: float32 [1536], replicated, may hold values from 0.1 to 1.9
- kv_gain: float32 [512], replicated, may hold values from 0.1 to 1.9
- q_up: bfloat16 [1536, 24576], P('seq', 'tensor'), may hold values from -0.15625 to 0.15625
- key_up: bfloat16 [512, 16384], P(None, 'tensor'), may hold values from -0.25 to 0.25
- value_up: bfloat16 [512, 16384], P(None, 'tensor'), may hold values from -0.0625 to 0.0625
- latent_block_store: bfloat16 [2048, 128, 512], P(('seq', 'tensor')), may hold values from -24 to 24
- rope_pool: bfloat16 [2048, 64, 128], P(('seq', 'tensor')), may hold values from -124 to 124
- lengths: int32 [16], replicated, may hold values from 8192 to 16384, as said below
- block_table: int32 [16, 128], P(None, 'seq'), may hold values from 0 to 2047, as said below
Outputs:
- attn_out: bfloat16 [16, 16384], P(None, 'tensor')
- new_entry: bfloat16 [16, 576], replicated
The draws below stay inside these ranges and needn't reach their ends.
Inputs may be any that keep to these rules, and one draw needn't show every extreme that they name: `lengths`: every sequence holds 8192 to 16384 cached positions; one sequence holds exactly 16384 and another exactly 8192. block_table[b, j] is the pool slot of positions j * 128 to (j + 1) * 128 - 1 of sequence b. The columns j with j // 4 = s name exactly the 64 slots s * 16 * 4 to (s + 1) * 16 * 4 - 1, each once, in any order; blocks past a sequence's length also name such slots.
All inputs are finite; a program needn't handle non-finite values.
Results may differ from the reference program's by a relative error of at most 0.015.
The reference program's roundings to bfloat16 on the way count: a program that leaves them out, or rounds other values in their place, can miss the bound.
Values may be sent and summed in bfloat16 or wider, within the bound.
No kernel may reach another device: no remote copies, remote signals or barrier semaphores. Data moves between devices by JAX's collectives and lax.ppermute only.
A program may use at most 128 MiB of HBM per device.

```python
import jax
import jax.numpy as jnp
from jax import lax

D = 5120
QR = 1536
LATENT_RANK = 512
NOPE = 128
ROTARY_WIDTH = 64
VD = 128
H = 128
B = 16
BLOCK_POSITIONS = 128
SPAN_BLK = 4
QH = 192
UNITED = 2112
NBLK = 128
LMAX = 16384
POOL_BLOCKS = 2048


def draw_rope_pool(key, part):
    tensor_dims = (POOL_BLOCKS, ROTARY_WIDTH, BLOCK_POSITIONS)
    base_key, active_key, sign_key = jax.random.split(key, 3)
    drawn = jnp.clip(jax.random.normal(base_key, tensor_dims, jnp.float32), -4.0, 4.0)
    return drawn.astype(jnp.bfloat16)


def draw_lengths(key, part):
    first_key, second_key, third_key = jax.random.split(key, 3)
    drawn = jax.random.randint(first_key, (B,), LMAX // 2, LMAX + 1, dtype=jnp.int32)
    longest = jax.random.randint(second_key, (), 0, B, dtype=jnp.int32)
    shortest = (longest + jax.random.randint(third_key, (), 1, B, dtype=jnp.int32)) % B
    seq_ids = jnp.arange(B, dtype=jnp.int32)
    drawn = jnp.where(seq_ids == shortest, LMAX // 2, drawn)
    return jnp.where(seq_ids == longest, LMAX, drawn).astype(jnp.int32)


def draw_block_table(key, part):
    group_size = B * SPAN_BLK
    group_count = NBLK // SPAN_BLK
    group_keys = jax.random.split(key, group_count)
    orders = jax.vmap(lambda one_key: jax.random.permutation(one_key, group_size))(group_keys)
    offsets = jnp.arange(group_count, dtype=jnp.int32)[:, None] * group_size
    placed = (orders.astype(jnp.int32) + offsets).reshape(group_count, B, SPAN_BLK)
    return jnp.transpose(placed, (1, 0, 2)).reshape(B, NBLK).astype(jnp.int32)


def steps_of(rng, dims, pieces, least, high):
    level = 1.0
    for axis_at, blocks in pieces:
        steps = jax.random.uniform(jax.random.fold_in(jax.random.fold_in(rng, 6), axis_at), (blocks,), jnp.float32, least / len(pieces), high / len(pieces))
        level = level * jnp.repeat(jnp.exp(steps), dims[axis_at] // blocks).reshape((-1,) + (1,) * (len(dims) - 1 - axis_at))
    return level


def scatter_about(own_key, dims, spread, limit, cuts=(), kind=jnp.bfloat16):
    array = spread * jax.random.normal(own_key, dims, jnp.float32)
    if cuts:
        array = array * steps_of(own_key, dims, cuts, -0.22, 0.18)
    return jnp.clip(array, -limit, limit).astype(kind)


def setup_inputs(seed: int = 0) -> dict:
    seeds = jax.random.split(jax.random.key(seed), 12)
    hidden_in = scatter_about(seeds[0], (B, D), 1.0, 6.0)
    united_down = scatter_about(seeds[1], (D, UNITED), D ** -0.5, 0.078125, ((1, 8),))
    q_gain = jnp.clip(1.0 + 0.18 * jax.random.normal(seeds[2], (QR,), jnp.float32), 0.1, 1.9)
    kv_gain = jnp.clip(1.0 + 0.18 * jax.random.normal(seeds[3], (LATENT_RANK,), jnp.float32), 0.1, 1.9)
    q_up = scatter_about(seeds[4], (QR, H * QH), QR ** -0.5, 0.15625, ((0, 32), (1, 8)))
    key_up = scatter_about(seeds[5], (LATENT_RANK, H * NOPE), LATENT_RANK ** -0.5, 0.25, ((1, 8),))
    value_up = scatter_about(seeds[6], (LATENT_RANK, H * VD), (16 * LATENT_RANK) ** -0.5, 0.0625, ((1, 8),))
    latent_block_store = scatter_about(seeds[7], (POOL_BLOCKS, BLOCK_POSITIONS, LATENT_RANK), 4.0, 24.0, ((0, 256),))
    rope_pool = draw_rope_pool(jax.random.fold_in(seeds[11], 71), 0)
    lengths = draw_lengths(jax.random.fold_in(seeds[11], 71), 0)
    block_table = draw_block_table(jax.random.fold_in(seeds[11], 71), 0)
    return {"hidden_in": hidden_in, "united_down": united_down, "q_gain": q_gain, "kv_gain": kv_gain, "q_up": q_up, "key_up": key_up, "value_up": value_up, "latent_block_store": latent_block_store, "rope_pool": rope_pool, "lengths": lengths, "block_table": block_table}


NORM_FLOOR = 1.0

def rms_scale(row_values, gain_row):
    mean_square = lax.optimization_barrier(jnp.mean(row_values * row_values, axis=-1, keepdims=True))
    return row_values * lax.rsqrt(mean_square + NORM_FLOOR) * gain_row

def rotate_pairs(rope_pairs, positions):
    half_dim = rope_pairs.shape[-1] // 2
    inverse_freq = 10000.0 ** (-2.0 * jnp.arange(half_dim, dtype=jnp.float32) / rope_pairs.shape[-1])
    angles = positions[..., None] * inverse_freq
    cosine = jnp.cos(angles)
    sine_part = jnp.sin(angles)
    front_half = rope_pairs[..., :half_dim]
    back_half = rope_pairs[..., half_dim:]
    return jnp.concatenate([front_half * cosine - back_half * sine_part, front_half * sine_part + back_half * cosine], axis=-1)

def reference(hidden_in, united_down, q_gain, kv_gain, q_up, key_up, value_up, latent_block_store, rope_pool, lengths, block_table):
    united = jnp.dot(hidden_in, united_down, preferred_element_type=jnp.float32).astype(jnp.bfloat16)
    united_wide = united.astype(jnp.float32)
    positions = lengths.astype(jnp.float32)
    query_latent = rms_scale(united_wide[:, :QR], q_gain).astype(jnp.bfloat16)
    new_latent = rms_scale(united_wide[:, QR:QR + LATENT_RANK], kv_gain).astype(jnp.bfloat16)
    new_rope = rotate_pairs(united_wide[:, QR + LATENT_RANK:], positions).astype(jnp.bfloat16)
    new_entry = jnp.concatenate([new_latent, new_rope], axis=1)
    query_full = jnp.dot(query_latent, q_up, preferred_element_type=jnp.float32).reshape(B, H, QH)
    query_nope = query_full[:, :, :NOPE].astype(jnp.bfloat16)
    key_heads = key_up.reshape(LATENT_RANK, H, NOPE)
    score_scale = QH ** (-0.5)
    absorbed = jnp.einsum('bhn,khn->bhk', query_nope.astype(jnp.float32), key_heads.astype(jnp.float32))
    query_lat = (absorbed * score_scale).astype(jnp.bfloat16)
    query_rot = (rotate_pairs(query_full[:, :, NOPE:], positions[:, None]) * score_scale).astype(jnp.bfloat16)
    cache_rows = jnp.arange(LMAX, dtype=jnp.int32)

    def one_sequence(inputs):
        lat_query, rot_query, table_row, length_one, own_latent, own_rope = inputs
        keys_latent = latent_block_store[table_row].reshape(LMAX, LATENT_RANK)
        keys_rope = jnp.swapaxes(rope_pool[table_row], 1, 2).reshape(LMAX, ROTARY_WIDTH)
        scores = jnp.dot(lat_query, keys_latent.T, preferred_element_type=jnp.float32)
        scores = scores + jnp.dot(rot_query, keys_rope.T, preferred_element_type=jnp.float32)
        valid_mask = cache_rows < length_one
        scores = jnp.where(valid_mask[None, :], scores, -jnp.inf)
        own_score = lax.optimization_barrier(jnp.sum(lat_query.astype(jnp.float32) * own_latent.astype(jnp.float32)[None, :], axis=1))
        own_score = own_score + lax.optimization_barrier(jnp.sum(rot_query.astype(jnp.float32) * own_rope.astype(jnp.float32)[None, :], axis=1))
        top_score = jnp.maximum(lax.optimization_barrier(jnp.max(scores, axis=1)), own_score)
        weights = jnp.exp(scores - top_score[:, None])
        own_weight = jnp.exp(own_score - top_score)
        totals = lax.optimization_barrier(jnp.sum(weights, axis=1)) + own_weight
        mixture = jnp.dot(weights.astype(jnp.bfloat16), keys_latent, preferred_element_type=jnp.float32)
        mixture = mixture + own_weight.astype(jnp.bfloat16).astype(jnp.float32)[:, None] * own_latent.astype(jnp.float32)[None, :]
        return (mixture / totals[:, None]).astype(jnp.bfloat16)
    attended = lax.map(one_sequence, (query_lat, query_rot, block_table, lengths, new_latent, new_rope))
    value_heads = value_up.reshape(LATENT_RANK, H, VD)
    attn_out = jnp.einsum('bhk,khv->bhv', attended.astype(jnp.float32), value_heads.astype(jnp.float32))
    attn_out = attn_out.reshape(B, H * VD).astype(jnp.bfloat16)
    return (attn_out, new_entry)
```

```python
import functools

import jax
import jax.numpy as jnp
from jax import lax
from jax.experimental import pallas as pl
from jax.experimental.pallas import tpu as pltpu
from jax.sharding import Mesh
from jax.sharding import PartitionSpec as P

D = 5120
QR = 1536
LR = 512
NOPE = 128
ROT = 64
VD = 128
B = 16
BP = 128
QH = 192
SCALE = QH ** (-0.5)
FLOOR = -1e30
S = ("z", "x")
T = ("y", "c")
bf16 = jnp.bfloat16
f32 = jnp.float32
VM = pltpu.MemorySpace.VMEM
SM = pltpu.MemorySpace.SMEM
HB = pltpu.MemorySpace.HBM


def spec(space):
    return pl.BlockSpec(memory_space=space)


def exchange(pieces, axes):
    return lax.all_to_all(pieces, axes, split_axis=0, concat_axis=0, tiled=True)


UK = 5


def united_kernel(hid, wt, lat, rope, out, pack_a, pack_b, wbuf, wsem, psem):
    step = D // UK
    copies = []
    for k in range(UK):
        cp = pltpu.make_async_copy(wt.at[:, pl.ds(k * step, step)], wbuf.at[k], wsem.at[k])
        cp.start()
        copies.append(cp)
    packs = []
    for h, dst in enumerate((pack_a, pack_b)):
        packs.append(pltpu.make_async_copy(lat.at[pl.ds(4 * h, 4)], dst.at[:, pl.ds(0, BP), :], psem.at[h, 0]))
        for g in range(4):
            packs.append(
                pltpu.make_async_copy(
                    rope.at[pl.ds(4 * h, 4), pl.ds(16 * g, 16), :],
                    dst.at[:, pl.ds(BP, 16), pl.ds(128 * g, 128)],
                    psem.at[h, 1 + g],
                )
            )
    for p in packs:
        p.start()
    acc = jnp.zeros((B, out.shape[2]), f32)
    for k in range(UK):
        copies[k].wait()
        acc = acc + lax.dot_general(
            hid[:, k * step : (k + 1) * step],
            wbuf[k],
            (((1,), (1,)), ((), ())),
            preferred_element_type=f32,
        )
    val = acc.astype(bf16)
    for i in range(out.shape[0]):
        out[i] = val
    for p in packs:
        p.wait()


def united_call(hid, down, lat, rope):
    cols = down.shape[1]
    half = jax.ShapeDtypeStruct((4, BP + 16, LR), bf16)
    return pl.pallas_call(
        united_kernel,
        out_shape=(jax.ShapeDtypeStruct((8, B, cols), bf16), half, half),
        in_specs=[spec(VM), spec(HB), spec(HB), spec(HB)],
        out_specs=(spec(VM), spec(HB), spec(HB)),
        scratch_shapes=[
            pltpu.VMEM((UK, cols, D // UK), bf16),
            pltpu.SemaphoreType.DMA((UK,)),
            pltpu.SemaphoreType.DMA((2, 5)),
        ],
        name="united",
    )(hid, down.T, lat, rope)


def rotated(x, cs):
    lane = lax.broadcasted_iota(jnp.int32, x.shape, 1)
    swapped = jnp.where(lane < 32, pltpu.roll(x, 96, 1), pltpu.roll(x, 32, 1))
    return x * cs + swapped * pltpu.roll(cs, 64, 1)


def query_kernel(idx, parts, q_gain, kv_gain, cs, q_up, entry, wide, out, ql):
    s = idx[0]
    width = 264
    tiles = [None] * 17
    for i in range(8):
        piece = parts[i].astype(f32)
        piece = jnp.concatenate([piece, jnp.zeros((B, 384 - width), f32)], axis=1)
        if i:
            piece = pltpu.roll(piece, 8 * i, 1)
        for k in range(3):
            part = piece[:, 128 * k : 128 * k + 128]
            if 2 * i + k < 17:
                tiles[2 * i + k] = part if tiles[2 * i + k] is None else tiles[2 * i + k] + part
    u = jnp.concatenate(tiles, axis=1)
    uq = u[:, :QR]
    ul = u[:, QR : QR + LR]
    ur = u[:, QR + LR : QR + LR + 128]
    rq = lax.rsqrt(jnp.sum(uq * uq, axis=1, keepdims=True) / QR + 1.0)
    rl = lax.rsqrt(jnp.sum(ul * ul, axis=1, keepdims=True) / LR + 1.0)
    ql[:, :QR] = (uq * rq * q_gain[...]).astype(bf16).astype(f32)
    ql[:, QR:] = jnp.zeros((B, 128), f32)
    lat = (ul * rl * kv_gain[...]).astype(bf16)
    lane = lax.broadcasted_iota(jnp.int32, (B, 128), 1)
    rot = jnp.where(lane < ROT, rotated(ur, cs[...]), 0.0).astype(bf16)
    entry[:, :LR] = lat
    entry[:, LR:] = rot[:, :ROT]
    wide[:, :LR] = lat.astype(f32)
    wide[:, LR:] = rot.astype(f32)
    first = s * 48
    tile = first // 128
    own = ql[:, pl.ds(pl.multiple_of(tile * 128, 128), 256)]
    own = pltpu.roll(own, 256 - (first - tile * 128), 1)[:, :48].astype(bf16)
    q = jnp.dot(own, q_up[...], preferred_element_type=f32)
    for p in range(8):
        t0 = q[:, 384 * p : 384 * p + 128]
        t1 = q[:, 384 * p + 128 : 384 * p + 256]
        t2 = q[:, 384 * p + 256 : 384 * p + 384]
        hh, j = (2 * p) // 8, (2 * p) % 8
        t1r = pltpu.roll(t1, 64, 1)
        t2r = pltpu.roll(t2, 64, 1)
        out[:, hh, j, :] = t0
        out[:, hh, 8 + j, :] = t1
        out[:, hh, j + 1, :] = jnp.where(lane < 64, t1r, t2r)
        out[:, hh, 8 + j + 1, :] = t2r


def query_call(idx, parts, q_gain, kv_gain, cs, q_up):
    return pl.pallas_call(
        query_kernel,
        out_shape=(
            jax.ShapeDtypeStruct((B, LR + ROT), bf16),
            jax.ShapeDtypeStruct((B, LR + 128), f32),
            jax.ShapeDtypeStruct((B, 2, 16, 128), f32),
        ),
        in_specs=[spec(SM)] + [spec(VM)] * 5,
        out_specs=(spec(VM),) * 3,
        scratch_shapes=[pltpu.VMEM((B, QR + 128), f32)],
        name="query",
    )(idx, parts, q_gain, kv_gain, cs, q_up)


def absorb_kernel(idx, parts, cs, key_up, own, out, keys, sem):
    s = idx[0]
    b, hh = s // 2, s % 2
    cp = pltpu.make_async_copy(key_up.at[:, pl.ds(pl.multiple_of(hh * 1024, 128), 1024)], keys, sem)
    cp.start()
    q = parts[0]
    for i in range(1, 32):
        q = q + parts[i]
    nope = q[:8].astype(bf16)
    rot = rotated(q[8:], jnp.broadcast_to(cs[pl.ds(b, 1), :], (8, 128)))
    lane = lax.broadcasted_iota(jnp.int32, (8, 128), 1)
    row = lax.broadcasted_iota(jnp.int32, (8, 128), 0)
    rot = jnp.where(lane < ROT, rot * SCALE, 0.0).astype(bf16)
    zero = jnp.zeros((8, 128), bf16)
    spread = jnp.concatenate(
        [jnp.where(row == j, nope.astype(f32), 0.0).astype(bf16) for j in range(8)], axis=1
    )
    cp.wait()
    lat = lax.dot_general(spread, keys[...], (((1,), (1,)), ((), ())), preferred_element_type=f32)
    pack = jnp.concatenate([(lat * SCALE).astype(bf16), rot], axis=1)
    own[...] = pack
    for i in range(32):
        out[i] = pack


def absorb_call(idx, parts, cs, key_up):
    return pl.pallas_call(
        absorb_kernel,
        out_shape=(
            jax.ShapeDtypeStruct((8, LR + 128), bf16),
            jax.ShapeDtypeStruct((32, 8, LR + 128), bf16),
        ),
        in_specs=[spec(SM), spec(VM), spec(VM), spec(HB)],
        out_specs=(spec(VM),) * 2,
        scratch_shapes=[pltpu.VMEM((LR, 1024), bf16), pltpu.SemaphoreType.DMA],
        name="absorb",
    )(idx, parts, cs, key_up)


ORDER = [(dy, dc, h) for dy in (0, 3, 1, 2) for dc in (0, 1) for h in (0, 1)]


def attend_kernel(idx, table, lengths, q, *rest):
    bufs, out = rest[:16], rest[16]
    kv, o_s, m_s, l_s, inv, sem = rest[17:]
    s, y, c = idx[0], idx[1], idx[2]

    def load(i):
        return pltpu.make_async_copy(bufs[i], kv.at[i], sem.at[i])

    for i in range(16):
        load(i).start()

    def fill(e, _):
        inv[table[e] - s * 64] = e
        return 0

    lax.fori_loop(0, 64, fill, 0, unroll=8)
    lane = lax.broadcasted_iota(jnp.int32, (B, BP), 1)

    def group(i, _):
        pltpu.make_async_copy(kv.at[i], kv.at[i], sem.at[i]).wait()
        dyi = i // 4
        dy = jnp.where(dyi == 0, 0, jnp.where(dyi == 1, 3, jnp.where(dyi == 2, 1, 2)))
        dc = (i // 2) % 2
        half = i % 2
        ys = lax.rem(y + dy, 4)
        cs = c + dc - 2 * c * dc
        first = (ys * 2 + cs) * 8 + half * 4
        for k in range(4):
            e = inv[first + k]
            b = e // 4
            limit = lengths[b] - (s * 4 + e - b * 4) * BP
            qb = q[b]
            keys = kv[i, k, :BP, :]
            rope = jnp.concatenate([kv[i, k, BP:, 128 * g : 128 * g + 128] for g in range(4)], axis=0)
            sc = lax.dot_general(qb[:, :LR], keys, (((1,), (1,)), ((), ())), preferred_element_type=f32)
            sc = sc + jnp.dot(qb[:, LR : LR + ROT], rope, preferred_element_type=f32)
            live = lane < limit
            sc = jnp.where(live, sc, FLOOR)
            m = jnp.max(sc, axis=1, keepdims=True)
            p = jnp.where(live, jnp.exp(sc - m), 0.0)
            l = jnp.sum(p, axis=1, keepdims=True)
            o_s[e] = jnp.dot(p.astype(bf16), keys, preferred_element_type=f32)
            m_s[e] = jnp.broadcast_to(m, (B, 128))
            l_s[e] = jnp.broadcast_to(l, (B, 128))
        return 0

    lax.fori_loop(0, 16, group, 0)

    def join(b, _):
        m4 = [m_s[b * 4 + j] for j in range(4)]
        m = jnp.maximum(jnp.maximum(m4[0], m4[1]), jnp.maximum(m4[2], m4[3]))
        w = [jnp.exp(v - m) for v in m4]
        l = sum(w[j] * l_s[b * 4 + j] for j in range(4))
        m1 = m.astype(bf16).astype(f32)
        m2 = (m - m1).astype(bf16).astype(f32)
        m3 = m - m1 - m2
        l1 = l.astype(bf16).astype(f32)
        l2 = (l - l1).astype(bf16).astype(f32)
        l3 = l - l1 - l2
        stats = jnp.zeros((B, 128), f32)
        for n, v in enumerate((m1, m2, m3, l1, l2, l3)):
            stats = jnp.where(lane == n, v, stats)
        mix = sum(jnp.concatenate([w[j]] * 4, axis=1) * o_s[b * 4 + j] for j in range(4))
        both = jnp.concatenate([mix, stats], axis=1).astype(bf16)
        out[b] = both
        return 0

    lax.fori_loop(0, B, join, 0, unroll=2)


def attend_call(idx, table, lengths, q, bufs):
    return pl.pallas_call(
        attend_kernel,
        out_shape=jax.ShapeDtypeStruct((B, 16, LR + 128), bf16),
        in_specs=[spec(SM)] * 3 + [spec(VM)] + [spec(HB)] * 16,
        out_specs=spec(VM),
        scratch_shapes=[
            pltpu.VMEM((16, 4, BP + 16, LR), bf16),
            pltpu.VMEM((64, B, LR), f32),
            pltpu.VMEM((64, B, 128), f32),
            pltpu.VMEM((64, B, 128), f32),
            pltpu.SMEM((64,), jnp.int32),
            pltpu.SemaphoreType.DMA((16,)),
        ],
        name="attend",
    )(idx, table, lengths, q, *bufs)


def value_kernel(idx, parts, own, wide, value_up, out, vals, sem):
    s = idx[0]
    b, hh = s // 2, s % 2
    cp = pltpu.make_async_copy(value_up.at[:, pl.ds(pl.multiple_of(hh * 1024, 128), 1024)], vals, sem)
    cp.start()
    entry = wide[pl.ds(b, 1), :]
    own_score = jnp.sum(own[...].astype(f32) * entry, axis=1, keepdims=True)
    tops, tots = [], []
    for i in range(32):
        st = parts[i, :, LR:].astype(f32)
        tops.append(st[:, 0:1] + st[:, 1:2] + st[:, 2:3])
        tots.append(st[:, 3:4] + st[:, 4:5] + st[:, 5:6])
    top = own_score
    for i in range(32):
        top = jnp.maximum(top, tops[i])
    own_w = jnp.exp(own_score - top)
    total = own_w
    mix = own_w.astype(bf16).astype(f32) * entry[:, :LR]
    for i in range(32):
        w = jnp.exp(tops[i] - top)
        total = total + w * tots[i]
        mix = mix + w * parts[i, :, :LR].astype(f32)
    att = (mix / total).astype(bf16)
    cp.wait()
    full = jnp.dot(att, vals[...], preferred_element_type=f32)
    row = lax.broadcasted_iota(jnp.int32, (8, 128), 0)
    res = jnp.zeros((8, 128), f32)
    for j in range(8):
        res = jnp.where(row == j, full[:, 128 * j : 128 * j + 128], res)
    res = res.astype(bf16)
    for i in range(32):
        out[i] = res


def value_call(idx, parts, own, wide, value_up):
    return pl.pallas_call(
        value_kernel,
        out_shape=jax.ShapeDtypeStruct((32, 8, VD), bf16),
        in_specs=[spec(SM), spec(VM), spec(VM), spec(VM), spec(HB)],
        out_specs=spec(VM),
        scratch_shapes=[pltpu.VMEM((LR, 1024), bf16), pltpu.SemaphoreType.DMA],
        name="value",
    )(idx, parts, own, wide, value_up)


UP = [(i, (i + 1) % 4) for i in range(4)]
DOWN = [(i, (i + 3) % 4) for i in range(4)]
SWAP = [(0, 1), (1, 0)]


def body(hidden_in, united_down, q_gain, kv_gain, q_up, key_up, value_up, store, rope_pool, lengths, table):
    s = lax.axis_index(S)
    idx = jnp.stack([s, lax.axis_index("y"), lax.axis_index("c")]).astype(jnp.int32)
    cols, half_a, half_b = united_call(hidden_in, united_down, store, rope_pool)
    freq = 10000.0 ** (-2.0 * jnp.arange(32, dtype=f32) / ROT)
    angles = lengths.astype(f32)[:, None] * freq
    cos, sin = jnp.cos(angles), jnp.sin(angles)
    cs = jnp.concatenate([cos, cos, -sin, sin], axis=1)
    parts = exchange(cols, T)
    up_a = lax.ppermute(half_a, "y", UP)
    down_b = lax.ppermute(half_b, "y", DOWN)
    up_b = lax.ppermute(half_b, "y", UP)
    down_a = lax.ppermute(half_a, "y", DOWN)
    far_a = lax.ppermute(up_a, "y", UP)
    far_b = lax.ppermute(down_b, "y", DOWN)
    near = {0: (half_a, half_b), 3: (up_a, up_b), 1: (down_a, down_b), 2: (far_a, far_b)}
    bufs = []
    for dy, dc, h in ORDER:
        bufs.append(near[dy][h] if dc == 0 else lax.ppermute(near[dy][h], "c", SWAP))
    entry, wide, q_part = query_call(idx, parts, q_gain[None], kv_gain[None], cs, q_up)
    q_sum = exchange(q_part.reshape(32, 16, 128), S)
    own, q_copies = absorb_call(idx, q_sum, cs, key_up)
    q_all = exchange(q_copies, S).reshape(B, 16, LR + 128)
    mixed = attend_call(idx, table.reshape(-1), lengths, q_all, bufs)
    spans = exchange(mixed.reshape(32, 8, LR + 128), S)
    res = exchange(value_call(idx, spans, own, wide, value_up), S)
    return res.reshape(B, 16 * VD), entry


def solution(mesh):
    split = Mesh(mesh.devices.reshape(8, 4, 4, 2), ("z", "x", "y", "c"))
    return jax.shard_map(
        body,
        mesh=split,
        in_specs=(
            P(),
            P(None, T),
            P(),
            P(),
            P(S, T),
            P(None, T),
            P(None, T),
            P(S + T, None, None),
            P(S + T, None, None),
            P(),
            P(None, S),
        ),
        out_specs=(P(None, T), P()),
        check_vma=False,
    )
```

```python
import jax
import jax.numpy as jnp
from jax import lax
from jax.experimental import pallas as pl
from jax.experimental.pallas import tpu as pltpu
from jax.sharding import Mesh
from jax.sharding import PartitionSpec as P


D = 5120
QR = 1536
LR = 512
ROT = 64
VD = 128
B = 16
BP = 128
QH = 192
SCALE = QH ** (-0.5)
FLOOR = -1e30
S = ("z", "x")
T = ("y", "c")
bf16 = jnp.bfloat16
f32 = jnp.float32
VM = pltpu.MemorySpace.VMEM
SM = pltpu.MemorySpace.SMEM
HB = pltpu.MemorySpace.HBM


def spec(space):
    return pl.BlockSpec(memory_space=space)


def exchange(pieces, axes):
    return lax.all_to_all(pieces, axes, split_axis=0, concat_axis=0, tiled=True)


UK = 5


def united_kernel(hid, wt, lat, rope, out, pack_a, pack_b, wbuf, cache, ropes, wsem, psem):
    step = D // UK
    copies = []
    for k in range(UK):
        cp = pltpu.make_async_copy(wt.at[:, pl.ds(k * step, step)], wbuf.at[k], wsem.at[k])
        cp.start()
        copies.append(cp)
    fetch_rope = pltpu.make_async_copy(rope, ropes, psem.at[0])
    fetch_rope.start()
    fetch_lat = pltpu.make_async_copy(lat, cache.at[:, pl.ds(0, BP), :], psem.at[1])
    fetch_lat.start()
    acc = jnp.zeros((B, out.shape[2]), f32)
    for k in range(UK):
        copies[k].wait()
        acc = acc + lax.dot_general(
            hid[:, k * step : (k + 1) * step],
            wbuf[k],
            (((1,), (1,)), ((), ())),
            preferred_element_type=f32,
        )
    fetch_rope.wait()
    for n in range(8):
        for g in range(4):
            cache[n, BP:, 128 * g : 128 * g + 128] = ropes[n, 16 * g : 16 * g + 16, :]
    fetch_lat.wait()
    stores = []
    for h, dst in enumerate((pack_a, pack_b)):
        st = pltpu.make_async_copy(cache.at[pl.ds(4 * h, 4)], dst, psem.at[2 + h])
        st.start()
        stores.append(st)
    val = acc.astype(bf16)
    for i in range(out.shape[0]):
        out[i] = val
    for st in stores:
        st.wait()


def united_call(hid, down, lat, rope):
    cols = down.shape[1]
    half = jax.ShapeDtypeStruct((4, BP + 16, LR), bf16)
    return pl.pallas_call(
        united_kernel,
        out_shape=(jax.ShapeDtypeStruct((8, B, cols), bf16), half, half),
        in_specs=[spec(VM), spec(HB), spec(HB), spec(HB)],
        out_specs=(spec(VM), spec(HB), spec(HB)),
        scratch_shapes=[
            pltpu.VMEM((UK, cols, D // UK), bf16),
            pltpu.VMEM((8, BP + 16, LR), bf16),
            pltpu.VMEM((8, ROT, BP), bf16),
            pltpu.SemaphoreType.DMA((UK,)),
            pltpu.SemaphoreType.DMA((4,)),
        ],
        name="united",
    )(hid, down.T, lat, rope)


def rotated(x, cs):
    lane = lax.broadcasted_iota(jnp.int32, x.shape, 1)
    swapped = jnp.where(lane < 32, pltpu.roll(x, 96, 1), pltpu.roll(x, 32, 1))
    return x * cs + swapped * pltpu.roll(cs, 64, 1)


def query_kernel(idx, parts, q_gain, kv_gain, cs, q_up, entry, wide, out, ql):
    s = idx[0]
    width = 264
    tiles = [None] * 17
    for i in range(8):
        piece = parts[i].astype(f32)
        piece = jnp.concatenate([piece, jnp.zeros((B, 384 - width), f32)], axis=1)
        if i:
            piece = pltpu.roll(piece, 8 * i, 1)
        for k in range(3):
            part = piece[:, 128 * k : 128 * k + 128]
            if 2 * i + k < 17:
                tiles[2 * i + k] = part if tiles[2 * i + k] is None else tiles[2 * i + k] + part
    u = jnp.concatenate(tiles, axis=1)
    uq = u[:, :QR]
    ul = u[:, QR : QR + LR]
    ur = u[:, QR + LR : QR + LR + 128]
    rq = lax.rsqrt(jnp.sum(uq * uq, axis=1, keepdims=True) / QR + 1.0)
    rl = lax.rsqrt(jnp.sum(ul * ul, axis=1, keepdims=True) / LR + 1.0)
    ql[:, :QR] = (uq * rq * q_gain[...]).astype(bf16).astype(f32)
    ql[:, QR:] = jnp.zeros((B, 128), f32)
    lat = (ul * rl * kv_gain[...]).astype(bf16)
    lane = lax.broadcasted_iota(jnp.int32, (B, 128), 1)
    rot = jnp.where(lane < ROT, rotated(ur, cs[...]), 0.0).astype(bf16)
    entry[:, :LR] = lat
    entry[:, LR:] = rot[:, :ROT]
    wide[:, :LR] = lat.astype(f32)
    wide[:, LR:] = rot.astype(f32)
    first = s * 48
    tile = first // 128
    own = ql[:, pl.ds(pl.multiple_of(tile * 128, 128), 256)]
    own = pltpu.roll(own, 256 - (first - tile * 128), 1)[:, :48].astype(bf16)
    q = jnp.dot(own, q_up[...], preferred_element_type=f32)
    for p in range(8):
        t0 = q[:, 384 * p : 384 * p + 128]
        t1 = q[:, 384 * p + 128 : 384 * p + 256]
        t2 = q[:, 384 * p + 256 : 384 * p + 384]
        hh, j = (2 * p) // 8, (2 * p) % 8
        t1r = pltpu.roll(t1, 64, 1)
        t2r = pltpu.roll(t2, 64, 1)
        out[:, hh, j, :] = t0
        out[:, hh, 8 + j, :] = t1
        out[:, hh, j + 1, :] = jnp.where(lane < 64, t1r, t2r)
        out[:, hh, 8 + j + 1, :] = t2r


def query_call(idx, parts, q_gain, kv_gain, cs, q_up):
    return pl.pallas_call(
        query_kernel,
        out_shape=(
            jax.ShapeDtypeStruct((B, LR + ROT), bf16),
            jax.ShapeDtypeStruct((B, LR + 128), f32),
            jax.ShapeDtypeStruct((B, 2, 16, 128), f32),
        ),
        in_specs=[spec(SM)] + [spec(VM)] * 5,
        out_specs=(spec(VM),) * 3,
        scratch_shapes=[pltpu.VMEM((B, QR + 128), f32)],
        name="query",
    )(idx, parts, q_gain, kv_gain, cs, q_up)


def absorb_kernel(idx, parts, cs, key_up, own, out, keys, sem):
    s = idx[0]
    b, hh = s // 2, s % 2
    cp = pltpu.make_async_copy(key_up.at[:, pl.ds(pl.multiple_of(hh * 1024, 128), 1024)], keys, sem)
    cp.start()
    q = parts[0]
    for i in range(1, 32):
        q = q + parts[i]
    nope = q[:8].astype(bf16)
    rot = rotated(q[8:], jnp.broadcast_to(cs[pl.ds(b, 1), :], (8, 128)))
    lane = lax.broadcasted_iota(jnp.int32, (8, 128), 1)
    row = lax.broadcasted_iota(jnp.int32, (8, 128), 0)
    rot = jnp.where(lane < ROT, rot * SCALE, 0.0).astype(bf16)
    zero = jnp.zeros((8, 128), bf16)
    spread = jnp.concatenate(
        [jnp.where(row == j, nope.astype(f32), 0.0).astype(bf16) for j in range(8)], axis=1
    )
    cp.wait()
    lat = lax.dot_general(spread, keys[...], (((1,), (1,)), ((), ())), preferred_element_type=f32)
    pack = jnp.concatenate([(lat * SCALE).astype(bf16), rot], axis=1)
    own[...] = pack
    for i in range(32):
        out[i] = pack


def absorb_call(idx, parts, cs, key_up):
    return pl.pallas_call(
        absorb_kernel,
        out_shape=(
            jax.ShapeDtypeStruct((8, LR + 128), bf16),
            jax.ShapeDtypeStruct((32, 8, LR + 128), bf16),
        ),
        in_specs=[spec(SM), spec(VM), spec(VM), spec(HB)],
        out_specs=(spec(VM),) * 2,
        scratch_shapes=[pltpu.VMEM((LR, 1024), bf16), pltpu.SemaphoreType.DMA],
        name="absorb",
    )(idx, parts, cs, key_up)


ORDER = [(dy, dc, h) for dy in (0, 3, 1, 2) for dc in (0, 1) for h in (0, 1)]


def attend_kernel(idx, table, lengths, q, *rest):
    bufs, out = rest[:16], rest[16]
    kv, s_s, p_s, st_s, inv, place, sem = rest[17:]
    s, y, c = idx[0], idx[1], idx[2]
    for i in range(16):
        pltpu.make_async_copy(bufs[i], kv.at[pl.ds(4 * i, 4)], sem.at[i // 4]).start()

    def fill(e, _):
        inv[table[e] - s * 64] = e
        return 0

    lax.fori_loop(0, 64, fill, 0, unroll=8)
    lane = lax.broadcasted_iota(jnp.int32, (B, BP), 1)

    def scores(g, _):
        here = kv.at[pl.ds(16 * g, 16)]
        pltpu.make_async_copy(here, here, sem.at[g]).wait()
        dy = jnp.where(g == 0, 0, jnp.where(g == 1, 3, jnp.where(g == 2, 1, 2)))
        ys = lax.rem(y + dy, 4)
        for dc in range(2):
            cs = c if dc == 0 else 1 - c
            first = (ys * 2 + cs) * 8
            for k in range(8):
                at = g * 16 + dc * 8 + k
                e = inv[first + k]
                place[e] = at
                qb = q[e // 4]
                keys = kv[at, :BP, :]
                rope = jnp.concatenate([kv[at, BP:, 128 * n : 128 * n + 128] for n in range(4)], axis=0)
                sc = lax.dot_general(qb[:, :LR], keys, (((1,), (1,)), ((), ())), preferred_element_type=f32)
                s_s[e] = sc + jnp.dot(qb[:, LR : LR + ROT], rope, preferred_element_type=f32)
        return 0

    lax.fori_loop(0, 4, scores, 0)

    def softmax(b, _):
        room = lengths[b] - s * (4 * BP)
        live = [lane < room - j * BP for j in range(4)]
        sc = [jnp.where(live[j], s_s[b * 4 + j], FLOOR) for j in range(4)]
        m = jnp.maximum(jnp.maximum(sc[0], sc[1]), jnp.maximum(sc[2], sc[3]))
        m = jnp.max(m, axis=1, keepdims=True)
        p = [jnp.where(live[j], jnp.exp(sc[j] - m), 0.0) for j in range(4)]
        l = jnp.sum((p[0] + p[1]) + (p[2] + p[3]), axis=1, keepdims=True)
        m1 = m.astype(bf16).astype(f32)
        m2 = (m - m1).astype(bf16).astype(f32)
        m3 = m - m1 - m2
        l1 = l.astype(bf16).astype(f32)
        l2 = (l - l1).astype(bf16).astype(f32)
        l3 = l - l1 - l2
        stats = jnp.zeros((B, 128), f32)
        for n, v in enumerate((m1, m2, m3, l1, l2, l3)):
            stats = jnp.where(lane == n, v, stats)
        st_s[b] = stats.astype(bf16)
        p_s[b] = jnp.concatenate(p, axis=1).astype(bf16)
        return 0

    lax.fori_loop(0, B, softmax, 0, unroll=4)

    def mixing(b, _):
        p = p_s[b]
        mix = jnp.zeros((B, LR), f32)
        for j in range(4):
            keys = kv[place[b * 4 + j], :BP, :]
            mix = mix + jnp.dot(p[:, 128 * j : 128 * j + 128], keys, preferred_element_type=f32)
        out[b] = jnp.concatenate([mix.astype(bf16), st_s[b]], axis=1)
        return 0

    lax.fori_loop(0, B, mixing, 0, unroll=4)


def attend_call(idx, table, lengths, q, bufs):
    return pl.pallas_call(
        attend_kernel,
        out_shape=jax.ShapeDtypeStruct((B, 16, LR + 128), bf16),
        in_specs=[spec(SM)] * 3 + [spec(VM)] + [spec(HB)] * 16,
        out_specs=spec(VM),
        scratch_shapes=[
            pltpu.VMEM((64, BP + 16, LR), bf16),
            pltpu.VMEM((64, B, BP), f32),
            pltpu.VMEM((B, B, 4 * BP), bf16),
            pltpu.VMEM((B, B, 128), bf16),
            pltpu.SMEM((64,), jnp.int32),
            pltpu.SMEM((64,), jnp.int32),
            pltpu.SemaphoreType.DMA((4,)),
        ],
        name="attend",
    )(idx, table, lengths, q, *bufs)


def value_kernel(idx, parts, own, wide, value_up, out, vals, sem):
    s = idx[0]
    b, hh = s // 2, s % 2
    cp = pltpu.make_async_copy(value_up.at[:, pl.ds(pl.multiple_of(hh * 1024, 128), 1024)], vals, sem)
    cp.start()
    entry = wide[pl.ds(b, 1), :]
    own_score = jnp.sum(own[...].astype(f32) * entry, axis=1, keepdims=True)
    tops, tots = [], []
    for i in range(32):
        st = parts[i, :, LR:].astype(f32)
        tops.append(st[:, 0:1] + st[:, 1:2] + st[:, 2:3])
        tots.append(st[:, 3:4] + st[:, 4:5] + st[:, 5:6])
    top = own_score
    for i in range(32):
        top = jnp.maximum(top, tops[i])
    own_w = jnp.exp(own_score - top)
    total = own_w
    mix = own_w.astype(bf16).astype(f32) * entry[:, :LR]
    for i in range(32):
        w = jnp.exp(tops[i] - top)
        total = total + w * tots[i]
        mix = mix + w * parts[i, :, :LR].astype(f32)
    att = (mix / total).astype(bf16)
    cp.wait()
    full = jnp.dot(att, vals[...], preferred_element_type=f32)
    row = lax.broadcasted_iota(jnp.int32, (8, 128), 0)
    res = jnp.zeros((8, 128), f32)
    for j in range(8):
        res = jnp.where(row == j, full[:, 128 * j : 128 * j + 128], res)
    res = res.astype(bf16)
    for i in range(32):
        out[i] = res


def value_call(idx, parts, own, wide, value_up):
    return pl.pallas_call(
        value_kernel,
        out_shape=jax.ShapeDtypeStruct((32, 8, VD), bf16),
        in_specs=[spec(SM), spec(VM), spec(VM), spec(VM), spec(HB)],
        out_specs=spec(VM),
        scratch_shapes=[pltpu.VMEM((LR, 1024), bf16), pltpu.SemaphoreType.DMA],
        name="value",
    )(idx, parts, own, wide, value_up)


UP = [(i, (i + 1) % 4) for i in range(4)]
DOWN = [(i, (i + 3) % 4) for i in range(4)]
SWAP = [(0, 1), (1, 0)]


def body(hidden_in, united_down, q_gain, kv_gain, q_up, key_up, value_up, store, rope_pool, lengths, table):
    s = lax.axis_index(S)
    idx = jnp.stack([s, lax.axis_index("y"), lax.axis_index("c")]).astype(jnp.int32)
    cols, half_a, half_b = united_call(hidden_in, united_down, store, rope_pool)
    freq = 10000.0 ** (-2.0 * jnp.arange(32, dtype=f32) / ROT)
    angles = lengths.astype(f32)[:, None] * freq
    cos, sin = jnp.cos(angles), jnp.sin(angles)
    cs = jnp.concatenate([cos, cos, -sin, sin], axis=1)
    parts = exchange(cols, T)
    up_a = lax.ppermute(half_a, "y", UP)
    down_b = lax.ppermute(half_b, "y", DOWN)
    up_b = lax.ppermute(half_b, "y", UP)
    down_a = lax.ppermute(half_a, "y", DOWN)
    far_a = lax.ppermute(up_a, "y", UP)
    far_b = lax.ppermute(down_b, "y", DOWN)
    near = {0: (half_a, half_b), 3: (up_a, up_b), 1: (down_a, down_b), 2: (far_a, far_b)}
    bufs = []
    for dy, dc, h in ORDER:
        bufs.append(near[dy][h] if dc == 0 else lax.ppermute(near[dy][h], "c", SWAP))
    entry, wide, q_part = query_call(idx, parts, q_gain[None], kv_gain[None], cs, q_up)
    q_sum = exchange(q_part.reshape(32, 16, 128), S)
    own, q_copies = absorb_call(idx, q_sum, cs, key_up)
    q_all = exchange(q_copies, S)
    q_all = q_all.reshape(B, 16, LR + 128)
    mixed = attend_call(idx, table.reshape(-1), lengths, q_all, bufs)
    spans = exchange(mixed.reshape(32, 8, LR + 128), S)
    res = value_call(idx, spans, own, wide, value_up)
    res = exchange(res, S)
    return res.reshape(B, 16 * VD), entry


def solution(mesh):
    split = Mesh(mesh.devices.reshape(8, 4, 4, 2), ("z", "x", "y", "c"))
    return jax.shard_map(
        body,
        mesh=split,
        in_specs=(
            P(),
            P(None, T),
            P(),
            P(),
            P(S, T),
            P(None, T),
            P(None, T),
            P(S + T, None, None),
            P(S + T, None, None),
            P(),
            P(None, S),
        ),
        out_specs=(P(None, T), P()),
        check_vma=False,
    )
```

```python
import functools

import jax
import jax.numpy as jnp
from jax import lax
from jax.experimental import pallas as pl
from jax.experimental.pallas import tpu as pltpu
from jax.sharding import Mesh
from jax.sharding import PartitionSpec as P


D = 5120
QR = 1536
LR = 512
ROT = 64
VD = 128
B = 16
BP = 128
QH = 192
SCALE = QH ** (-0.5)
FLOOR = -1e30
S = ("z", "x")
T = ("y", "c")
bf16 = jnp.bfloat16
f32 = jnp.float32
VM = pltpu.MemorySpace.VMEM
SM = pltpu.MemorySpace.SMEM
HB = pltpu.MemorySpace.HBM


def spec(space):
    return pl.BlockSpec(memory_space=space)


def exchange(pieces, axes):
    return lax.all_to_all(pieces, axes, split_axis=0, concat_axis=0, tiled=True)


UK = 5


def united_kernel(hid, wt, out, wbuf, wsem):
    step = D // UK
    copies = []
    for k in range(UK):
        cp = pltpu.make_async_copy(wt.at[:, pl.ds(k * step, step)], wbuf.at[k], wsem.at[k])
        cp.start()
        copies.append(cp)
    acc = jnp.zeros(out.shape, f32)
    for k in range(UK):
        copies[k].wait()
        acc = acc + lax.dot_general(
            hid[:, k * step : (k + 1) * step],
            wbuf[k],
            (((1,), (1,)), ((), ())),
            preferred_element_type=f32,
        )
    out[...] = acc.astype(bf16)


def united_call(hid, down):
    cols = down.shape[1]
    return pl.pallas_call(
        united_kernel,
        out_shape=jax.ShapeDtypeStruct((B, cols), bf16),
        in_specs=[spec(VM), spec(HB)],
        out_specs=spec(VM),
        scratch_shapes=[pltpu.VMEM((UK, cols, D // UK), bf16), pltpu.SemaphoreType.DMA((UK,))],
        name="united",
    )(hid, down.T)


def tiles_kernel(q_up, out):
    for k in range(32):
        j = k % 24
        out[k] = q_up[:, 128 * j : 128 * j + 128]


def tiles_call(q_up):
    return pl.pallas_call(
        tiles_kernel,
        out_shape=jax.ShapeDtypeStruct((32, 48, 128), bf16),
        in_specs=[spec(VM)],
        out_specs=spec(VM),
        name="tiles",
    )(q_up)


def pack_kernel(lat, rope, pack_a, pack_b, cache, ropes, sem):
    fetch_rope = pltpu.make_async_copy(rope, ropes, sem.at[0])
    fetch_rope.start()
    fetch = []
    for h in range(2):
        cp = pltpu.make_async_copy(lat.at[pl.ds(4 * h, 4)], cache.at[pl.ds(4 * h, 4), pl.ds(0, BP), :], sem.at[1 + h])
        cp.start()
        fetch.append(cp)
    fetch_rope.wait()
    for n in range(8):
        for g in range(4):
            cache[n, BP:, 128 * g : 128 * g + 128] = ropes[n, 16 * g : 16 * g + 16, :]
    stores = []
    for h, dst in enumerate((pack_a, pack_b)):
        fetch[h].wait()
        st = pltpu.make_async_copy(cache.at[pl.ds(4 * h, 4)], dst, sem.at[3 + h])
        st.start()
        stores.append(st)
    for st in stores:
        st.wait()


def pack_call(lat, rope):
    half = jax.ShapeDtypeStruct((4, BP + 16, LR), bf16)
    return pl.pallas_call(
        pack_kernel,
        out_shape=(half, half),
        in_specs=[spec(HB), spec(HB)],
        out_specs=(spec(HB), spec(HB)),
        scratch_shapes=[
            pltpu.VMEM((8, BP + 16, LR), bf16),
            pltpu.VMEM((8, ROT, BP), bf16),
            pltpu.SemaphoreType.DMA((5,)),
        ],
        name="pack",
    )(lat, rope)


def swapped(x):
    lane = lax.broadcasted_iota(jnp.int32, x.shape, 1)
    return jnp.where(lane % ROT < ROT // 2, pltpu.roll(x, 96, 1), pltpu.roll(x, 32, 1))


def query_kernel(idx, *refs):
    pieces, (q_gain, kv_gain, cos, sin, weights, entry, wide, out, parts) = refs[:8], refs[8:]
    s, y, c = idx[0], idx[1], idx[2]
    width = 264
    for i in range(8):
        cp = c if i % 2 == 0 else 1 - c
        parts[lax.rem(y + i // 2, 4) * 2 + cp] = pieces[i][...].astype(f32)
    tiles = [None] * 17
    for i in range(8):
        piece = parts[i]
        piece = jnp.concatenate([piece, jnp.zeros((B, 384 - width), f32)], axis=1)
        if i:
            piece = pltpu.roll(piece, 8 * i, 1)
        for k in range(3):
            part = piece[:, 128 * k : 128 * k + 128]
            if 2 * i + k < 17:
                tiles[2 * i + k] = part if tiles[2 * i + k] is None else tiles[2 * i + k] + part
    u = jnp.concatenate(tiles, axis=1)
    uq = u[:, :QR]
    ul = u[:, QR : QR + LR]
    ur = u[:, QR + LR : QR + LR + 128]
    rq = lax.rsqrt(jnp.sum(uq * uq, axis=1, keepdims=True) / QR + 1.0)
    rl = lax.rsqrt(jnp.sum(ul * ul, axis=1, keepdims=True) / LR + 1.0)
    ql = (uq * rq * q_gain[...]).astype(bf16)
    q = jnp.dot(ql, weights[...].reshape(QR, 128), preferred_element_type=f32)
    lane = lax.broadcasted_iota(jnp.int32, (B, 128), 1)
    kind = lax.rem(s, 3)
    in_rope = ((lane < ROT) & (kind == 1)) | ((lane >= ROT) & (kind == 2))
    res = jnp.where(in_rope, (q * cos[...] + swapped(q) * sin[...]) * SCALE, q).astype(bf16)
    for i in range(32):
        out[i] = res
    lat = (ul * rl * kv_gain[...]).astype(bf16)
    rot = jnp.where(lane < ROT, ur * cos[...] + swapped(ur) * sin[...], 0.0).astype(bf16)
    entry[:, :LR] = lat
    entry[:, LR:] = rot[:, :ROT]
    wide[:, :LR] = lat.astype(f32)
    wide[:, LR:] = rot.astype(f32)


def query_call(idx, parts, q_gain, kv_gain, cos, sin, weights):
    return pl.pallas_call(
        query_kernel,
        out_shape=(
            jax.ShapeDtypeStruct((B, LR + ROT), bf16),
            jax.ShapeDtypeStruct((B, LR + 128), f32),
            jax.ShapeDtypeStruct((32, B, 128), bf16),
        ),
        in_specs=[spec(SM)] + [spec(VM)] * 13,
        out_specs=(spec(VM),) * 3,
        scratch_shapes=[pltpu.VMEM((8, B, 264), f32)],
        name="query",
    )(idx, *parts, q_gain, kv_gain, cos, sin, weights)


ORDER = [(dy, dc, h) for dy in (0, 3, 1, 2) for dc in (0, 1) for h in (0, 1)]


def attend_kernel(idx, table, lengths, q, wide, key_up, *rest):
    bufs, out = rest[:16], rest[16]
    keys_v, kv, q_s, s_s, p_s, o_s, own_s, inv, place, ksem, sem = rest[17:]
    s, y, c = idx[0], idx[1], idx[2]
    load_keys = pltpu.make_async_copy(key_up, keys_v, ksem)
    load_keys.start()
    for i in range(16):
        pltpu.make_async_copy(bufs[i], kv.at[pl.ds(4 * i, 4)], sem.at[i // 4]).start()

    def fill(e, _):
        inv[table[e] - s * 64] = e
        return 0

    lax.fori_loop(0, 64, fill, 0, unroll=8)
    lane = lax.broadcasted_iota(jnp.int32, (B, BP), 1)
    load_keys.wait()
    for p in range(8):
        t0 = q[3 * p].astype(f32)
        t1 = pltpu.roll(q[3 * p + 1].astype(f32), 64, 1)
        t2 = pltpu.roll(q[3 * p + 2].astype(f32), 64, 1)
        r0 = q[3 * p + 1].astype(f32)
        nopes = (t0, jnp.where(lane < ROT, t1, t2))
        ropes = (jnp.where(lane < ROT, r0, 0.0), jnp.where(lane < ROT, t2, 0.0))
        for j in range(2):
            h = 2 * p + j
            lat = lax.dot_general(
                nopes[j].astype(bf16),
                keys_v[:, 128 * h : 128 * h + 128],
                (((1,), (1,)), ((), ())),
                preferred_element_type=f32,
            )
            q_s[:, h, :LR] = (lat * SCALE).astype(bf16).astype(f32)
            q_s[:, h, LR:] = ropes[j]

    def scores(g, _):
        here = kv.at[pl.ds(16 * g, 16)]
        pltpu.make_async_copy(here, here, sem.at[g]).wait()
        dy = jnp.where(g == 0, 0, jnp.where(g == 1, 3, jnp.where(g == 2, 1, 2)))
        ys = lax.rem(y + dy, 4)
        for dc in range(2):
            cs = c if dc == 0 else 1 - c
            first = (ys * 2 + cs) * 8
            for k in range(8):
                at = g * 16 + dc * 8 + k
                e = inv[first + k]
                place[e] = at
                qb = q_s[e // 4].astype(bf16)
                keys = kv[at, :BP, :]
                rope = jnp.concatenate([kv[at, BP:, 128 * n : 128 * n + 128] for n in range(4)], axis=0)
                sc = lax.dot_general(qb[:, :LR], keys, (((1,), (1,)), ((), ())), preferred_element_type=f32)
                s_s[e] = sc + jnp.dot(qb[:, LR : LR + ROT], rope, preferred_element_type=f32)
        return 0

    lax.fori_loop(0, 4, scores, 0)

    def softmax(bh, r):
        b = bh * 8 + r
        room = lengths[b] - s * (4 * BP)
        new = jnp.sum(q_s[b] * wide[pl.ds(b, 1), :], axis=1, keepdims=True)
        mine = jnp.full((B, 1), s, jnp.int32) == 0
        live = [lane < room - j * BP for j in range(4)]
        sc = [jnp.where(live[j], s_s[b * 4 + j], FLOOR) for j in range(4)]
        m = jnp.maximum(jnp.maximum(sc[0], sc[1]), jnp.maximum(sc[2], sc[3]))
        m = jnp.maximum(jnp.max(m, axis=1, keepdims=True), jnp.where(mine, new, FLOOR))
        p = [jnp.where(live[j], jnp.exp(sc[j] - m), 0.0) for j in range(4)]
        new = jnp.where(mine, jnp.exp(new - m), 0.0)
        l = jnp.sum((p[0] + p[1]) + (p[2] + p[3]), axis=1, keepdims=True) + new
        m1 = m.astype(bf16).astype(f32)
        m2 = (m - m1).astype(bf16).astype(f32)
        m3 = m - m1 - m2
        l1 = l.astype(bf16).astype(f32)
        l2 = (l - l1).astype(bf16).astype(f32)
        l3 = l - l1 - l2
        stats = jnp.zeros((B, 128), f32)
        for n, v in enumerate((m1, m2, m3, l1, l2, l3)):
            stats = jnp.where(lane == n, v, stats)
        o_s[pl.ds(bh * 16, 16), r, LR:] = stats
        own_s[b] = new.astype(bf16).astype(f32) * wide[pl.ds(b, 1), :LR]
        p_s[b] = jnp.concatenate(p, axis=1).astype(bf16)

    def mixing(bh, r):
        b = bh * 8 + r
        p = p_s[b]
        mix = own_s[b]
        for j in range(4):
            keys = kv[place[b * 4 + j], :BP, :]
            mix = mix + jnp.dot(p[:, 128 * j : 128 * j + 128], keys, preferred_element_type=f32)
        o_s[pl.ds(bh * 16, 16), r, :LR] = mix

    def halves(step):
        def both(bh, _):
            for r in range(8):
                step(bh, r)
            return 0

        lax.fori_loop(0, 2, both, 0)

    halves(softmax)
    halves(mixing)

    def pour(i, _):
        out[i] = o_s[i].astype(bf16)
        return 0

    lax.fori_loop(0, 32, pour, 0, unroll=8)


def attend_call(idx, table, lengths, q, wide, key_up, bufs):
    return pl.pallas_call(
        attend_kernel,
        out_shape=jax.ShapeDtypeStruct((32, 8, LR + 128), bf16),
        in_specs=[spec(SM)] * 3 + [spec(VM)] * 2 + [spec(HB)] * 17,
        out_specs=spec(VM),
        scratch_shapes=[
            pltpu.VMEM((LR, 2048), bf16),
            pltpu.VMEM((64, BP + 16, LR), bf16),
            pltpu.VMEM((B, B, LR + 128), f32),
            pltpu.VMEM((64, B, BP), f32),
            pltpu.VMEM((B, B, 4 * BP), bf16),
            pltpu.VMEM((32, 8, LR + 128), f32),
            pltpu.VMEM((B, B, LR), f32),
            pltpu.SMEM((64,), jnp.int32),
            pltpu.SMEM((64,), jnp.int32),
            pltpu.SemaphoreType.DMA,
            pltpu.SemaphoreType.DMA((4,)),
        ],
        name="attend",
    )(idx, table, lengths, q, wide, key_up, *bufs)


def value_kernel(idx, parts, value_up, out, vals, sem):
    h = lax.rem(idx[0], 16)
    cp = pltpu.make_async_copy(value_up.at[:, pl.ds(pl.multiple_of(h * VD, VD), VD)], vals, sem)
    cp.start()
    tops, tots = [], []
    for i in range(32):
        st = parts[i, :, LR:].astype(f32)
        tops.append(st[:, 0:1] + st[:, 1:2] + st[:, 2:3])
        tots.append(st[:, 3:4] + st[:, 4:5] + st[:, 5:6])
    top = functools.reduce(jnp.maximum, tops)
    total = jnp.zeros((8, 1), f32)
    mix = jnp.zeros((8, LR), f32)
    for i in range(32):
        w = jnp.exp(tops[i] - top)
        total = total + w * tots[i]
        mix = mix + w * parts[i, :, :LR].astype(f32)
    att = (mix / total).astype(bf16)
    cp.wait()
    res = jnp.dot(att, vals[...], preferred_element_type=f32).astype(bf16)
    for i in range(32):
        out[i] = res


def value_call(idx, parts, value_up):
    return pl.pallas_call(
        value_kernel,
        out_shape=jax.ShapeDtypeStruct((32, 8, VD), bf16),
        in_specs=[spec(SM), spec(VM), spec(HB)],
        out_specs=spec(VM),
        scratch_shapes=[pltpu.VMEM((LR, VD), bf16), pltpu.SemaphoreType.DMA],
        name="value",
    )(idx, parts, value_up)


UP = [(i, (i + 1) % 4) for i in range(4)]
DOWN = [(i, (i + 3) % 4) for i in range(4)]
SWAP = [(0, 1), (1, 0)]


def shift(value, axis, pairs):
    return lax.ppermute(value, axis, pairs)


def body(hidden_in, united_down, q_gain, kv_gain, q_up, key_up, value_up, store, rope_pool, lengths, table):
    s = lax.axis_index(S)
    idx = jnp.stack([s, lax.axis_index("y"), lax.axis_index("c")]).astype(jnp.int32)
    lane = jnp.arange(128)
    freq = 10000.0 ** (-2.0 * (lane % 32).astype(f32) / ROT)
    angles = lengths.astype(f32)[:, None] * freq
    cos, sin = jnp.cos(angles), jnp.sin(angles)
    sin = jnp.where(lane % ROT < ROT // 2, -sin, sin)
    half_a, half_b = pack_call(store, rope_pool)
    up_a = shift(half_a, "y", UP)
    down_b = shift(half_b, "y", DOWN)
    q_tile = exchange(tiles_call(q_up), S)
    cols = united_call(hidden_in, united_down)
    spread = [cols] + [shift(cols, "y", [((i + d) % 4, i) for i in range(4)]) for d in (1, 2, 3)]
    parts = []
    for d in range(4):
        parts += [spread[d], shift(spread[d], "c", SWAP)]
    up_b = shift(half_b, "y", UP)
    down_a = shift(half_a, "y", DOWN)
    far_a = shift(up_a, "y", UP)
    far_b = shift(down_b, "y", DOWN)
    near = {0: (half_a, half_b), 3: (up_a, up_b), 1: (down_a, down_b), 2: (far_a, far_b)}
    bufs = []
    for dy, dc, h in ORDER:
        bufs.append(near[dy][h] if dc == 0 else shift(near[dy][h], "c", SWAP))
    entry, wide, q_copies = query_call(idx, parts, q_gain[None], kv_gain[None], cos, sin, q_tile)
    q_all = exchange(q_copies, S)
    mixed = attend_call(idx, table.reshape(-1), lengths, q_all, wide, key_up, bufs)
    spans = exchange(mixed, S)
    res = value_call(idx, spans, value_up)
    res = exchange(res, S)
    res = res.reshape(2, 16, 8, VD).transpose(0, 2, 1, 3).reshape(B, 16 * VD)
    return res, entry


def solution(mesh):
    split = Mesh(mesh.devices.reshape(8, 4, 4, 2), ("z", "x", "y", "c"))
    return jax.shard_map(
        body,
        mesh=split,
        in_specs=(
            P(),
            P(None, T),
            P(),
            P(),
            P(S, T),
            P(None, T),
            P(None, T),
            P(S + T, None, None),
            P(S + T, None, None),
            P(),
            P(None, S),
        ),
        out_specs=(P(None, T), P()),
        check_vma=False,
    )
```

```python
import functools

import jax
import jax.numpy as jnp
from jax import lax
from jax.experimental import pallas as pl
from jax.experimental.pallas import tpu as pltpu
from jax.sharding import Mesh
from jax.sharding import PartitionSpec as P


D = 5120
QR = 1536
LR = 512
ROT = 64
VD = 128
B = 16
BP = 128
QH = 192
SCALE = QH ** (-0.5)
FLOOR = -1e30
S = ("z", "x")
T = ("y", "c")
bf16 = jnp.bfloat16
f32 = jnp.float32
VM = pltpu.MemorySpace.VMEM
SM = pltpu.MemorySpace.SMEM
HB = pltpu.MemorySpace.HBM


def spec(space):
    return pl.BlockSpec(memory_space=space)


def here(*values):
    return tuple(pltpu.with_memory_space_constraint(v, VM) for v in values)


def exchange(pieces, axes):
    return lax.all_to_all(pieces, axes, split_axis=0, concat_axis=0, tiled=True)


UK = 5


def united_kernel(hid, wt, out, wbuf, wsem):
    step = D // UK
    copies = []
    for k in range(UK):
        cp = pltpu.make_async_copy(wt.at[:, pl.ds(k * step, step)], wbuf.at[k], wsem.at[k])
        cp.start()
        copies.append(cp)
    acc = jnp.zeros(out.shape, f32)
    for k in range(UK):
        copies[k].wait()
        acc = acc + lax.dot_general(
            hid[:, k * step : (k + 1) * step],
            wbuf[k],
            (((1,), (1,)), ((), ())),
            preferred_element_type=f32,
        )
    out[...] = acc.astype(bf16)


def united_call(hid, down):
    cols = down.shape[1]
    return pl.pallas_call(
        united_kernel,
        out_shape=pltpu.VMEM((B, cols), bf16),
        in_specs=[spec(VM), spec(HB)],
        out_specs=spec(VM),
        scratch_shapes=[pltpu.VMEM((UK, cols, D // UK), bf16), pltpu.SemaphoreType.DMA((UK,))],
        name="united",
    )(*here(hid), down.T)


def pack_kernel(lat, rope, q_up, pack_a, pack_b, out, cache, ropes, wide_q, sem):
    fetch_q = pltpu.make_async_copy(q_up, wide_q, sem.at[5])
    fetch_q.start()
    fetch_rope = pltpu.make_async_copy(rope, ropes, sem.at[0])
    fetch_rope.start()
    fetch = []
    for h in range(2):
        cp = pltpu.make_async_copy(lat.at[pl.ds(4 * h, 4)], cache.at[pl.ds(4 * h, 4), pl.ds(0, BP), :], sem.at[1 + h])
        cp.start()
        fetch.append(cp)
    fetch_q.wait()
    for k in range(32):
        j = k % 24
        out[k] = wide_q[:, 128 * j : 128 * j + 128]
    fetch_rope.wait()
    for n in range(8):
        for g in range(4):
            cache[n, BP:, 128 * g : 128 * g + 128] = ropes[n, 16 * g : 16 * g + 16, :]
    stores = []
    for h, dst in enumerate((pack_a, pack_b)):
        fetch[h].wait()
        st = pltpu.make_async_copy(cache.at[pl.ds(4 * h, 4)], dst, sem.at[3 + h])
        st.start()
        stores.append(st)
    for st in stores:
        st.wait()


def pack_call(lat, rope, q_up):
    half = jax.ShapeDtypeStruct((4, BP + 16, LR), bf16)
    return pl.pallas_call(
        pack_kernel,
        out_shape=(half, half, pltpu.VMEM((32, 48, 128), bf16)),
        in_specs=[spec(HB)] * 3,
        out_specs=(spec(HB), spec(HB), spec(VM)),
        scratch_shapes=[
            pltpu.VMEM((8, BP + 16, LR), bf16),
            pltpu.VMEM((8, ROT, BP), bf16),
            pltpu.VMEM((48, 3072), bf16),
            pltpu.SemaphoreType.DMA((6,)),
        ],
        name="pack",
    )(lat, rope, q_up)


def place_of():
    return lax.axis_index("z") * 4 + lax.axis_index("x"), lax.axis_index("y"), lax.axis_index("c")


def swapped(x):
    lane = lax.broadcasted_iota(jnp.int32, x.shape, 1)
    return jnp.where(lane % ROT < ROT // 2, pltpu.roll(x, 96, 1), pltpu.roll(x, 32, 1))


def query_kernel(*refs):
    pieces, (q_gain, kv_gain, cos, sin_part, weights, entry, wide, out, parts) = refs[:8], refs[8:]
    s, y, c = place_of()
    width = 264
    for i in range(8):
        cp = c if i % 2 == 0 else 1 - c
        parts[lax.rem(y + i // 2, 4) * 2 + cp] = pieces[i][...].astype(f32)
    tiles = [None] * 17
    for i in range(8):
        piece = parts[i]
        piece = jnp.concatenate([piece, jnp.zeros((B, 384 - width), f32)], axis=1)
        if i:
            piece = pltpu.roll(piece, 8 * i, 1)
        for k in range(3):
            part = piece[:, 128 * k : 128 * k + 128]
            if 2 * i + k < 17:
                tiles[2 * i + k] = part if tiles[2 * i + k] is None else tiles[2 * i + k] + part
    u = jnp.concatenate(tiles, axis=1)
    uq = u[:, :QR]
    ul = u[:, QR : QR + LR]
    ur = u[:, QR + LR : QR + LR + 128]
    rq = lax.rsqrt(jnp.sum(uq * uq, axis=1, keepdims=True) / QR + 1.0)
    rl = lax.rsqrt(jnp.sum(ul * ul, axis=1, keepdims=True) / LR + 1.0)
    ql = (uq * rq * q_gain[...].reshape(1, QR)).astype(bf16)
    q = jnp.dot(ql, weights[...].reshape(QR, 128), preferred_element_type=f32)
    lane = lax.broadcasted_iota(jnp.int32, (B, 128), 1)
    sin = jnp.where(lane % ROT < ROT // 2, -sin_part[...], sin_part[...])
    kind = lax.rem(s, 3)
    in_rope = ((lane < ROT) & (kind == 1)) | ((lane >= ROT) & (kind == 2))
    res = jnp.where(in_rope, (q * cos[...] + swapped(q) * sin) * SCALE, q).astype(bf16)
    for i in range(32):
        out[i] = res
    lat = (ul * rl * kv_gain[...].reshape(1, LR)).astype(bf16)
    rot = jnp.where(lane < ROT, ur * cos[...] + swapped(ur) * sin, 0.0).astype(bf16)
    entry[:, :LR] = lat
    entry[:, LR:] = rot[:, :ROT]
    wide[:, :LR] = lat.astype(f32)
    wide[:, LR:] = rot.astype(f32)


def query_call(parts, q_gain, kv_gain, cos, sin, weights):
    return pl.pallas_call(
        query_kernel,
        out_shape=(
            jax.ShapeDtypeStruct((B, LR + ROT), bf16),
            pltpu.VMEM((B, LR + 128), f32),
            pltpu.VMEM((32, B, 128), bf16),
        ),
        in_specs=[spec(VM)] * 13,
        out_specs=(spec(VM),) * 3,
        scratch_shapes=[pltpu.VMEM((8, B, 264), f32)],
        name="query",
    )(*here(*parts, q_gain, kv_gain, cos, sin, weights))


def keys_kernel(src, dst, sem):
    cp = pltpu.make_async_copy(src, dst, sem)
    cp.start()
    cp.wait()


def keys_call(key_up):
    return pl.pallas_call(
        keys_kernel,
        out_shape=pltpu.VMEM(key_up.shape, bf16),
        in_specs=[spec(HB)],
        out_specs=spec(VM),
        scratch_shapes=[pltpu.SemaphoreType.DMA],
        name="keys",
    )(key_up)


ORDER = [(dy, dc, h) for dy in (0, 3, 1, 2) for dc in (0, 1) for h in (0, 1)]


def attend_kernel(table, lengths, q, wide, keys_v, *rest):
    bufs, out = rest[:16], rest[16]
    kv, q_s, s_s, p_s, o_s, own_s, inv, place, sem = rest[17:]
    s, y, c = place_of()
    for i in range(16):
        pltpu.make_async_copy(bufs[i], kv.at[pl.ds(4 * i, 4)], sem.at[i // 4]).start()

    def fill(e, _):
        inv[table[e // 4, e % 4] - s * 64] = e
        return 0

    lax.fori_loop(0, 64, fill, 0, unroll=8)
    lane = lax.broadcasted_iota(jnp.int32, (B, BP), 1)
    for p in range(8):
        t0 = q[3 * p].astype(f32)
        t1 = pltpu.roll(q[3 * p + 1].astype(f32), 64, 1)
        t2 = pltpu.roll(q[3 * p + 2].astype(f32), 64, 1)
        r0 = q[3 * p + 1].astype(f32)
        nopes = (t0, jnp.where(lane < ROT, t1, t2))
        ropes = (jnp.where(lane < ROT, r0, 0.0), jnp.where(lane < ROT, t2, 0.0))
        for j in range(2):
            h = 2 * p + j
            lat = lax.dot_general(
                nopes[j].astype(bf16),
                keys_v[:, 128 * h : 128 * h + 128],
                (((1,), (1,)), ((), ())),
                preferred_element_type=f32,
            )
            q_s[:, h, :LR] = (lat * SCALE).astype(bf16).astype(f32)
            q_s[:, h, LR:] = ropes[j]

    def scores(g, _):
        here = kv.at[pl.ds(16 * g, 16)]
        pltpu.make_async_copy(here, here, sem.at[g]).wait()
        dy = jnp.where(g == 0, 0, jnp.where(g == 1, 3, jnp.where(g == 2, 1, 2)))
        ys = lax.rem(y + dy, 4)
        for dc in range(2):
            cs = c if dc == 0 else 1 - c
            first = (ys * 2 + cs) * 8
            for k in range(8):
                at = g * 16 + dc * 8 + k
                e = inv[first + k]
                place[e] = at
                qb = q_s[e // 4].astype(bf16)
                keys = kv[at, :BP, :]
                rope = jnp.concatenate([kv[at, BP:, 128 * n : 128 * n + 128] for n in range(4)], axis=0)
                sc = lax.dot_general(qb[:, :LR], keys, (((1,), (1,)), ((), ())), preferred_element_type=f32)
                s_s[e] = sc + jnp.dot(qb[:, LR : LR + ROT], rope, preferred_element_type=f32)
        return 0

    lax.fori_loop(0, 4, scores, 0)

    def softmax(bh, r):
        b = bh * 8 + r
        room = lengths[b] - s * (4 * BP)
        new = jnp.sum(q_s[b] * wide[pl.ds(b, 1), :], axis=1, keepdims=True)
        mine = jnp.full((B, 1), s, jnp.int32) == 0
        live = [lane < room - j * BP for j in range(4)]
        sc = [jnp.where(live[j], s_s[b * 4 + j], FLOOR) for j in range(4)]
        m = jnp.maximum(jnp.maximum(sc[0], sc[1]), jnp.maximum(sc[2], sc[3]))
        m = jnp.maximum(jnp.max(m, axis=1, keepdims=True), jnp.where(mine, new, FLOOR))
        p = [jnp.where(live[j], jnp.exp(sc[j] - m), 0.0) for j in range(4)]
        new = jnp.where(mine, jnp.exp(new - m), 0.0)
        l = jnp.sum((p[0] + p[1]) + (p[2] + p[3]), axis=1, keepdims=True) + new
        m1 = m.astype(bf16).astype(f32)
        m2 = (m - m1).astype(bf16).astype(f32)
        m3 = m - m1 - m2
        l1 = l.astype(bf16).astype(f32)
        l2 = (l - l1).astype(bf16).astype(f32)
        l3 = l - l1 - l2
        stats = jnp.zeros((B, 128), f32)
        for n, v in enumerate((m1, m2, m3, l1, l2, l3)):
            stats = jnp.where(lane == n, v, stats)
        o_s[pl.ds(bh * 16, 16), r, LR:] = stats
        own_s[b] = new.astype(bf16).astype(f32) * wide[pl.ds(b, 1), :LR]
        p_s[b] = jnp.concatenate(p, axis=1).astype(bf16)

    def mixing(bh, r):
        b = bh * 8 + r
        p = p_s[b]
        mix = own_s[b]
        for j in range(4):
            keys = kv[place[b * 4 + j], :BP, :]
            mix = mix + jnp.dot(p[:, 128 * j : 128 * j + 128], keys, preferred_element_type=f32)
        o_s[pl.ds(bh * 16, 16), r, :LR] = mix

    def halves(step):
        def both(bh, _):
            for r in range(8):
                step(bh, r)
            return 0

        lax.fori_loop(0, 2, both, 0)

    halves(softmax)
    halves(mixing)

    def pour(i, _):
        out[i] = o_s[i].astype(bf16)
        return 0

    lax.fori_loop(0, 32, pour, 0, unroll=8)


def attend_call(table, lengths, q, wide, key_up, bufs):
    return pl.pallas_call(
        attend_kernel,
        out_shape=pltpu.VMEM((32, 8, LR + 128), bf16),
        in_specs=[spec(SM)] * 2 + [spec(VM)] * 3 + [spec(HB)] * 16,
        out_specs=spec(VM),
        scratch_shapes=[
            pltpu.VMEM((64, BP + 16, LR), bf16),
            pltpu.VMEM((B, B, LR + 128), f32),
            pltpu.VMEM((64, B, BP), f32),
            pltpu.VMEM((B, B, 4 * BP), bf16),
            pltpu.VMEM((32, 8, LR + 128), f32),
            pltpu.VMEM((B, B, LR), f32),
            pltpu.SMEM((64,), jnp.int32),
            pltpu.SMEM((64,), jnp.int32),
            pltpu.SemaphoreType.DMA((4,)),
        ],
        name="attend",
    )(table, lengths, *here(q, wide, key_up), *bufs)


def value_kernel(parts, value_up, out, vals, sem):
    h = lax.rem(place_of()[0], 16)
    cp = pltpu.make_async_copy(value_up.at[:, pl.ds(pl.multiple_of(h * VD, VD), VD)], vals, sem)
    cp.start()
    tops, tots = [], []
    for i in range(32):
        st = parts[i, :, LR:].astype(f32)
        tops.append(st[:, 0:1] + st[:, 1:2] + st[:, 2:3])
        tots.append(st[:, 3:4] + st[:, 4:5] + st[:, 5:6])
    top = functools.reduce(jnp.maximum, tops)
    total = jnp.zeros((8, 1), f32)
    mix = jnp.zeros((8, LR), f32)
    for i in range(32):
        w = jnp.exp(tops[i] - top)
        total = total + w * tots[i]
        mix = mix + w * parts[i, :, :LR].astype(f32)
    att = (mix / total).astype(bf16)
    cp.wait()
    res = jnp.dot(att, vals[...], preferred_element_type=f32).astype(bf16)
    for i in range(32):
        out[i] = res


def value_call(parts, value_up):
    return pl.pallas_call(
        value_kernel,
        out_shape=pltpu.VMEM((32, 8, VD), bf16),
        in_specs=[spec(VM), spec(HB)],
        out_specs=spec(VM),
        scratch_shapes=[pltpu.VMEM((LR, VD), bf16), pltpu.SemaphoreType.DMA],
        name="value",
    )(*here(parts), value_up)


UP = [(i, (i + 1) % 4) for i in range(4)]
DOWN = [(i, (i + 3) % 4) for i in range(4)]
SWAP = [(0, 1), (1, 0)]


def shift(value, axis, pairs):
    return lax.ppermute(value, axis, pairs)


def body(hidden_in, united_down, q_gain, kv_gain, q_up, key_up, value_up, store, rope_pool, lengths, table):
    lane = jnp.arange(128)
    freq = 10000.0 ** (-2.0 * (lane % 32).astype(f32) / ROT)
    angles = lengths.astype(f32)[:, None] * freq
    cos, sin = jnp.cos(angles), jnp.sin(angles)
    half_a, half_b, tiles = pack_call(store, rope_pool, q_up)
    up_a = shift(half_a, "y", UP)
    down_b = shift(half_b, "y", DOWN)
    q_tile = exchange(tiles, S)
    cols = united_call(hidden_in, united_down)
    spread = [cols] + [shift(cols, "y", [((i + d) % 4, i) for i in range(4)]) for d in (1, 2, 3)]
    parts = []
    for d in range(4):
        parts += [spread[d], shift(spread[d], "c", SWAP)]
    up_b = shift(half_b, "y", UP)
    down_a = shift(half_a, "y", DOWN)
    far_a = shift(up_a, "y", UP)
    far_b = shift(down_b, "y", DOWN)
    near = {0: (half_a, half_b), 3: (up_a, up_b), 1: (down_a, down_b), 2: (far_a, far_b)}
    bufs = []
    for dy, dc, h in ORDER:
        bufs.append(near[dy][h] if dc == 0 else shift(near[dy][h], "c", SWAP))
    entry, wide, q_copies = query_call(parts, q_gain, kv_gain, cos, sin, q_tile)
    q_all = exchange(q_copies, S)
    mixed = attend_call(table, lengths, q_all, wide, keys_call(key_up), bufs)
    spans = exchange(mixed, S)
    res = value_call(spans, value_up)
    res = exchange(res, S)
    res = res.reshape(2, 16, 8, VD).transpose(0, 2, 1, 3).reshape(B, 16 * VD)
    return res, entry


def solution(mesh):
    split = Mesh(mesh.devices.reshape(8, 4, 4, 2), ("z", "x", "y", "c"))
    return jax.shard_map(
        body,
        mesh=split,
        in_specs=(
            P(),
            P(None, T),
            P(),
            P(),
            P(S, T),
            P(None, T),
            P(None, T),
            P(S + T, None, None),
            P(S + T, None, None),
            P(),
            P(None, S),
        ),
        out_specs=(P(None, T), P()),
        check_vma=False,
    )
```

```python
import functools

import jax
import jax.numpy as jnp
from jax import lax
from jax.experimental import pallas as pl
from jax.experimental.pallas import tpu as pltpu
from jax.sharding import Mesh
from jax.sharding import PartitionSpec as P


D = 5120
QR = 1536
LR = 512
ROT = 64
VD = 128
B = 16
BP = 128
QH = 192
SCALE = QH ** (-0.5)
FLOOR = -1e30
S = ("z", "x")
T = ("y", "c")
bf16 = jnp.bfloat16
f32 = jnp.float32
VM = pltpu.MemorySpace.VMEM
SM = pltpu.MemorySpace.SMEM
HB = pltpu.MemorySpace.HBM


def spec(space):
    return pl.BlockSpec(memory_space=space)


def here(*values):
    return tuple(pltpu.with_memory_space_constraint(v, VM) for v in values)


def exchange(pieces, axes):
    return lax.all_to_all(pieces, axes, split_axis=0, concat_axis=0, tiled=True)


UK = 5


def united_kernel(hid_hbm, wt, out, hid, wbuf, hsem, wsem):
    step = D // UK
    copies = []
    fetch = pltpu.make_async_copy(hid_hbm, hid, hsem)
    fetch.start()
    for k in range(UK):
        cp = pltpu.make_async_copy(wt.at[:, pl.ds(k * step, step)], wbuf.at[k], wsem.at[k])
        cp.start()
        copies.append(cp)
    acc = jnp.zeros(out.shape, f32)
    fetch.wait()
    for k in range(UK):
        copies[k].wait()
        acc = acc + lax.dot_general(
            hid[:, k * step : (k + 1) * step],
            wbuf[k],
            (((1,), (1,)), ((), ())),
            preferred_element_type=f32,
        )
    out[...] = acc.astype(bf16)


def united_call(hid, down):
    cols = down.shape[1]
    return pl.pallas_call(
        united_kernel,
        out_shape=pltpu.VMEM((B, cols), bf16),
        in_specs=[spec(HB), spec(HB)],
        out_specs=spec(VM),
        scratch_shapes=[
            pltpu.VMEM((B, D), bf16),
            pltpu.VMEM((UK, cols, D // UK), bf16),
            pltpu.SemaphoreType.DMA,
            pltpu.SemaphoreType.DMA((UK,)),
        ],
        name="united",
    )(hid, down.T)


def tiles_kernel(q_up, out):
    for k in range(32):
        j = k % 24
        out[k] = q_up[:, 128 * j : 128 * j + 128]


def tiles_call(q_up):
    return pl.pallas_call(
        tiles_kernel,
        out_shape=pltpu.VMEM((32, 48, 128), bf16),
        in_specs=[spec(VM)],
        out_specs=spec(VM),
        name="tiles",
    )(*here(q_up))


def pack_kernel(lat, rope, pack_a, pack_b, ropes, sem):
    fetch_rope = pltpu.make_async_copy(rope, ropes, sem.at[0])
    fetch_rope.start()
    fetch = []
    for h, dst in enumerate((pack_a, pack_b)):
        cp = pltpu.make_async_copy(lat.at[pl.ds(4 * h, 4)], dst.at[:, pl.ds(0, BP), :], sem.at[1 + h])
        cp.start()
        fetch.append(cp)
    fetch_rope.wait()
    for n in range(8):
        dst = (pack_a, pack_b)[n // 4]
        for g in range(4):
            dst[n % 4, BP:, 128 * g : 128 * g + 128] = ropes[n, 16 * g : 16 * g + 16, :]
    for cp in fetch:
        cp.wait()


def pack_call(lat, rope):
    half = pltpu.VMEM((4, BP + 16, LR), bf16)
    return pl.pallas_call(
        pack_kernel,
        out_shape=(half, half),
        in_specs=[spec(HB)] * 2,
        out_specs=(spec(VM), spec(VM)),
        scratch_shapes=[pltpu.VMEM((8, ROT, BP), bf16), pltpu.SemaphoreType.DMA((3,))],
        name="pack",
    )(lat, rope)


def place_of():
    return lax.axis_index("z") * 4 + lax.axis_index("x"), lax.axis_index("y"), lax.axis_index("c")


def swapped(x):
    lane = lax.broadcasted_iota(jnp.int32, x.shape, 1)
    return jnp.where(lane % ROT < ROT // 2, pltpu.roll(x, 96, 1), pltpu.roll(x, 32, 1))


def query_kernel(*refs):
    pieces, (q_gain, kv_gain, cos, sin_part, weights, entry, wide, out, parts) = refs[:8], refs[8:]
    s, y, c = place_of()
    width = 264
    for i in range(8):
        cp = c if i % 2 == 0 else 1 - c
        parts[lax.rem(y + i // 2, 4) * 2 + cp] = pieces[i][...].astype(f32)
    tiles = [None] * 17
    for i in range(8):
        piece = parts[i]
        piece = jnp.concatenate([piece, jnp.zeros((B, 384 - width), f32)], axis=1)
        if i:
            piece = pltpu.roll(piece, 8 * i, 1)
        for k in range(3):
            part = piece[:, 128 * k : 128 * k + 128]
            if 2 * i + k < 17:
                tiles[2 * i + k] = part if tiles[2 * i + k] is None else tiles[2 * i + k] + part
    u = jnp.concatenate(tiles, axis=1)
    uq = u[:, :QR]
    ul = u[:, QR : QR + LR]
    ur = u[:, QR + LR : QR + LR + 128]
    rq = lax.rsqrt(jnp.sum(uq * uq, axis=1, keepdims=True) / QR + 1.0)
    rl = lax.rsqrt(jnp.sum(ul * ul, axis=1, keepdims=True) / LR + 1.0)
    ql = (uq * rq * q_gain[...].reshape(1, QR)).astype(bf16)
    q = jnp.dot(ql, weights[...].reshape(QR, 128), preferred_element_type=f32)
    lane = lax.broadcasted_iota(jnp.int32, (B, 128), 1)
    sin = jnp.where(lane % ROT < ROT // 2, -sin_part[...], sin_part[...])
    kind = lax.rem(s, 3)
    in_rope = ((lane < ROT) & (kind == 1)) | ((lane >= ROT) & (kind == 2))
    res = jnp.where(in_rope, (q * cos[...] + swapped(q) * sin) * SCALE, q).astype(bf16)
    for i in range(32):
        out[i] = res
    lat = (ul * rl * kv_gain[...].reshape(1, LR)).astype(bf16)
    rot = jnp.where(lane < ROT, ur * cos[...] + swapped(ur) * sin, 0.0).astype(bf16)
    entry[:, :LR] = lat
    entry[:, LR:] = rot[:, :ROT]
    wide[:, :LR] = lat.astype(f32)
    wide[:, LR:] = rot.astype(f32)


def query_call(parts, q_gain, kv_gain, cos, sin, weights):
    return pl.pallas_call(
        query_kernel,
        out_shape=(
            jax.ShapeDtypeStruct((B, LR + ROT), bf16),
            pltpu.VMEM((B, LR + 128), f32),
            pltpu.VMEM((32, B, 128), bf16),
        ),
        in_specs=[spec(VM)] * 13,
        out_specs=(spec(VM),) * 3,
        scratch_shapes=[pltpu.VMEM((8, B, 264), f32)],
        name="query",
    )(*here(*parts, q_gain, kv_gain, cos, sin, weights))


def keys_kernel(table, src, dst, inv, sem):
    cp = pltpu.make_async_copy(src, dst, sem)
    cp.start()
    base = place_of()[0] * 64

    def fill(b, _):
        for j in range(4):
            inv[table[b, j] - base] = b * 4 + j
        return 0

    lax.fori_loop(0, B, fill, 0, unroll=4)
    cp.wait()


def keys_call(table, key_up):
    return pl.pallas_call(
        keys_kernel,
        out_shape=(pltpu.VMEM(key_up.shape, bf16), jax.ShapeDtypeStruct((64,), jnp.int32)),
        in_specs=[spec(SM), spec(HB)],
        out_specs=(spec(VM), spec(SM)),
        scratch_shapes=[pltpu.SemaphoreType.DMA],
        name="keys",
    )(table, key_up)


ORDER = [(dy, dc, h) for dy in (0, 3, 1, 2) for dc in (0, 1) for h in (0, 1)]


def attend_kernel(inv, lengths, q, wide, keys_v, *rest):
    bufs, out = rest[:16], rest[16]
    kv, q_s, s_s, p_s, o_s, own_s, place, sem = rest[17:]
    s, y, c = place_of()
    for i in range(16):
        pltpu.make_async_copy(bufs[i], kv.at[pl.ds(4 * i, 4)], sem.at[i // 4]).start()

    lane = lax.broadcasted_iota(jnp.int32, (B, BP), 1)
    for p in range(8):
        t0 = q[3 * p].astype(f32)
        t1 = pltpu.roll(q[3 * p + 1].astype(f32), 64, 1)
        t2 = pltpu.roll(q[3 * p + 2].astype(f32), 64, 1)
        r0 = q[3 * p + 1].astype(f32)
        nopes = (t0, jnp.where(lane < ROT, t1, t2))
        ropes = (jnp.where(lane < ROT, r0, 0.0), jnp.where(lane < ROT, t2, 0.0))
        for j in range(2):
            h = 2 * p + j
            lat = lax.dot_general(
                nopes[j].astype(bf16),
                keys_v[:, 128 * h : 128 * h + 128],
                (((1,), (1,)), ((), ())),
                preferred_element_type=f32,
            )
            q_s[:, h, :LR] = (lat * SCALE).astype(bf16).astype(f32)
            q_s[:, h, LR:] = ropes[j]

    def scores(g, _):
        here = kv.at[pl.ds(16 * g, 16)]
        pltpu.make_async_copy(here, here, sem.at[g]).wait()
        dy = jnp.where(g == 0, 0, jnp.where(g == 1, 3, jnp.where(g == 2, 1, 2)))
        ys = lax.rem(y + dy, 4)
        for dc in range(2):
            cs = c if dc == 0 else 1 - c
            first = (ys * 2 + cs) * 8
            for k in range(8):
                at = g * 16 + dc * 8 + k
                e = inv[first + k]
                place[e] = at
                qb = q_s[e // 4].astype(bf16)
                keys = kv[at, :BP, :]
                rope = jnp.concatenate([kv[at, BP:, 128 * n : 128 * n + 128] for n in range(4)], axis=0)
                sc = lax.dot_general(qb[:, :LR], keys, (((1,), (1,)), ((), ())), preferred_element_type=f32)
                s_s[e] = sc + jnp.dot(qb[:, LR : LR + ROT], rope, preferred_element_type=f32)
        return 0

    lax.fori_loop(0, 4, scores, 0)

    def softmax(bh, r):
        b = bh * 8 + r
        room = lengths[b] - s * (4 * BP)
        new = jnp.sum(q_s[b] * wide[pl.ds(b, 1), :], axis=1, keepdims=True)
        mine = jnp.full((B, 1), s, jnp.int32) == 0
        live = [lane < room - j * BP for j in range(4)]
        sc = [jnp.where(live[j], s_s[b * 4 + j], FLOOR) for j in range(4)]
        m = jnp.maximum(jnp.maximum(sc[0], sc[1]), jnp.maximum(sc[2], sc[3]))
        m = jnp.maximum(jnp.max(m, axis=1, keepdims=True), jnp.where(mine, new, FLOOR))
        p = [jnp.where(live[j], jnp.exp(sc[j] - m), 0.0) for j in range(4)]
        new = jnp.where(mine, jnp.exp(new - m), 0.0)
        l = jnp.sum((p[0] + p[1]) + (p[2] + p[3]), axis=1, keepdims=True) + new
        m1 = m.astype(bf16).astype(f32)
        m2 = (m - m1).astype(bf16).astype(f32)
        m3 = m - m1 - m2
        l1 = l.astype(bf16).astype(f32)
        l2 = (l - l1).astype(bf16).astype(f32)
        l3 = l - l1 - l2
        stats = jnp.zeros((B, 128), f32)
        for n, v in enumerate((m1, m2, m3, l1, l2, l3)):
            stats = jnp.where(lane == n, v, stats)
        o_s[pl.ds(bh * 16, 16), r, LR:] = stats
        own_s[b] = new.astype(bf16).astype(f32) * wide[pl.ds(b, 1), :LR]
        p_s[b] = jnp.concatenate(p, axis=1).astype(bf16)

    def mixing(bh, r):
        b = bh * 8 + r
        p = p_s[b]
        mix = own_s[b]
        for j in range(4):
            keys = kv[place[b * 4 + j], :BP, :]
            mix = mix + jnp.dot(p[:, 128 * j : 128 * j + 128], keys, preferred_element_type=f32)
        o_s[pl.ds(bh * 16, 16), r, :LR] = mix

    def halves(step):
        def both(bh, _):
            for r in range(8):
                step(bh, r)
            return 0

        lax.fori_loop(0, 2, both, 0)

    halves(softmax)
    halves(mixing)

    def pour(i, _):
        out[i] = o_s[i].astype(bf16)
        return 0

    lax.fori_loop(0, 32, pour, 0, unroll=8)


def attend_call(inv, lengths, q, wide, keys, bufs):
    return pl.pallas_call(
        attend_kernel,
        out_shape=pltpu.VMEM((32, 8, LR + 128), bf16),
        in_specs=[spec(SM)] * 2 + [spec(VM)] * 3 + [spec(HB)] * 16,
        out_specs=spec(VM),
        scratch_shapes=[
            pltpu.VMEM((64, BP + 16, LR), bf16),
            pltpu.VMEM((B, B, LR + 128), f32),
            pltpu.VMEM((64, B, BP), f32),
            pltpu.VMEM((B, B, 4 * BP), bf16),
            pltpu.VMEM((32, 8, LR + 128), f32),
            pltpu.VMEM((B, B, LR), f32),
            pltpu.SMEM((64,), jnp.int32),
            pltpu.SemaphoreType.DMA((4,)),
        ],
        name="attend",
    )(inv, lengths, *here(q, wide, keys), *bufs)


def value_kernel(parts, value_up, out, vals, sem):
    h = lax.rem(place_of()[0], 16)
    cp = pltpu.make_async_copy(value_up.at[:, pl.ds(pl.multiple_of(h * VD, VD), VD)], vals, sem)
    cp.start()
    tops, tots = [], []
    for i in range(32):
        st = parts[i, :, LR:].astype(f32)
        tops.append(st[:, 0:1] + st[:, 1:2] + st[:, 2:3])
        tots.append(st[:, 3:4] + st[:, 4:5] + st[:, 5:6])
    top = functools.reduce(jnp.maximum, tops)
    total = jnp.zeros((8, 1), f32)
    mix = jnp.zeros((8, LR), f32)
    for i in range(32):
        w = jnp.exp(tops[i] - top)
        total = total + w * tots[i]
        mix = mix + w * parts[i, :, :LR].astype(f32)
    att = (mix / total).astype(bf16)
    cp.wait()
    res = jnp.dot(att, vals[...], preferred_element_type=f32).astype(bf16)
    for i in range(32):
        out[i] = res


def value_call(parts, value_up):
    return pl.pallas_call(
        value_kernel,
        out_shape=pltpu.VMEM((32, 8, VD), bf16),
        in_specs=[spec(VM), spec(HB)],
        out_specs=spec(VM),
        scratch_shapes=[pltpu.VMEM((LR, VD), bf16), pltpu.SemaphoreType.DMA],
        name="value",
    )(*here(parts), value_up)


UP = [(i, (i + 1) % 4) for i in range(4)]
DOWN = [(i, (i + 3) % 4) for i in range(4)]
SWAP = [(0, 1), (1, 0)]


def shift(value, axis, pairs):
    return lax.ppermute(value, axis, pairs)


def body(hidden_in, united_down, q_gain, kv_gain, q_up, key_up, value_up, store, rope_pool, lengths, table):
    lane = jnp.arange(128)
    freq = 10000.0 ** (-2.0 * (lane % 32).astype(f32) / ROT)
    angles = lengths.astype(f32)[:, None] * freq
    cos, sin = jnp.cos(angles), jnp.sin(angles)
    half_a, half_b = pack_call(store, rope_pool)
    up_a = shift(half_a, "y", UP)
    down_b = shift(half_b, "y", DOWN)
    q_tile = exchange(tiles_call(q_up), S)
    cols = united_call(hidden_in, united_down)
    spread = [cols] + [shift(cols, "y", [((i + d) % 4, i) for i in range(4)]) for d in (1, 2, 3)]
    parts = []
    for d in range(4):
        parts += [spread[d], shift(spread[d], "c", SWAP)]
    up_b = shift(half_b, "y", UP)
    down_a = shift(half_a, "y", DOWN)
    far_a = shift(up_a, "y", UP)
    far_b = shift(down_b, "y", DOWN)
    near = {0: (half_a, half_b), 3: (up_a, up_b), 1: (down_a, down_b), 2: (far_a, far_b)}
    bufs = []
    for dy, dc, h in ORDER:
        bufs.append(near[dy][h] if dc == 0 else shift(near[dy][h], "c", SWAP))
    entry, wide, q_copies = query_call(parts, q_gain, kv_gain, cos, sin, q_tile)
    q_all = exchange(q_copies, S)
    keys, inv = keys_call(table, key_up)
    mixed = attend_call(inv, lengths, q_all, wide, keys, bufs)
    spans = exchange(mixed, S)
    res = value_call(spans, value_up)
    res = exchange(res, S)
    res = res.reshape(2, 16, 8, VD).transpose(0, 2, 1, 3).reshape(B, 16 * VD)
    return res, entry


def solution(mesh):
    split = Mesh(mesh.devices.reshape(8, 4, 4, 2), ("z", "x", "y", "c"))
    return jax.shard_map(
        body,
        mesh=split,
        in_specs=(
            P(),
            P(None, T),
            P(),
            P(),
            P(S, T),
            P(None, T),
            P(None, T),
            P(S + T, None, None),
            P(S + T, None, None),
            P(),
            P(None, S),
        ),
        out_specs=(P(None, T), P()),
        check_vma=False,
    )
```

```python
import functools

import jax
import jax.numpy as jnp
from jax import lax
from jax.experimental import pallas as pl
from jax.experimental.pallas import tpu as pltpu
from jax.sharding import Mesh
from jax.sharding import PartitionSpec as P


D = 5120
QR = 1536
LR = 512
ROT = 64
VD = 128
B = 16
BP = 128
QH = 192
SCALE = QH ** (-0.5)
FLOOR = -1e30
S = ("z", "x")
T = ("y", "c")
bf16 = jnp.bfloat16
f32 = jnp.float32
VM = pltpu.MemorySpace.VMEM
SM = pltpu.MemorySpace.SMEM
HB = pltpu.MemorySpace.HBM


def spec(space):
    return pl.BlockSpec(memory_space=space)


def here(*values):
    return tuple(pltpu.with_memory_space_constraint(v, VM) for v in values)


def exchange(pieces, axes):
    return lax.all_to_all(pieces, axes, split_axis=0, concat_axis=0, tiled=True)


UK = 5


def united_kernel(hid_hbm, wt, out, hid, wbuf, hsem, wsem):
    step = D // UK
    copies = []
    fetch = pltpu.make_async_copy(hid_hbm, hid, hsem)
    fetch.start()
    for k in range(UK):
        cp = pltpu.make_async_copy(wt.at[:, pl.ds(k * step, step)], wbuf.at[k], wsem.at[k])
        cp.start()
        copies.append(cp)
    acc = jnp.zeros(out.shape, f32)
    fetch.wait()
    for k in range(UK):
        copies[k].wait()
        acc = acc + lax.dot_general(
            hid[:, k * step : (k + 1) * step],
            wbuf[k],
            (((1,), (1,)), ((), ())),
            preferred_element_type=f32,
        )
    out[...] = acc.astype(bf16)


def united_call(hid, down):
    cols = down.shape[1]
    return pl.pallas_call(
        united_kernel,
        out_shape=pltpu.VMEM((B, cols), bf16),
        in_specs=[spec(HB), spec(HB)],
        out_specs=spec(VM),
        scratch_shapes=[
            pltpu.VMEM((B, D), bf16),
            pltpu.VMEM((UK, cols, D // UK), bf16),
            pltpu.SemaphoreType.DMA,
            pltpu.SemaphoreType.DMA((UK,)),
        ],
        name="united",
    )(hid, down.T)


def tiles_kernel(q_up, out):
    for k in range(32):
        j = k % 24
        out[k] = q_up[:, 128 * j : 128 * j + 128]


def tiles_call(q_up):
    return pl.pallas_call(
        tiles_kernel,
        out_shape=pltpu.VMEM((32, 48, 128), bf16),
        in_specs=[spec(VM)],
        out_specs=spec(VM),
        name="tiles",
    )(*here(q_up))


def pack_kernel(lat, rope, pack_a, pack_b, ropes, sem):
    fetch_rope = pltpu.make_async_copy(rope, ropes, sem.at[0])
    fetch_rope.start()
    fetch = []
    for h, dst in enumerate((pack_a, pack_b)):
        cp = pltpu.make_async_copy(lat.at[pl.ds(4 * h, 4)], dst.at[:, pl.ds(0, BP), :], sem.at[1 + h])
        cp.start()
        fetch.append(cp)
    fetch_rope.wait()
    for n in range(8):
        dst = (pack_a, pack_b)[n // 4]
        for g in range(4):
            dst[n % 4, BP:, 128 * g : 128 * g + 128] = ropes[n, 16 * g : 16 * g + 16, :]
    for cp in fetch:
        cp.wait()


def pack_call(lat, rope):
    half = pltpu.VMEM((4, BP + 16, LR), bf16)
    return pl.pallas_call(
        pack_kernel,
        out_shape=(half, half),
        in_specs=[spec(HB)] * 2,
        out_specs=(spec(VM), spec(VM)),
        scratch_shapes=[pltpu.VMEM((8, ROT, BP), bf16), pltpu.SemaphoreType.DMA((3,))],
        name="pack",
    )(lat, rope)


def place_of():
    return lax.axis_index("z") * 4 + lax.axis_index("x"), lax.axis_index("y"), lax.axis_index("c")


def swapped(x):
    lane = lax.broadcasted_iota(jnp.int32, x.shape, 1)
    return jnp.where(lane % ROT < ROT // 2, pltpu.roll(x, 96, 1), pltpu.roll(x, 32, 1))


def query_kernel(*refs):
    pieces, (q_gain, kv_gain, cos, sin_part, weights, entry, wide, out, parts) = refs[:8], refs[8:]
    s, y, c = place_of()
    width = 264
    for i in range(8):
        cp = c if i % 2 == 0 else 1 - c
        parts[lax.rem(y + i // 2, 4) * 2 + cp] = pieces[i][...].astype(f32)
    tiles = [None] * 17
    for i in range(8):
        piece = parts[i]
        piece = jnp.concatenate([piece, jnp.zeros((B, 384 - width), f32)], axis=1)
        if i:
            piece = pltpu.roll(piece, 8 * i, 1)
        for k in range(3):
            part = piece[:, 128 * k : 128 * k + 128]
            if 2 * i + k < 17:
                tiles[2 * i + k] = part if tiles[2 * i + k] is None else tiles[2 * i + k] + part
    u = jnp.concatenate(tiles, axis=1)
    uq = u[:, :QR]
    ul = u[:, QR : QR + LR]
    ur = u[:, QR + LR : QR + LR + 128]
    rq = lax.rsqrt(jnp.sum(uq * uq, axis=1, keepdims=True) / QR + 1.0)
    rl = lax.rsqrt(jnp.sum(ul * ul, axis=1, keepdims=True) / LR + 1.0)
    ql = (uq * rq * q_gain[...].reshape(1, QR)).astype(bf16)
    q = jnp.dot(ql, weights[...].reshape(QR, 128), preferred_element_type=f32)
    lane = lax.broadcasted_iota(jnp.int32, (B, 128), 1)
    sin = jnp.where(lane % ROT < ROT // 2, -sin_part[...], sin_part[...])
    kind = lax.rem(s, 3)
    in_rope = ((lane < ROT) & (kind == 1)) | ((lane >= ROT) & (kind == 2))
    res = jnp.where(in_rope, (q * cos[...] + swapped(q) * sin) * SCALE, q).astype(bf16)
    for i in range(32):
        out[i] = res
    lat = (ul * rl * kv_gain[...].reshape(1, LR)).astype(bf16)
    rot = jnp.where(lane < ROT, ur * cos[...] + swapped(ur) * sin, 0.0).astype(bf16)
    entry[:, :LR] = lat
    entry[:, LR:] = rot[:, :ROT]
    wide[:, :LR] = lat.astype(f32)
    wide[:, LR:] = rot.astype(f32)


def query_call(parts, q_gain, kv_gain, cos, sin, weights):
    return pl.pallas_call(
        query_kernel,
        out_shape=(
            jax.ShapeDtypeStruct((B, LR + ROT), bf16),
            pltpu.VMEM((B, LR + 128), f32),
            pltpu.VMEM((32, B, 128), bf16),
        ),
        in_specs=[spec(VM)] * 13,
        out_specs=(spec(VM),) * 3,
        scratch_shapes=[pltpu.VMEM((8, B, 264), f32)],
        name="query",
    )(*here(*parts, q_gain, kv_gain, cos, sin, weights))


def keys_kernel(table, lengths, src, dst, slots, sem):
    cp = pltpu.make_async_copy(src, dst, sem)
    cp.start()
    s = place_of()[0]

    def fill(b, _):
        slots[64 + b] = lengths[b] - s * (4 * BP)
        for j in range(4):
            slots[table[b, j] - s * 64] = b * 4 + j
        return 0

    lax.fori_loop(0, B, fill, 0, unroll=4)
    for i in range(80, 128):
        slots[i] = 0
    cp.wait()


def keys_call(table, lengths, key_up):
    return pl.pallas_call(
        keys_kernel,
        out_shape=(pltpu.VMEM(key_up.shape, bf16), jax.ShapeDtypeStruct((128,), jnp.int32)),
        in_specs=[spec(SM), spec(SM), spec(HB)],
        out_specs=(spec(VM), spec(SM)),
        scratch_shapes=[pltpu.SemaphoreType.DMA],
        name="keys",
    )(table, lengths, key_up)


ORDER = [(dy, dc, h) for dy in (0, 3, 1, 2) for dc in (0, 1) for h in (0, 1)]


def attend_kernel(slots, q, wide, keys_v, *rest):
    bufs, out = rest[:16], rest[16]
    kv, q_s, s_s, p_s, o_s, own_s, place, inv, tsem, sem = rest[17:]
    fetch = pltpu.make_async_copy(slots, inv, tsem)
    fetch.start()
    s, y, c = place_of()
    for i in range(16):
        pltpu.make_async_copy(bufs[i], kv.at[pl.ds(4 * i, 4)], sem.at[i // 4]).start()

    lane = lax.broadcasted_iota(jnp.int32, (B, BP), 1)
    for p in range(8):
        t0 = q[3 * p].astype(f32)
        t1 = pltpu.roll(q[3 * p + 1].astype(f32), 64, 1)
        t2 = pltpu.roll(q[3 * p + 2].astype(f32), 64, 1)
        r0 = q[3 * p + 1].astype(f32)
        nopes = (t0, jnp.where(lane < ROT, t1, t2))
        ropes = (jnp.where(lane < ROT, r0, 0.0), jnp.where(lane < ROT, t2, 0.0))
        for j in range(2):
            h = 2 * p + j
            lat = lax.dot_general(
                nopes[j].astype(bf16),
                keys_v[:, 128 * h : 128 * h + 128],
                (((1,), (1,)), ((), ())),
                preferred_element_type=f32,
            )
            q_s[:, h, :LR] = (lat * SCALE).astype(bf16).astype(f32)
            q_s[:, h, LR:] = ropes[j]

    fetch.wait()

    def scores(g, _):
        here = kv.at[pl.ds(16 * g, 16)]
        pltpu.make_async_copy(here, here, sem.at[g]).wait()
        dy = jnp.where(g == 0, 0, jnp.where(g == 1, 3, jnp.where(g == 2, 1, 2)))
        ys = lax.rem(y + dy, 4)
        for dc in range(2):
            cs = c if dc == 0 else 1 - c
            first = (ys * 2 + cs) * 8
            for k in range(8):
                at = g * 16 + dc * 8 + k
                e = inv[first + k]
                place[e] = at
                qb = q_s[e // 4].astype(bf16)
                keys = kv[at, :BP, :]
                rope = jnp.concatenate([kv[at, BP:, 128 * n : 128 * n + 128] for n in range(4)], axis=0)
                sc = lax.dot_general(qb[:, :LR], keys, (((1,), (1,)), ((), ())), preferred_element_type=f32)
                s_s[e] = sc + jnp.dot(qb[:, LR : LR + ROT], rope, preferred_element_type=f32)
        return 0

    lax.fori_loop(0, 4, scores, 0)

    def softmax(bh, r):
        b = bh * 8 + r
        room = inv[64 + b]
        new = jnp.sum(q_s[b] * wide[pl.ds(b, 1), :], axis=1, keepdims=True)
        mine = jnp.full((B, 1), s, jnp.int32) == 0
        live = [lane < room - j * BP for j in range(4)]
        sc = [jnp.where(live[j], s_s[b * 4 + j], FLOOR) for j in range(4)]
        m = jnp.maximum(jnp.maximum(sc[0], sc[1]), jnp.maximum(sc[2], sc[3]))
        m = jnp.maximum(jnp.max(m, axis=1, keepdims=True), jnp.where(mine, new, FLOOR))
        p = [jnp.where(live[j], jnp.exp(sc[j] - m), 0.0) for j in range(4)]
        new = jnp.where(mine, jnp.exp(new - m), 0.0)
        l = jnp.sum((p[0] + p[1]) + (p[2] + p[3]), axis=1, keepdims=True) + new
        m1 = m.astype(bf16).astype(f32)
        m2 = (m - m1).astype(bf16).astype(f32)
        m3 = m - m1 - m2
        l1 = l.astype(bf16).astype(f32)
        l2 = (l - l1).astype(bf16).astype(f32)
        l3 = l - l1 - l2
        stats = jnp.zeros((B, 128), f32)
        for n, v in enumerate((m1, m2, m3, l1, l2, l3)):
            stats = jnp.where(lane == n, v, stats)
        o_s[pl.ds(bh * 16, 16), r, LR:] = stats
        own_s[b] = new.astype(bf16).astype(f32) * wide[pl.ds(b, 1), :LR]
        p_s[b] = jnp.concatenate(p, axis=1).astype(bf16)

    def mixing(bh, r):
        b = bh * 8 + r
        p = p_s[b]
        mix = own_s[b]
        for j in range(4):
            keys = kv[place[b * 4 + j], :BP, :]
            mix = mix + jnp.dot(p[:, 128 * j : 128 * j + 128], keys, preferred_element_type=f32)
        o_s[pl.ds(bh * 16, 16), r, :LR] = mix

    def halves(step):
        def both(bh, _):
            for r in range(8):
                step(bh, r)
            return 0

        lax.fori_loop(0, 2, both, 0)

    halves(softmax)
    halves(mixing)

    def pour(i, _):
        out[i] = o_s[i].astype(bf16)
        return 0

    lax.fori_loop(0, 32, pour, 0, unroll=8)


def attend_call(slots, q, wide, keys, bufs):
    return pl.pallas_call(
        attend_kernel,
        out_shape=pltpu.VMEM((32, 8, LR + 128), bf16),
        in_specs=[spec(HB)] + [spec(VM)] * 3 + [spec(HB)] * 16,
        out_specs=spec(VM),
        scratch_shapes=[
            pltpu.VMEM((64, BP + 16, LR), bf16),
            pltpu.VMEM((B, B, LR + 128), f32),
            pltpu.VMEM((64, B, BP), f32),
            pltpu.VMEM((B, B, 4 * BP), bf16),
            pltpu.VMEM((32, 8, LR + 128), f32),
            pltpu.VMEM((B, B, LR), f32),
            pltpu.SMEM((64,), jnp.int32),
            pltpu.SMEM((128,), jnp.int32),
            pltpu.SemaphoreType.DMA,
            pltpu.SemaphoreType.DMA((4,)),
        ],
        name="attend",
    )(slots, *here(q, wide, keys), *bufs)


def value_kernel(parts, value_up, out, vals, sem):
    h = lax.rem(place_of()[0], 16)
    cp = pltpu.make_async_copy(value_up.at[:, pl.ds(pl.multiple_of(h * VD, VD), VD)], vals, sem)
    cp.start()
    tops, tots = [], []
    for i in range(32):
        st = parts[i, :, LR:].astype(f32)
        tops.append(st[:, 0:1] + st[:, 1:2] + st[:, 2:3])
        tots.append(st[:, 3:4] + st[:, 4:5] + st[:, 5:6])
    top = functools.reduce(jnp.maximum, tops)
    total = jnp.zeros((8, 1), f32)
    mix = jnp.zeros((8, LR), f32)
    for i in range(32):
        w = jnp.exp(tops[i] - top)
        total = total + w * tots[i]
        mix = mix + w * parts[i, :, :LR].astype(f32)
    att = (mix / total).astype(bf16)
    cp.wait()
    res = jnp.dot(att, vals[...], preferred_element_type=f32).astype(bf16)
    for i in range(32):
        out[i] = res


def value_call(parts, value_up):
    return pl.pallas_call(
        value_kernel,
        out_shape=pltpu.VMEM((32, 8, VD), bf16),
        in_specs=[spec(VM), spec(HB)],
        out_specs=spec(VM),
        scratch_shapes=[pltpu.VMEM((LR, VD), bf16), pltpu.SemaphoreType.DMA],
        name="value",
    )(*here(parts), value_up)


UP = [(i, (i + 1) % 4) for i in range(4)]
DOWN = [(i, (i + 3) % 4) for i in range(4)]
SWAP = [(0, 1), (1, 0)]


def shift(value, axis, pairs):
    return lax.ppermute(value, axis, pairs)


def body(hidden_in, united_down, q_gain, kv_gain, q_up, key_up, value_up, store, rope_pool, lengths, table):
    lane = jnp.arange(128)
    freq = 10000.0 ** (-2.0 * (lane % 32).astype(f32) / ROT)
    angles = lengths.astype(f32)[:, None] * freq
    cos, sin = jnp.cos(angles), jnp.sin(angles)
    half_a, half_b = pack_call(store, rope_pool)
    up_a = shift(half_a, "y", UP)
    down_b = shift(half_b, "y", DOWN)
    q_tile = exchange(tiles_call(q_up), S)
    cols = united_call(hidden_in, united_down)
    spread = [cols] + [shift(cols, "y", [((i + d) % 4, i) for i in range(4)]) for d in (1, 2, 3)]
    parts = []
    for d in range(4):
        parts += [spread[d], shift(spread[d], "c", SWAP)]
    up_b = shift(half_b, "y", UP)
    down_a = shift(half_a, "y", DOWN)
    far_a = shift(up_a, "y", UP)
    far_b = shift(down_b, "y", DOWN)
    near = {0: (half_a, half_b), 3: (up_a, up_b), 1: (down_a, down_b), 2: (far_a, far_b)}
    bufs = []
    for dy, dc, h in ORDER:
        bufs.append(near[dy][h] if dc == 0 else shift(near[dy][h], "c", SWAP))
    entry, wide, q_copies = query_call(parts, q_gain, kv_gain, cos, sin, q_tile)
    q_all = exchange(q_copies, S)
    keys, slots = keys_call(table, lengths, key_up)
    mixed = attend_call(slots, q_all, wide, keys, bufs)
    spans = exchange(mixed, S)
    res = value_call(spans, value_up)
    res = exchange(res, S)
    res = res.reshape(2, 16, 8, VD).transpose(0, 2, 1, 3).reshape(B, 16 * VD)
    return res, entry


def solution(mesh):
    split = Mesh(mesh.devices.reshape(8, 4, 4, 2), ("z", "x", "y", "c"))
    return jax.shard_map(
        body,
        mesh=split,
        in_specs=(
            P(),
            P(None, T),
            P(),
            P(),
            P(S, T),
            P(None, T),
            P(None, T),
            P(S + T, None, None),
            P(S + T, None, None),
            P(),
            P(None, S),
        ),
        out_specs=(P(None, T), P()),
        check_vma=False,
    )
```

```python
import functools

import jax
import jax.numpy as jnp
from jax import lax
from jax.experimental import pallas as pl
from jax.experimental.pallas import tpu as pltpu
from jax.sharding import Mesh
from jax.sharding import PartitionSpec as P


D = 5120
QR = 1536
LR = 512
ROT = 64
VD = 128
B = 16
BP = 128
QH = 192
SCALE = QH ** (-0.5)
FLOOR = -1e30
S = ("z", "x")
T = ("y", "c")
bf16 = jnp.bfloat16
f32 = jnp.float32
VM = pltpu.MemorySpace.VMEM
SM = pltpu.MemorySpace.SMEM
HB = pltpu.MemorySpace.HBM


def spec(space):
    return pl.BlockSpec(memory_space=space)


def here(*values):
    return tuple(pltpu.with_memory_space_constraint(v, VM) for v in values)


def exchange(pieces, axes):
    return lax.all_to_all(pieces, axes, split_axis=0, concat_axis=0, tiled=True)


UK = 5


def united_kernel(hid_hbm, wt, out, hid, wbuf, hsem, wsem):
    step = D // UK
    copies = []
    fetch = pltpu.make_async_copy(hid_hbm, hid, hsem)
    fetch.start()
    for k in range(UK):
        cp = pltpu.make_async_copy(wt.at[:, pl.ds(k * step, step)], wbuf.at[k], wsem.at[k])
        cp.start()
        copies.append(cp)
    acc = jnp.zeros(out.shape, f32)
    fetch.wait()
    for k in range(UK):
        copies[k].wait()
        acc = acc + lax.dot_general(
            hid[:, k * step : (k + 1) * step],
            wbuf[k],
            (((1,), (1,)), ((), ())),
            preferred_element_type=f32,
        )
    out[...] = acc.astype(bf16)


def united_call(hid, down):
    cols = down.shape[1]
    return pl.pallas_call(
        united_kernel,
        out_shape=pltpu.VMEM((B, cols), bf16),
        in_specs=[spec(HB), spec(HB)],
        out_specs=spec(VM),
        scratch_shapes=[
            pltpu.VMEM((B, D), bf16),
            pltpu.VMEM((UK, cols, D // UK), bf16),
            pltpu.SemaphoreType.DMA,
            pltpu.SemaphoreType.DMA((UK,)),
        ],
        name="united",
    )(hid, down.T)


def tiles_kernel(q_up, out):
    for k in range(32):
        j = k % 24
        out[k] = q_up[:, 128 * j : 128 * j + 128]


def tiles_call(q_up):
    return pl.pallas_call(
        tiles_kernel,
        out_shape=pltpu.VMEM((32, 48, 128), bf16),
        in_specs=[spec(VM)],
        out_specs=spec(VM),
        name="tiles",
    )(*here(q_up))


def pack_kernel(lat, rope, out, ropes, sem):
    fetch_rope = pltpu.make_async_copy(rope, ropes, sem.at[0])
    fetch_rope.start()
    fetch = pltpu.make_async_copy(lat, out.at[:, pl.ds(0, BP), :], sem.at[1])
    fetch.start()
    fetch_rope.wait()
    for n in range(8):
        for g in range(4):
            out[n, BP:, 128 * g : 128 * g + 128] = ropes[n, 16 * g : 16 * g + 16, :]
    fetch.wait()


def pack_call(lat, rope):
    return pl.pallas_call(
        pack_kernel,
        out_shape=pltpu.VMEM((8, BP + 16, LR), bf16),
        in_specs=[spec(HB)] * 2,
        out_specs=spec(VM),
        scratch_shapes=[pltpu.VMEM((8, ROT, BP), bf16), pltpu.SemaphoreType.DMA((2,))],
        name="pack",
    )(lat, rope)


def place_of():
    return lax.axis_index("z") * 4 + lax.axis_index("x"), lax.axis_index("y"), lax.axis_index("c")


def swapped(x):
    lane = lax.broadcasted_iota(jnp.int32, x.shape, 1)
    return jnp.where(lane % ROT < ROT // 2, pltpu.roll(x, 96, 1), pltpu.roll(x, 32, 1))


def query_kernel(*refs):
    pairs, (q_gain, kv_gain, cos, sin_part, weights, entry, wide, out, parts) = refs[:4], refs[4:]
    s, y, c = place_of()
    width = 264
    step = 1 - 2 * c
    for ref, dy, core in zip(pairs, (0, step, -step, 2), (c, c, 1 - c, c)):
        at = lax.rem(y + dy + 4, 4) * 2
        parts[at + core] = ref[0].astype(f32)
        parts[at + 1 - core] = ref[1].astype(f32)
    tiles = [None] * 17
    for i in range(8):
        piece = parts[i]
        piece = jnp.concatenate([piece, jnp.zeros((B, 384 - width), f32)], axis=1)
        if i:
            piece = pltpu.roll(piece, 8 * i, 1)
        for k in range(3):
            part = piece[:, 128 * k : 128 * k + 128]
            if 2 * i + k < 17:
                tiles[2 * i + k] = part if tiles[2 * i + k] is None else tiles[2 * i + k] + part
    u = jnp.concatenate(tiles, axis=1)
    uq = u[:, :QR]
    ul = u[:, QR : QR + LR]
    ur = u[:, QR + LR : QR + LR + 128]
    rq = lax.rsqrt(jnp.sum(uq * uq, axis=1, keepdims=True) / QR + 1.0)
    rl = lax.rsqrt(jnp.sum(ul * ul, axis=1, keepdims=True) / LR + 1.0)
    ql = (uq * rq * q_gain[...].reshape(1, QR)).astype(bf16)
    q = jnp.dot(ql, weights[...].reshape(QR, 128), preferred_element_type=f32)
    lane = lax.broadcasted_iota(jnp.int32, (B, 128), 1)
    sin = jnp.where(lane % ROT < ROT // 2, -sin_part[...], sin_part[...])
    kind = lax.rem(s, 3)
    in_rope = ((lane < ROT) & (kind == 1)) | ((lane >= ROT) & (kind == 2))
    res = jnp.where(in_rope, (q * cos[...] + swapped(q) * sin) * SCALE, q).astype(bf16)
    for i in range(32):
        out[i] = res
    lat = (ul * rl * kv_gain[...].reshape(1, LR)).astype(bf16)
    rot = jnp.where(lane < ROT, ur * cos[...] + swapped(ur) * sin, 0.0).astype(bf16)
    entry[:, :LR] = lat
    entry[:, LR:] = rot[:, :ROT]
    wide[:, :LR] = lat.astype(f32)
    wide[:, LR:] = rot.astype(f32)


def query_call(parts, q_gain, kv_gain, cos, sin, weights):
    return pl.pallas_call(
        query_kernel,
        out_shape=(
            jax.ShapeDtypeStruct((B, LR + ROT), bf16),
            pltpu.VMEM((B, LR + 128), f32),
            pltpu.VMEM((32, B, 128), bf16),
        ),
        in_specs=[spec(VM)] * 9,
        out_specs=(spec(VM),) * 3,
        scratch_shapes=[pltpu.VMEM((8, B, 264), f32)],
        name="query",
    )(*here(*parts, q_gain, kv_gain, cos, sin, weights))


def slots_kernel(table, lengths, slots):
    s = place_of()[0]

    def fill(b, _):
        slots[64 + b] = lengths[b] - s * (4 * BP)
        for j in range(4):
            slots[table[b, j] - s * 64] = b * 4 + j
        return 0

    lax.fori_loop(0, B, fill, 0, unroll=4)
    for i in range(80, 128):
        slots[i] = 0


def slots_call(table, lengths):
    return pl.pallas_call(
        slots_kernel,
        out_shape=jax.ShapeDtypeStruct((128,), jnp.int32),
        in_specs=[spec(SM), spec(SM)],
        out_specs=spec(SM),
        name="slots",
    )(table, lengths)


def attend_kernel(slots, q, wide, key_up, *rest):
    bufs, out = rest[:8], rest[8]
    keys_v, kv, q_s, s_s, p_s, o_s, own_s, place, inv, ksem, tsem, sem = rest[9:]
    fetch = pltpu.make_async_copy(slots, inv, tsem)
    fetch.start()
    s, y, c = place_of()
    loads = []
    for n in range(4):
        cols = pl.ds(512 * n, 512)
        cp = pltpu.make_async_copy(key_up.at[:, cols], keys_v.at[:, cols], ksem.at[n])
        cp.start()
        loads.append(cp)
    for i in range(8):
        pltpu.make_async_copy(bufs[i], kv.at[pl.ds(8 * i, 8)], sem.at[i // 2]).start()

    lane = lax.broadcasted_iota(jnp.int32, (B, BP), 1)
    for p in range(8):
        if p % 2 == 0:
            loads[p // 2].wait()
        t0 = q[3 * p].astype(f32)
        t1 = pltpu.roll(q[3 * p + 1].astype(f32), 64, 1)
        t2 = pltpu.roll(q[3 * p + 2].astype(f32), 64, 1)
        r0 = q[3 * p + 1].astype(f32)
        nopes = (t0, jnp.where(lane < ROT, t1, t2))
        ropes = (jnp.where(lane < ROT, r0, 0.0), jnp.where(lane < ROT, t2, 0.0))
        for j in range(2):
            h = 2 * p + j
            lat = lax.dot_general(
                nopes[j].astype(bf16),
                keys_v[:, 128 * h : 128 * h + 128],
                (((1,), (1,)), ((), ())),
                preferred_element_type=f32,
            )
            q_s[:, h, :LR] = (lat * SCALE).astype(bf16).astype(f32)
            q_s[:, h, LR:] = ropes[j]

    fetch.wait()

    def scores(g, _):
        here = kv.at[pl.ds(16 * g, 16)]
        pltpu.make_async_copy(here, here, sem.at[g]).wait()
        for dc in range(2):
            cs = c if dc == 0 else 1 - c
            alpha = 3 - 2 * cs
            dy = jnp.where(g == 0, 0, jnp.where(g == 1, alpha, jnp.where(g == 2, 2, 4 - alpha)))
            first = (lax.rem(y + dy, 4) * 2 + cs) * 8
            for k in range(8):
                at = g * 16 + dc * 8 + k
                e = inv[first + k]
                place[e] = at
                qb = q_s[e // 4].astype(bf16)
                keys = kv[at, :BP, :]
                rope = jnp.concatenate([kv[at, BP:, 128 * n : 128 * n + 128] for n in range(4)], axis=0)
                sc = lax.dot_general(qb[:, :LR], keys, (((1,), (1,)), ((), ())), preferred_element_type=f32)
                s_s[e] = sc + jnp.dot(qb[:, LR : LR + ROT], rope, preferred_element_type=f32)
        return 0

    lax.fori_loop(0, 4, scores, 0)

    def softmax(bh, r):
        b = bh * 8 + r
        room = inv[64 + b]
        new = jnp.sum(q_s[b] * wide[pl.ds(b, 1), :], axis=1, keepdims=True)
        mine = jnp.full((B, 1), s, jnp.int32) == 0
        live = [lane < room - j * BP for j in range(4)]
        sc = [jnp.where(live[j], s_s[b * 4 + j], FLOOR) for j in range(4)]
        m = jnp.maximum(jnp.maximum(sc[0], sc[1]), jnp.maximum(sc[2], sc[3]))
        m = jnp.maximum(jnp.max(m, axis=1, keepdims=True), jnp.where(mine, new, FLOOR))
        p = [jnp.where(live[j], jnp.exp(sc[j] - m), 0.0) for j in range(4)]
        new = jnp.where(mine, jnp.exp(new - m), 0.0)
        l = jnp.sum((p[0] + p[1]) + (p[2] + p[3]), axis=1, keepdims=True) + new
        m1 = m.astype(bf16).astype(f32)
        m2 = (m - m1).astype(bf16).astype(f32)
        m3 = m - m1 - m2
        l1 = l.astype(bf16).astype(f32)
        l2 = (l - l1).astype(bf16).astype(f32)
        l3 = l - l1 - l2
        stats = jnp.zeros((B, 128), f32)
        for n, v in enumerate((m1, m2, m3, l1, l2, l3)):
            stats = jnp.where(lane == n, v, stats)
        o_s[pl.ds(bh * 16, 16), r, LR:] = stats
        own_s[b] = new.astype(bf16).astype(f32) * wide[pl.ds(b, 1), :LR]
        p_s[b] = jnp.concatenate(p, axis=1).astype(bf16)

    def mixing(bh, r):
        b = bh * 8 + r
        p = p_s[b]
        mix = own_s[b]
        for j in range(4):
            keys = kv[place[b * 4 + j], :BP, :]
            mix = mix + jnp.dot(p[:, 128 * j : 128 * j + 128], keys, preferred_element_type=f32)
        o_s[pl.ds(bh * 16, 16), r, :LR] = mix

    def halves(step):
        def both(bh, _):
            for r in range(8):
                step(bh, r)
            return 0

        lax.fori_loop(0, 2, both, 0)

    halves(softmax)
    halves(mixing)

    def pour(i, _):
        out[i] = o_s[i].astype(bf16)
        return 0

    lax.fori_loop(0, 32, pour, 0, unroll=8)


def attend_call(slots, q, wide, key_up, bufs):
    return pl.pallas_call(
        attend_kernel,
        out_shape=pltpu.VMEM((32, 8, LR + 128), bf16),
        in_specs=[spec(HB)] + [spec(VM)] * 2 + [spec(HB)] * 9,
        out_specs=spec(VM),
        scratch_shapes=[
            pltpu.VMEM((LR, 2048), bf16),
            pltpu.VMEM((64, BP + 16, LR), bf16),
            pltpu.VMEM((B, B, LR + 128), f32),
            pltpu.VMEM((64, B, BP), f32),
            pltpu.VMEM((B, B, 4 * BP), bf16),
            pltpu.VMEM((32, 8, LR + 128), f32),
            pltpu.VMEM((B, B, LR), f32),
            pltpu.SMEM((64,), jnp.int32),
            pltpu.SMEM((128,), jnp.int32),
            pltpu.SemaphoreType.DMA((4,)),
            pltpu.SemaphoreType.DMA,
            pltpu.SemaphoreType.DMA((4,)),
        ],
        name="attend",
    )(slots, *here(q, wide), key_up, *(pltpu.with_memory_space_constraint(v, HB) for v in bufs))


def value_kernel(parts, value_up, out, vals, sem):
    h = lax.rem(place_of()[0], 16)
    cp = pltpu.make_async_copy(value_up.at[:, pl.ds(pl.multiple_of(h * VD, VD), VD)], vals, sem)
    cp.start()
    tops, tots = [], []
    for i in range(32):
        st = parts[i, :, LR:].astype(f32)
        tops.append(st[:, 0:1] + st[:, 1:2] + st[:, 2:3])
        tots.append(st[:, 3:4] + st[:, 4:5] + st[:, 5:6])
    top = functools.reduce(jnp.maximum, tops)
    total = jnp.zeros((8, 1), f32)
    mix = jnp.zeros((8, LR), f32)
    for i in range(32):
        w = jnp.exp(tops[i] - top)
        total = total + w * tots[i]
        mix = mix + w * parts[i, :, :LR].astype(f32)
    att = (mix / total).astype(bf16)
    cp.wait()
    res = jnp.dot(att, vals[...], preferred_element_type=f32).astype(bf16)
    for i in range(32):
        out[i] = res


def value_call(parts, value_up):
    return pl.pallas_call(
        value_kernel,
        out_shape=pltpu.VMEM((32, 8, VD), bf16),
        in_specs=[spec(VM), spec(HB)],
        out_specs=spec(VM),
        scratch_shapes=[pltpu.VMEM((LR, VD), bf16), pltpu.SemaphoreType.DMA],
        name="value",
    )(*here(parts), value_up)


ALPHA = [(2 * y + c, 2 * ((y + 1 - 2 * c) % 4) + c) for y in range(4) for c in range(2)]
BETA = [(b, a) for a, b in ALPHA]
SWAP = [(0, 1), (1, 0)]


def body(hidden_in, united_down, q_gain, kv_gain, q_up, key_up, value_up, store, rope_pool, lengths, table):
    lane = jnp.arange(128)
    freq = 10000.0 ** (-2.0 * (lane % 32).astype(f32) / ROT)
    angles = lengths.astype(f32)[:, None] * freq
    cos, sin = jnp.cos(angles), jnp.sin(angles)
    mine = pack_call(store, rope_pool)
    alpha = lax.ppermute(mine, T, ALPHA)
    far = lax.ppermute(alpha, T, ALPHA)
    beta = lax.ppermute(mine, T, BETA)
    q_tile = exchange(tiles_call(q_up), S)
    cols = united_call(hidden_in, united_down)
    pair = jnp.stack([cols, lax.ppermute(cols, "c", SWAP)])
    near = lax.ppermute(pair, T, BETA)
    parts = [pair, near, lax.ppermute(near, "c", SWAP), lax.ppermute(near, T, BETA)]
    bufs = []
    for value in (mine, alpha, far, beta):
        bufs += [value, lax.ppermute(value, "c", SWAP)]
    entry, wide, q_copies = query_call(parts, q_gain, kv_gain, cos, sin, q_tile)
    q_all = exchange(q_copies, S)
    mixed = attend_call(slots_call(table, lengths), q_all, wide, key_up, bufs)
    spans = exchange(mixed, S)
    res = value_call(spans, value_up)
    res = exchange(res, S)
    res = res.reshape(2, 16, 8, VD).transpose(0, 2, 1, 3).reshape(B, 16 * VD)
    return res, entry


def solution(mesh):
    split = Mesh(mesh.devices.reshape(8, 4, 4, 2), ("z", "x", "y", "c"))
    return jax.shard_map(
        body,
        mesh=split,
        in_specs=(
            P(),
            P(None, T),
            P(),
            P(),
            P(S, T),
            P(None, T),
            P(None, T),
            P(S + T, None, None),
            P(S + T, None, None),
            P(),
            P(None, S),
        ),
        out_specs=(P(None, T), P()),
        check_vma=False,
    )
```

```python
import functools

import jax
import jax.numpy as jnp
from jax import lax
from jax.experimental import pallas as pl
from jax.experimental.pallas import tpu as pltpu
from jax.sharding import Mesh
from jax.sharding import PartitionSpec as P


D = 5120
QR = 1536
LR = 512
ROT = 64
VD = 128
B = 16
BP = 128
QH = 192
SCALE = QH ** (-0.5)
FLOOR = -1e30
S = ("z", "x")
T = ("y", "c")
bf16 = jnp.bfloat16
f32 = jnp.float32
VM = pltpu.MemorySpace.VMEM
SM = pltpu.MemorySpace.SMEM
HB = pltpu.MemorySpace.HBM


def spec(space):
    return pl.BlockSpec(memory_space=space)


def here(*values):
    return tuple(pltpu.with_memory_space_constraint(v, VM) for v in values)


def exchange(pieces, axes):
    return lax.all_to_all(pieces, axes, split_axis=0, concat_axis=0, tiled=True)


UK = 5


def united_kernel(hid_hbm, wt, out, hid, wbuf, hsem, wsem):
    step = D // UK
    copies = []
    fetch = pltpu.make_async_copy(hid_hbm, hid, hsem)
    fetch.start()
    for k in range(UK):
        cp = pltpu.make_async_copy(wt.at[:, pl.ds(k * step, step)], wbuf.at[k], wsem.at[k])
        cp.start()
        copies.append(cp)
    acc = jnp.zeros(out.shape, f32)
    fetch.wait()
    for k in range(UK):
        copies[k].wait()
        acc = acc + lax.dot_general(
            hid[:, k * step : (k + 1) * step],
            wbuf[k],
            (((1,), (1,)), ((), ())),
            preferred_element_type=f32,
        )
    out[...] = acc.astype(bf16)


def united_call(hid, down):
    cols = down.shape[1]
    return pl.pallas_call(
        united_kernel,
        out_shape=pltpu.VMEM((B, cols), bf16),
        in_specs=[spec(HB), spec(HB)],
        out_specs=spec(VM),
        scratch_shapes=[
            pltpu.VMEM((B, D), bf16),
            pltpu.VMEM((UK, cols, D // UK), bf16),
            pltpu.SemaphoreType.DMA,
            pltpu.SemaphoreType.DMA((UK,)),
        ],
        name="united",
    )(hid, down.T)


def tiles_kernel(q_up, out):
    for k in range(32):
        j = k % 24
        out[k] = q_up[:, 128 * j : 128 * j + 128]


def tiles_call(q_up):
    return pl.pallas_call(
        tiles_kernel,
        out_shape=pltpu.VMEM((32, 48, 128), bf16),
        in_specs=[spec(VM)],
        out_specs=spec(VM),
        name="tiles",
    )(*here(q_up))


def pack_kernel(lat, rope, out, ropes, sem):
    fetch_rope = pltpu.make_async_copy(rope, ropes, sem.at[0])
    fetch_rope.start()
    fetch = pltpu.make_async_copy(lat, out.at[:, pl.ds(0, BP), :], sem.at[1])
    fetch.start()
    fetch_rope.wait()
    for n in range(8):
        for g in range(4):
            out[n, BP:, 128 * g : 128 * g + 128] = ropes[n, 16 * g : 16 * g + 16, :]
    fetch.wait()


def pack_call(lat, rope):
    return pl.pallas_call(
        pack_kernel,
        out_shape=pltpu.VMEM((8, BP + 16, LR), bf16),
        in_specs=[spec(HB)] * 2,
        out_specs=spec(VM),
        scratch_shapes=[pltpu.VMEM((8, ROT, BP), bf16), pltpu.SemaphoreType.DMA((2,))],
        name="pack",
    )(lat, rope)


def place_of():
    return lax.axis_index("z") * 4 + lax.axis_index("x"), lax.axis_index("y"), lax.axis_index("c")


def swapped(x):
    lane = lax.broadcasted_iota(jnp.int32, x.shape, 1)
    return jnp.where(lane % ROT < ROT // 2, pltpu.roll(x, 96, 1), pltpu.roll(x, 32, 1))


def query_kernel(*refs):
    pairs, (q_gain, kv_gain, cos, sin_part, weights, entry, wide, out, parts) = refs[:4], refs[4:]
    s, y, c = place_of()
    width = 264
    step = 1 - 2 * c
    for ref, dy, core in zip(pairs, (0, step, -step, 2), (c, c, 1 - c, c)):
        at = lax.rem(y + dy + 4, 4) * 2
        parts[at + core] = ref[0].astype(f32)
        parts[at + 1 - core] = ref[1].astype(f32)
    tiles = [None] * 17
    for i in range(8):
        piece = parts[i]
        piece = jnp.concatenate([piece, jnp.zeros((B, 384 - width), f32)], axis=1)
        if i:
            piece = pltpu.roll(piece, 8 * i, 1)
        for k in range(3):
            part = piece[:, 128 * k : 128 * k + 128]
            if 2 * i + k < 17:
                tiles[2 * i + k] = part if tiles[2 * i + k] is None else tiles[2 * i + k] + part
    u = jnp.concatenate(tiles, axis=1)
    uq = u[:, :QR]
    ul = u[:, QR : QR + LR]
    ur = u[:, QR + LR : QR + LR + 128]
    rq = lax.rsqrt(jnp.sum(uq * uq, axis=1, keepdims=True) / QR + 1.0)
    rl = lax.rsqrt(jnp.sum(ul * ul, axis=1, keepdims=True) / LR + 1.0)
    ql = (uq * rq * q_gain[...].reshape(1, QR)).astype(bf16)
    q = jnp.dot(ql, weights[...].reshape(QR, 128), preferred_element_type=f32)
    lane = lax.broadcasted_iota(jnp.int32, (B, 128), 1)
    sin = jnp.where(lane % ROT < ROT // 2, -sin_part[...], sin_part[...])
    kind = lax.rem(s, 3)
    in_rope = ((lane < ROT) & (kind == 1)) | ((lane >= ROT) & (kind == 2))
    res = jnp.where(in_rope, (q * cos[...] + swapped(q) * sin) * SCALE, q).astype(bf16)
    for i in range(32):
        out[i] = res
    lat = (ul * rl * kv_gain[...].reshape(1, LR)).astype(bf16)
    rot = jnp.where(lane < ROT, ur * cos[...] + swapped(ur) * sin, 0.0).astype(bf16)
    entry[:, :LR] = lat
    entry[:, LR:] = rot[:, :ROT]
    wide[:, :LR] = lat.astype(f32)
    wide[:, LR:] = rot.astype(f32)


def query_call(parts, q_gain, kv_gain, cos, sin, weights):
    return pl.pallas_call(
        query_kernel,
        out_shape=(
            jax.ShapeDtypeStruct((B, LR + ROT), bf16),
            pltpu.VMEM((B, LR + 128), f32),
            pltpu.VMEM((32, B, 128), bf16),
        ),
        in_specs=[spec(VM)] * 9,
        out_specs=(spec(VM),) * 3,
        scratch_shapes=[pltpu.VMEM((8, B, 264), f32)],
        name="query",
    )(*here(*parts, q_gain, kv_gain, cos, sin, weights))


def slots_kernel(table, lengths, slots):
    s = place_of()[0]

    def fill(b, _):
        slots[64 + b] = lengths[b] - s * (4 * BP)
        for j in range(4):
            slots[table[j, b] - s * 64] = b * 4 + j
        return 0

    lax.fori_loop(0, B, fill, 0, unroll=4)
    for i in range(80, 128):
        slots[i] = 0


def slots_call(table, lengths):
    return pl.pallas_call(
        slots_kernel,
        out_shape=jax.ShapeDtypeStruct((128,), jnp.int32),
        in_specs=[spec(SM), spec(SM)],
        out_specs=spec(SM),
        name="slots",
    )(table.T, lengths)


def keys_kernel(src, dst, sem):
    cp = pltpu.make_async_copy(src, dst, sem)
    cp.start()
    cp.wait()


def keys_call(key_up):
    return pl.pallas_call(
        keys_kernel,
        out_shape=pltpu.VMEM(key_up.shape, bf16),
        in_specs=[spec(HB)],
        out_specs=spec(VM),
        scratch_shapes=[pltpu.SemaphoreType.DMA],
        name="keys",
    )(key_up)


def attend_kernel(slots, q, wide, keys_v, *rest):
    bufs, out = rest[:8], rest[8]
    kv, q_s, s_s, p_s, o_s, own_s, place, inv, tsem, sem = rest[9:]
    fetch = pltpu.make_async_copy(slots, inv, tsem)
    fetch.start()
    s, y, c = place_of()
    for i in range(8):
        pltpu.make_async_copy(bufs[i], kv.at[pl.ds(8 * i, 8)], sem.at[i // 2]).start()

    lane = lax.broadcasted_iota(jnp.int32, (B, BP), 1)
    for p in range(8):
        t0 = q[3 * p].astype(f32)
        t1 = pltpu.roll(q[3 * p + 1].astype(f32), 64, 1)
        t2 = pltpu.roll(q[3 * p + 2].astype(f32), 64, 1)
        r0 = q[3 * p + 1].astype(f32)
        nopes = (t0, jnp.where(lane < ROT, t1, t2))
        ropes = (jnp.where(lane < ROT, r0, 0.0), jnp.where(lane < ROT, t2, 0.0))
        for j in range(2):
            h = 2 * p + j
            lat = lax.dot_general(
                nopes[j].astype(bf16),
                keys_v[:, 128 * h : 128 * h + 128],
                (((1,), (1,)), ((), ())),
                preferred_element_type=f32,
            )
            q_s[:, h, :LR] = (lat * SCALE).astype(bf16).astype(f32)
            q_s[:, h, LR:] = ropes[j]

    fetch.wait()

    def scores(g, _):
        here = kv.at[pl.ds(16 * g, 16)]
        pltpu.make_async_copy(here, here, sem.at[g]).wait()
        for dc in range(2):
            cs = c if dc == 0 else 1 - c
            alpha = 3 - 2 * cs
            dy = jnp.where(g == 0, 0, jnp.where(g == 1, alpha, jnp.where(g == 2, 2, 4 - alpha)))
            first = (lax.rem(y + dy, 4) * 2 + cs) * 8
            for k in range(8):
                at = g * 16 + dc * 8 + k
                e = inv[first + k]
                place[e] = at
                qb = q_s[e // 4].astype(bf16)
                keys = kv[at, :BP, :]
                rope = jnp.concatenate([kv[at, BP:, 128 * n : 128 * n + 128] for n in range(4)], axis=0)
                sc = lax.dot_general(qb[:, :LR], keys, (((1,), (1,)), ((), ())), preferred_element_type=f32)
                s_s[e] = sc + jnp.dot(qb[:, LR : LR + ROT], rope, preferred_element_type=f32)
        return 0

    lax.fori_loop(0, 4, scores, 0)

    def softmax(bh, r):
        b = bh * 8 + r
        room = inv[64 + b]
        new = jnp.sum(q_s[b] * wide[pl.ds(b, 1), :], axis=1, keepdims=True)
        mine = jnp.full((B, 1), s, jnp.int32) == 0
        live = [lane < room - j * BP for j in range(4)]
        sc = [jnp.where(live[j], s_s[b * 4 + j], FLOOR) for j in range(4)]
        m = jnp.maximum(jnp.maximum(sc[0], sc[1]), jnp.maximum(sc[2], sc[3]))
        m = jnp.maximum(jnp.max(m, axis=1, keepdims=True), jnp.where(mine, new, FLOOR))
        p = [jnp.where(live[j], jnp.exp(sc[j] - m), 0.0) for j in range(4)]
        new = jnp.where(mine, jnp.exp(new - m), 0.0)
        l = jnp.sum((p[0] + p[1]) + (p[2] + p[3]), axis=1, keepdims=True) + new
        m1 = m.astype(bf16).astype(f32)
        m2 = (m - m1).astype(bf16).astype(f32)
        m3 = m - m1 - m2
        l1 = l.astype(bf16).astype(f32)
        l2 = (l - l1).astype(bf16).astype(f32)
        l3 = l - l1 - l2
        stats = jnp.zeros((B, 128), f32)
        for n, v in enumerate((m1, m2, m3, l1, l2, l3)):
            stats = jnp.where(lane == n, v, stats)
        o_s[pl.ds(bh * 16, 16), r, LR:] = stats
        own_s[b] = new.astype(bf16).astype(f32) * wide[pl.ds(b, 1), :LR]
        p_s[b] = jnp.concatenate(p, axis=1).astype(bf16)

    def mixing(bh, r):
        b = bh * 8 + r
        p = p_s[b]
        mix = own_s[b]
        for j in range(4):
            keys = kv[place[b * 4 + j], :BP, :]
            mix = mix + jnp.dot(p[:, 128 * j : 128 * j + 128], keys, preferred_element_type=f32)
        o_s[pl.ds(bh * 16, 16), r, :LR] = mix

    def halves(step):
        def both(bh, _):
            for r in range(8):
                step(bh, r)
            return 0

        lax.fori_loop(0, 2, both, 0)

    halves(softmax)
    halves(mixing)

    def pour(i, _):
        out[i] = o_s[i].astype(bf16)
        return 0

    lax.fori_loop(0, 32, pour, 0, unroll=8)


def attend_call(slots, q, wide, keys, bufs):
    return pl.pallas_call(
        attend_kernel,
        out_shape=pltpu.VMEM((32, 8, LR + 128), bf16),
        in_specs=[spec(HB)] + [spec(VM)] * 3 + [spec(HB)] * 8,
        out_specs=spec(VM),
        scratch_shapes=[
            pltpu.VMEM((64, BP + 16, LR), bf16),
            pltpu.VMEM((B, B, LR + 128), f32),
            pltpu.VMEM((64, B, BP), f32),
            pltpu.VMEM((B, B, 4 * BP), bf16),
            pltpu.VMEM((32, 8, LR + 128), f32),
            pltpu.VMEM((B, B, LR), f32),
            pltpu.SMEM((64,), jnp.int32),
            pltpu.SMEM((128,), jnp.int32),
            pltpu.SemaphoreType.DMA,
            pltpu.SemaphoreType.DMA((4,)),
        ],
        name="attend",
    )(slots, *here(q, wide, keys), *(pltpu.with_memory_space_constraint(v, HB) for v in bufs))


def value_kernel(parts, value_up, out, vals, sem):
    h = lax.rem(place_of()[0], 16)
    cp = pltpu.make_async_copy(value_up.at[:, pl.ds(pl.multiple_of(h * VD, VD), VD)], vals, sem)
    cp.start()
    tops, tots = [], []
    for i in range(32):
        st = parts[i, :, LR:].astype(f32)
        tops.append(st[:, 0:1] + st[:, 1:2] + st[:, 2:3])
        tots.append(st[:, 3:4] + st[:, 4:5] + st[:, 5:6])
    top = functools.reduce(jnp.maximum, tops)
    total = jnp.zeros((8, 1), f32)
    mix = jnp.zeros((8, LR), f32)
    for i in range(32):
        w = jnp.exp(tops[i] - top)
        total = total + w * tots[i]
        mix = mix + w * parts[i, :, :LR].astype(f32)
    att = (mix / total).astype(bf16)
    cp.wait()
    res = jnp.dot(att, vals[...], preferred_element_type=f32).astype(bf16)
    for i in range(32):
        out[i] = res


def value_call(parts, value_up):
    return pl.pallas_call(
        value_kernel,
        out_shape=pltpu.VMEM((32, 8, VD), bf16),
        in_specs=[spec(VM), spec(HB)],
        out_specs=spec(VM),
        scratch_shapes=[pltpu.VMEM((LR, VD), bf16), pltpu.SemaphoreType.DMA],
        name="value",
    )(*here(parts), value_up)


ALPHA = [(2 * y + c, 2 * ((y + 1 - 2 * c) % 4) + c) for y in range(4) for c in range(2)]
BETA = [(b, a) for a, b in ALPHA]
SWAP = [(0, 1), (1, 0)]


def body(hidden_in, united_down, q_gain, kv_gain, q_up, key_up, value_up, store, rope_pool, lengths, table):
    lane = jnp.arange(128)
    freq = 10000.0 ** (-2.0 * (lane % 32).astype(f32) / ROT)
    angles = lengths.astype(f32)[:, None] * freq
    cos, sin = jnp.cos(angles), jnp.sin(angles)
    mine = pack_call(store, rope_pool)
    alpha = lax.ppermute(mine, T, ALPHA)
    far = lax.ppermute(alpha, T, ALPHA)
    beta = lax.ppermute(mine, T, BETA)
    q_tile = exchange(tiles_call(q_up), S)
    cols = united_call(hidden_in, united_down)
    pair = jnp.stack([cols, lax.ppermute(cols, "c", SWAP)])
    near = lax.ppermute(pair, T, BETA)
    parts = [pair, near, lax.ppermute(near, "c", SWAP), lax.ppermute(near, T, BETA)]
    bufs = []
    for value in (mine, alpha, far, beta):
        bufs += [value, lax.ppermute(value, "c", SWAP)]
    entry, wide, q_copies = query_call(parts, q_gain, kv_gain, cos, sin, q_tile)
    q_all = exchange(q_copies, S)
    mixed = attend_call(slots_call(table, lengths), q_all, wide, keys_call(key_up), bufs)
    spans = exchange(mixed, S)
    res = value_call(spans, value_up)
    res = exchange(res, S)
    res = res.reshape(2, 16, 8, VD).transpose(0, 2, 1, 3).reshape(B, 16 * VD)
    return res, entry


def solution(mesh):
    split = Mesh(mesh.devices.reshape(8, 4, 4, 2), ("z", "x", "y", "c"))
    return jax.shard_map(
        body,
        mesh=split,
        in_specs=(
            P(),
            P(None, T),
            P(),
            P(),
            P(S, T),
            P(None, T),
            P(None, T),
            P(S + T, None, None),
            P(S + T, None, None),
            P(),
            P(None, S),
        ),
        out_specs=(P(None, T), P()),
        check_vma=False,
    )
```

```python
import functools

import jax
import jax.numpy as jnp
from jax import lax
from jax.experimental import pallas as pl
from jax.experimental.pallas import tpu as pltpu
from jax.sharding import Mesh
from jax.sharding import PartitionSpec as P


D = 5120
QR = 1536
LR = 512
ROT = 64
VD = 128
B = 16
BP = 128
QH = 192
SCALE = QH ** (-0.5)
FLOOR = -1e30
S = ("z", "x")
T = ("y", "c")
bf16 = jnp.bfloat16
f32 = jnp.float32
VM = pltpu.MemorySpace.VMEM
SM = pltpu.MemorySpace.SMEM
HB = pltpu.MemorySpace.HBM


def grant(mib):
    return pltpu.CompilerParams(vmem_limit_bytes=mib << 20)


def spec(space):
    return pl.BlockSpec(memory_space=space)


def here(*values):
    return tuple(pltpu.with_memory_space_constraint(v, VM) for v in values)


def there(*values):
    return tuple(pltpu.with_memory_space_constraint(v, HB) for v in values)


def exchange(pieces, axes):
    return lax.all_to_all(pieces, axes, split_axis=0, concat_axis=0, tiled=True)


UK = 5


def united_kernel(hid_hbm, wt, out, hid, wbuf, hsem, wsem):
    step = D // UK
    copies = []
    fetch = pltpu.make_async_copy(hid_hbm, hid, hsem)
    fetch.start()
    for k in range(UK):
        cp = pltpu.make_async_copy(wt.at[:, pl.ds(k * step, step)], wbuf.at[k], wsem.at[k])
        cp.start()
        copies.append(cp)
    acc = jnp.zeros(out.shape, f32)
    fetch.wait()
    for k in range(UK):
        copies[k].wait()
        acc = acc + lax.dot_general(
            hid[:, k * step : (k + 1) * step],
            wbuf[k],
            (((1,), (1,)), ((), ())),
            preferred_element_type=f32,
        )
    out[...] = acc.astype(bf16)


def united_call(hid, down):
    cols = down.shape[1]
    return pl.pallas_call(
        united_kernel,
        out_shape=pltpu.VMEM((B, cols), bf16),
        in_specs=[spec(HB), spec(HB)],
        out_specs=spec(VM),
        scratch_shapes=[
            pltpu.VMEM((B, D), bf16),
            pltpu.VMEM((UK, cols, D // UK), bf16),
            pltpu.SemaphoreType.DMA,
            pltpu.SemaphoreType.DMA((UK,)),
        ],
        name="united",
    )(hid, down.T)


def tiles_kernel(q_up, out):
    for k in range(32):
        j = k % 24
        out[k] = q_up[:, 128 * j : 128 * j + 128]


def tiles_call(q_up):
    return pl.pallas_call(
        tiles_kernel,
        out_shape=pltpu.VMEM((32, 48, 128), bf16),
        in_specs=[spec(VM)],
        out_specs=spec(VM),
        name="tiles",
    )(*here(q_up))


def pack_kernel(lat, rope, out, ropes, sem):
    fetch_rope = pltpu.make_async_copy(rope, ropes, sem.at[0])
    fetch_rope.start()
    fetch = pltpu.make_async_copy(lat, out.at[:, pl.ds(0, BP), :], sem.at[1])
    fetch.start()
    fetch_rope.wait()
    for n in range(8):
        for g in range(4):
            out[n, BP:, 128 * g : 128 * g + 128] = ropes[n, 16 * g : 16 * g + 16, :]
    fetch.wait()


def pack_call(lat, rope):
    return pl.pallas_call(
        pack_kernel,
        out_shape=pltpu.VMEM((8, BP + 16, LR), bf16),
        in_specs=[spec(HB)] * 2,
        out_specs=spec(VM),
        scratch_shapes=[pltpu.VMEM((8, ROT, BP), bf16), pltpu.SemaphoreType.DMA((2,))],
        name="pack",
    )(lat, rope)


def place_of():
    return lax.axis_index("z") * 4 + lax.axis_index("x"), lax.axis_index("y"), lax.axis_index("c")


def swapped(x):
    lane = lax.broadcasted_iota(jnp.int32, x.shape, 1)
    return jnp.where(lane % ROT < ROT // 2, pltpu.roll(x, 96, 1), pltpu.roll(x, 32, 1))


def query_kernel(*refs):
    pairs, (q_gain, kv_gain, cos, sin_part, weights, entry, wide, out, parts) = refs[:4], refs[4:]
    s, y, c = place_of()
    width = 264
    step = 1 - 2 * c
    for ref, dy, core in zip(pairs, (0, step, -step, 2), (c, c, 1 - c, c)):
        at = lax.rem(y + dy + 4, 4) * 2
        parts[at + core] = ref[0].astype(f32)
        parts[at + 1 - core] = ref[1].astype(f32)
    tiles = [None] * 17
    for i in range(8):
        piece = parts[i]
        piece = jnp.concatenate([piece, jnp.zeros((B, 384 - width), f32)], axis=1)
        if i:
            piece = pltpu.roll(piece, 8 * i, 1)
        for k in range(3):
            part = piece[:, 128 * k : 128 * k + 128]
            if 2 * i + k < 17:
                tiles[2 * i + k] = part if tiles[2 * i + k] is None else tiles[2 * i + k] + part
    u = jnp.concatenate(tiles, axis=1)
    uq = u[:, :QR]
    ul = u[:, QR : QR + LR]
    ur = u[:, QR + LR : QR + LR + 128]
    rq = lax.rsqrt(jnp.sum(uq * uq, axis=1, keepdims=True) / QR + 1.0)
    rl = lax.rsqrt(jnp.sum(ul * ul, axis=1, keepdims=True) / LR + 1.0)
    ql = (uq * rq * q_gain[...].reshape(1, QR)).astype(bf16)
    q = jnp.dot(ql, weights[...].reshape(QR, 128), preferred_element_type=f32)
    lane = lax.broadcasted_iota(jnp.int32, (B, 128), 1)
    sin = jnp.where(lane % ROT < ROT // 2, -sin_part[...], sin_part[...])
    kind = lax.rem(s, 3)
    in_rope = ((lane < ROT) & (kind == 1)) | ((lane >= ROT) & (kind == 2))
    res = jnp.where(in_rope, (q * cos[...] + swapped(q) * sin) * SCALE, q).astype(bf16)
    for i in range(32):
        out[i] = res
    lat = (ul * rl * kv_gain[...].reshape(1, LR)).astype(bf16)
    rot = jnp.where(lane < ROT, ur * cos[...] + swapped(ur) * sin, 0.0).astype(bf16)
    entry[:, :LR] = lat
    entry[:, LR:] = rot[:, :ROT]
    wide[:, :LR] = lat.astype(f32)
    wide[:, LR:] = rot.astype(f32)


def query_call(parts, q_gain, kv_gain, cos, sin, weights):
    return pl.pallas_call(
        query_kernel,
        out_shape=(
            jax.ShapeDtypeStruct((B, LR + ROT), bf16),
            pltpu.VMEM((B, LR + 128), f32),
            pltpu.VMEM((32, B, 128), bf16),
        ),
        in_specs=[spec(VM)] * 9,
        out_specs=(spec(VM),) * 3,
        scratch_shapes=[pltpu.VMEM((8, B, 264), f32)],
        name="query",
    )(*here(*parts, q_gain, kv_gain, cos, sin, weights))


def slots_kernel(table, lengths, slots):
    s = place_of()[0]

    def fill(b, _):
        slots[64 + b] = lengths[b] - s * (4 * BP)
        for j in range(4):
            slots[table[j, b] - s * 64] = b * 4 + j
        return 0

    lax.fori_loop(0, B, fill, 0, unroll=4)
    for i in range(80, 128):
        slots[i] = 0


def slots_call(table, lengths):
    return pl.pallas_call(
        slots_kernel,
        out_shape=jax.ShapeDtypeStruct((128,), jnp.int32),
        in_specs=[spec(SM), spec(SM)],
        out_specs=spec(SM),
        name="slots",
    )(table.T, lengths)


def keys_kernel(src, dst, sem):
    cp = pltpu.make_async_copy(src, dst, sem)
    cp.start()
    cp.wait()


def keys_call(key_up):
    return pl.pallas_call(
        keys_kernel,
        out_shape=pltpu.VMEM(key_up.shape, bf16),
        in_specs=[spec(HB)],
        out_specs=spec(VM),
        scratch_shapes=[pltpu.SemaphoreType.DMA],
        name="keys",
        compiler_params=grant(54),
    )(*there(key_up))


def stage_kernel(*refs):
    bufs, kv, sem = refs[:6], refs[6], refs[7]
    loads = [pltpu.make_async_copy(ref, kv.at[pl.ds(8 * i, 8)], sem.at[i]) for i, ref in enumerate(bufs)]
    for cp in loads:
        cp.start()
    for cp in loads:
        cp.wait()


def stage_call(bufs):
    return pl.pallas_call(
        stage_kernel,
        out_shape=pltpu.VMEM((48, BP + 16, LR), bf16),
        in_specs=[spec(HB)] * 6,
        out_specs=spec(VM),
        scratch_shapes=[pltpu.SemaphoreType.DMA((6,))],
        name="stage",
        compiler_params=grant(54),
    )(*there(*bufs))


def absorb_kernel(q, keys, q_s):
    lane = lax.broadcasted_iota(jnp.int32, (B, 128), 1)
    for p in range(8):
        t0 = q[3 * p].astype(f32)
        r0 = q[3 * p + 1].astype(f32)
        t1 = pltpu.roll(r0, 64, 1)
        t2 = pltpu.roll(q[3 * p + 2].astype(f32), 64, 1)
        nopes = (t0, jnp.where(lane < ROT, t1, t2))
        ropes = (jnp.where(lane < ROT, r0, 0.0), jnp.where(lane < ROT, t2, 0.0))
        for j in range(2):
            h = 2 * p + j
            lat = lax.dot_general(
                nopes[j].astype(bf16),
                keys[:, 128 * h : 128 * h + 128],
                (((1,), (1,)), ((), ())),
                preferred_element_type=f32,
            )
            q_s[:, h, :LR] = (lat * SCALE).astype(bf16).astype(f32)
            q_s[:, h, LR:] = ropes[j]


def absorb_call(q, keys):
    return pl.pallas_call(
        absorb_kernel,
        out_shape=pltpu.VMEM((B, 16, LR + 128), f32),
        in_specs=[spec(VM)] * 2,
        out_specs=spec(VM),
        name="absorb",
        compiler_params=grant(54),
    )(*here(q, keys))


def attend_kernel(slots, q_s, wide, kv, late_a, late_b, out, kvb, s_s, p_s, mix_s, o_s, inv, tsem, sem):
    fetch = pltpu.make_async_copy(slots, inv, tsem)
    fetch.start()
    late = [pltpu.make_async_copy(ref, kvb.at[pl.ds(8 * i, 8)], sem.at[i]) for i, ref in enumerate((late_a, late_b))]
    for cp in late:
        cp.start()
    s, y, c = place_of()
    lane = lax.broadcasted_iota(jnp.int32, (B, BP), 1)

    def first_of(g, dc):
        cs = c if dc == 0 else 1 - c
        alpha = 3 - 2 * cs
        dy = jnp.where(g == 0, 0, jnp.where(g == 1, alpha, jnp.where(g == 2, 2, 4 - alpha)))
        return (lax.rem(y + dy, 4) * 2 + cs) * 8

    def scores(ref, base, g):
        for dc in range(2):
            first = first_of(g, dc)
            for k in range(8):
                at = base + dc * 8 + k
                e = inv[first + k]
                qb = q_s[e // 4].astype(bf16)
                keys = ref[at, :BP, :]
                rope = jnp.concatenate([ref[at, BP:, 128 * n : 128 * n + 128] for n in range(4)], axis=0)
                sc = lax.dot_general(qb[:, :LR], keys, (((1,), (1,)), ((), ())), preferred_element_type=f32)
                s_s[e] = sc + jnp.dot(qb[:, LR : LR + ROT], rope, preferred_element_type=f32)

    def mixing(ref, base, g):
        for dc in range(2):
            first = first_of(g, dc)
            for k in range(8):
                e = inv[first + k]
                b = e // 4
                got = jnp.dot(p_s[e], ref[base + dc * 8 + k, :BP, :], preferred_element_type=f32)
                mix_s[b] = mix_s[b] + got

    def groups(step):
        def early(g, _):
            step(kv, 16 * g, g)
            return 0

        lax.fori_loop(0, 3, early, 0)

    fetch.wait()
    groups(scores)
    for cp in late:
        cp.wait()
    scores(kvb, 0, jnp.int32(3))

    def softmax(bh, r):
        b = bh * 8 + r
        room = inv[64 + b]
        new = jnp.sum(q_s[b] * wide[pl.ds(b, 1), :], axis=1, keepdims=True)
        mine = jnp.full((B, 1), s, jnp.int32) == 0
        live = [lane < room - j * BP for j in range(4)]
        sc = [jnp.where(live[j], s_s[b * 4 + j], FLOOR) for j in range(4)]
        m = jnp.maximum(jnp.maximum(sc[0], sc[1]), jnp.maximum(sc[2], sc[3]))
        m = jnp.maximum(jnp.max(m, axis=1, keepdims=True), jnp.where(mine, new, FLOOR))
        p = [jnp.where(live[j], jnp.exp(sc[j] - m), 0.0) for j in range(4)]
        new = jnp.where(mine, jnp.exp(new - m), 0.0)
        l = jnp.sum((p[0] + p[1]) + (p[2] + p[3]), axis=1, keepdims=True) + new
        m1 = m.astype(bf16).astype(f32)
        m2 = (m - m1).astype(bf16).astype(f32)
        m3 = m - m1 - m2
        l1 = l.astype(bf16).astype(f32)
        l2 = (l - l1).astype(bf16).astype(f32)
        l3 = l - l1 - l2
        stats = jnp.zeros((B, 128), f32)
        for n, v in enumerate((m1, m2, m3, l1, l2, l3)):
            stats = jnp.where(lane == n, v, stats)
        o_s[pl.ds(bh * 16, 16), r, LR:] = stats
        mix_s[b] = new.astype(bf16).astype(f32) * wide[pl.ds(b, 1), :LR]
        for j in range(4):
            p_s[b * 4 + j] = p[j].astype(bf16)

    def spread(bh, r):
        o_s[pl.ds(bh * 16, 16), r, :LR] = mix_s[bh * 8 + r]

    def halves(step):
        def both(bh, _):
            for r in range(8):
                step(bh, r)
            return 0

        lax.fori_loop(0, 2, both, 0)

    halves(softmax)
    groups(mixing)
    mixing(kvb, 0, jnp.int32(3))
    halves(spread)

    def pour(i, _):
        out[i] = o_s[i].astype(bf16)
        return 0

    lax.fori_loop(0, 32, pour, 0, unroll=8)


def attend_call(slots, q, wide, kv, late):
    return pl.pallas_call(
        attend_kernel,
        out_shape=pltpu.VMEM((32, 8, LR + 128), bf16),
        in_specs=[spec(HB)] + [spec(VM)] * 3 + [spec(HB)] * 2,
        out_specs=spec(VM),
        scratch_shapes=[
            pltpu.VMEM((16, BP + 16, LR), bf16),
            pltpu.VMEM((64, B, BP), f32),
            pltpu.VMEM((64, B, BP), bf16),
            pltpu.VMEM((B, B, LR), f32),
            pltpu.VMEM((32, 8, LR + 128), f32),
            pltpu.SMEM((128,), jnp.int32),
            pltpu.SemaphoreType.DMA,
            pltpu.SemaphoreType.DMA((2,)),
        ],
        name="attend",
        compiler_params=grant(54),
    )(*there(slots), *here(q, wide, kv), *there(*late))


def value_kernel(parts, value_up, out, vals, sem):
    h = lax.rem(place_of()[0], 16)
    cp = pltpu.make_async_copy(value_up.at[:, pl.ds(pl.multiple_of(h * VD, VD), VD)], vals, sem)
    cp.start()
    tops, tots = [], []
    for i in range(32):
        st = parts[i, :, LR:].astype(f32)
        tops.append(st[:, 0:1] + st[:, 1:2] + st[:, 2:3])
        tots.append(st[:, 3:4] + st[:, 4:5] + st[:, 5:6])
    top = functools.reduce(jnp.maximum, tops)
    total = jnp.zeros((8, 1), f32)
    mix = jnp.zeros((8, LR), f32)
    for i in range(32):
        w = jnp.exp(tops[i] - top)
        total = total + w * tots[i]
        mix = mix + w * parts[i, :, :LR].astype(f32)
    att = (mix / total).astype(bf16)
    cp.wait()
    res = jnp.dot(att, vals[...], preferred_element_type=f32).astype(bf16)
    for i in range(32):
        out[i] = res


def value_call(parts, value_up):
    return pl.pallas_call(
        value_kernel,
        out_shape=pltpu.VMEM((32, 8, VD), bf16),
        in_specs=[spec(VM), spec(HB)],
        out_specs=spec(VM),
        scratch_shapes=[pltpu.VMEM((LR, VD), bf16), pltpu.SemaphoreType.DMA],
        name="value",
    )(*here(parts), value_up)


ALPHA = [(2 * y + c, 2 * ((y + 1 - 2 * c) % 4) + c) for y in range(4) for c in range(2)]
BETA = [(b, a) for a, b in ALPHA]
SWAP = [(0, 1), (1, 0)]


def body(hidden_in, united_down, q_gain, kv_gain, q_up, key_up, value_up, store, rope_pool, lengths, table):
    lane = jnp.arange(128)
    freq = 10000.0 ** (-2.0 * (lane % 32).astype(f32) / ROT)
    angles = lengths.astype(f32)[:, None] * freq
    cos, sin = jnp.cos(angles), jnp.sin(angles)
    mine = pack_call(store, rope_pool)
    alpha = lax.ppermute(mine, T, ALPHA)
    far = lax.ppermute(alpha, T, ALPHA)
    beta = lax.ppermute(mine, T, BETA)
    q_tile = exchange(tiles_call(q_up), S)
    cols = united_call(hidden_in, united_down)
    pair = jnp.stack([cols, lax.ppermute(cols, "c", SWAP)])
    near = lax.ppermute(pair, T, BETA)
    parts = [pair, near, lax.ppermute(near, "c", SWAP), lax.ppermute(near, T, BETA)]
    bufs = []
    for value in (mine, alpha, far, beta):
        bufs += [value, lax.ppermute(value, "c", SWAP)]
    entry, wide, q_copies = query_call(parts, q_gain, kv_gain, cos, sin, q_tile)
    q_all = exchange(q_copies, S)
    q_packs = absorb_call(q_all, keys_call(key_up))
    mixed = attend_call(slots_call(table, lengths), q_packs, wide, stage_call(bufs[:6]), bufs[6:])
    spans = exchange(mixed, S)
    res = value_call(spans, value_up)
    res = exchange(res, S)
    res = res.reshape(2, 16, 8, VD).transpose(0, 2, 1, 3).reshape(B, 16 * VD)
    return res, entry


def solution(mesh):
    split = Mesh(mesh.devices.reshape(8, 4, 4, 2), ("z", "x", "y", "c"))
    return jax.shard_map(
        body,
        mesh=split,
        in_specs=(
            P(),
            P(None, T),
            P(),
            P(),
            P(S, T),
            P(None, T),
            P(None, T),
            P(S + T, None, None),
            P(S + T, None, None),
            P(),
            P(None, S),
        ),
        out_specs=(P(None, T), P()),
        check_vma=False,
    )
```

```python
import functools

import jax
import jax.numpy as jnp
from jax import lax
from jax.experimental import pallas as pl
from jax.experimental.pallas import tpu as pltpu
from jax.sharding import Mesh
from jax.sharding import PartitionSpec as P


D = 5120
QR = 1536
LR = 512
ROT = 64
VD = 128
B = 16
BP = 128
QH = 192
SCALE = QH ** (-0.5)
FLOOR = -1e30
S = ("z", "x")
T = ("y", "c")
bf16 = jnp.bfloat16
f32 = jnp.float32
VM = pltpu.MemorySpace.VMEM
SM = pltpu.MemorySpace.SMEM
HB = pltpu.MemorySpace.HBM


def spec(space):
    return pl.BlockSpec(memory_space=space)


def here(*values):
    return tuple(pltpu.with_memory_space_constraint(v, VM) for v in values)


def there(*values):
    return tuple(pltpu.with_memory_space_constraint(v, HB) for v in values)


def exchange(pieces, axes):
    return lax.all_to_all(pieces, axes, split_axis=0, concat_axis=0, tiled=True)


UK = 5


def united_kernel(hid_hbm, wt, out, hid, wbuf, hsem, wsem):
    step = D // UK
    copies = []
    fetch = pltpu.make_async_copy(hid_hbm, hid, hsem)
    fetch.start()
    for k in range(UK):
        cp = pltpu.make_async_copy(wt.at[:, pl.ds(k * step, step)], wbuf.at[k], wsem.at[k])
        cp.start()
        copies.append(cp)
    acc = jnp.zeros(out.shape, f32)
    fetch.wait()
    for k in range(UK):
        copies[k].wait()
        acc = acc + lax.dot_general(
            hid[:, k * step : (k + 1) * step],
            wbuf[k],
            (((1,), (1,)), ((), ())),
            preferred_element_type=f32,
        )
    out[...] = acc.astype(bf16)


def united_call(hid, down):
    cols = down.shape[1]
    return pl.pallas_call(
        united_kernel,
        out_shape=pltpu.VMEM((B, cols), bf16),
        in_specs=[spec(HB), spec(HB)],
        out_specs=spec(VM),
        scratch_shapes=[
            pltpu.VMEM((B, D), bf16),
            pltpu.VMEM((UK, cols, D // UK), bf16),
            pltpu.SemaphoreType.DMA,
            pltpu.SemaphoreType.DMA((UK,)),
        ],
        name="united",
    )(hid, down.T)


def tiles_kernel(q_up, out):
    for k in range(32):
        j = k % 24
        out[k] = q_up[:, 128 * j : 128 * j + 128]


def tiles_call(q_up):
    return pl.pallas_call(
        tiles_kernel,
        out_shape=pltpu.VMEM((32, 48, 128), bf16),
        in_specs=[spec(VM)],
        out_specs=spec(VM),
        name="tiles",
    )(*here(q_up))


def pack_kernel(lat, rope, out, ropes, sem):
    fetch_rope = pltpu.make_async_copy(rope, ropes, sem.at[0])
    fetch_rope.start()
    fetch = pltpu.make_async_copy(lat, out.at[:, pl.ds(0, BP), :], sem.at[1])
    fetch.start()
    fetch_rope.wait()
    for n in range(8):
        for g in range(4):
            out[n, BP:, 128 * g : 128 * g + 128] = ropes[n, 16 * g : 16 * g + 16, :]
    fetch.wait()


def pack_call(lat, rope):
    return pl.pallas_call(
        pack_kernel,
        out_shape=pltpu.VMEM((8, BP + 16, LR), bf16),
        in_specs=[spec(HB)] * 2,
        out_specs=spec(VM),
        scratch_shapes=[pltpu.VMEM((8, ROT, BP), bf16), pltpu.SemaphoreType.DMA((2,))],
        name="pack",
    )(lat, rope)


def place_of():
    return lax.axis_index("z") * 4 + lax.axis_index("x"), lax.axis_index("y"), lax.axis_index("c")


def swapped(x):
    lane = lax.broadcasted_iota(jnp.int32, x.shape, 1)
    return jnp.where(lane % ROT < ROT // 2, pltpu.roll(x, 96, 1), pltpu.roll(x, 32, 1))


def query_kernel(*refs):
    pairs, (q_gain, kv_gain, cos, sin_part, weights, entry, wide, out, parts) = refs[:4], refs[4:]
    s, y, c = place_of()
    width = 264
    step = 1 - 2 * c
    for ref, dy, core in zip(pairs, (0, step, -step, 2), (c, c, 1 - c, c)):
        at = lax.rem(y + dy + 4, 4) * 2
        parts[at + core] = ref[0].astype(f32)
        parts[at + 1 - core] = ref[1].astype(f32)
    tiles = [None] * 17
    for i in range(8):
        piece = parts[i]
        piece = jnp.concatenate([piece, jnp.zeros((B, 384 - width), f32)], axis=1)
        if i:
            piece = pltpu.roll(piece, 8 * i, 1)
        for k in range(3):
            part = piece[:, 128 * k : 128 * k + 128]
            if 2 * i + k < 17:
                tiles[2 * i + k] = part if tiles[2 * i + k] is None else tiles[2 * i + k] + part
    u = jnp.concatenate(tiles, axis=1)
    uq = u[:, :QR]
    ul = u[:, QR : QR + LR]
    ur = u[:, QR + LR : QR + LR + 128]
    rq = lax.rsqrt(jnp.sum(uq * uq, axis=1, keepdims=True) / QR + 1.0)
    rl = lax.rsqrt(jnp.sum(ul * ul, axis=1, keepdims=True) / LR + 1.0)
    ql = (uq * rq * q_gain[...].reshape(1, QR)).astype(bf16)
    q = jnp.dot(ql, weights[...].reshape(QR, 128), preferred_element_type=f32)
    lane = lax.broadcasted_iota(jnp.int32, (B, 128), 1)
    sin = jnp.where(lane % ROT < ROT // 2, -sin_part[...], sin_part[...])
    kind = lax.rem(s, 3)
    in_rope = ((lane < ROT) & (kind == 1)) | ((lane >= ROT) & (kind == 2))
    res = jnp.where(in_rope, (q * cos[...] + swapped(q) * sin) * SCALE, q).astype(bf16)
    for i in range(32):
        out[i] = res
    lat = (ul * rl * kv_gain[...].reshape(1, LR)).astype(bf16)
    rot = jnp.where(lane < ROT, ur * cos[...] + swapped(ur) * sin, 0.0).astype(bf16)
    entry[:, :LR] = lat
    entry[:, LR:] = rot[:, :ROT]
    wide[:, :LR] = lat.astype(f32)
    wide[:, LR:] = rot.astype(f32)


def query_call(parts, q_gain, kv_gain, cos, sin, weights):
    return pl.pallas_call(
        query_kernel,
        out_shape=(
            jax.ShapeDtypeStruct((B, LR + ROT), bf16),
            pltpu.VMEM((B, LR + 128), f32),
            pltpu.VMEM((32, B, 128), bf16),
        ),
        in_specs=[spec(VM)] * 9,
        out_specs=(spec(VM),) * 3,
        scratch_shapes=[pltpu.VMEM((8, B, 264), f32)],
        name="query",
    )(*here(*parts, q_gain, kv_gain, cos, sin, weights))


def slots_kernel(table, lengths, slots):
    s = place_of()[0]

    def fill(b, _):
        slots[64 + b] = lengths[b] - s * (4 * BP)
        for j in range(4):
            slots[table[j, b] - s * 64] = b * 4 + j
        return 0

    lax.fori_loop(0, B, fill, 0, unroll=4)
    for i in range(80, 128):
        slots[i] = 0


def slots_call(table, lengths):
    return pl.pallas_call(
        slots_kernel,
        out_shape=jax.ShapeDtypeStruct((128,), jnp.int32),
        in_specs=[spec(SM), spec(SM)],
        out_specs=spec(SM),
        name="slots",
    )(table.T, lengths)


def keys_kernel(src, dst, sem):
    cp = pltpu.make_async_copy(src, dst, sem)
    cp.start()
    cp.wait()


def keys_call(key_up):
    return pl.pallas_call(
        keys_kernel,
        out_shape=pltpu.VMEM(key_up.shape, bf16),
        in_specs=[spec(HB)],
        out_specs=spec(VM),
        scratch_shapes=[pltpu.SemaphoreType.DMA],
        name="keys",
    )(*there(key_up))


def absorb_kernel(q, keys, q_s):
    lane = lax.broadcasted_iota(jnp.int32, (B, 128), 1)
    for p in range(8):
        t0 = q[3 * p].astype(f32)
        r0 = q[3 * p + 1].astype(f32)
        t1 = pltpu.roll(r0, 64, 1)
        t2 = pltpu.roll(q[3 * p + 2].astype(f32), 64, 1)
        nopes = (t0, jnp.where(lane < ROT, t1, t2))
        ropes = (jnp.where(lane < ROT, r0, 0.0), jnp.where(lane < ROT, t2, 0.0))
        for j in range(2):
            h = 2 * p + j
            lat = lax.dot_general(
                nopes[j].astype(bf16),
                keys[:, 128 * h : 128 * h + 128],
                (((1,), (1,)), ((), ())),
                preferred_element_type=f32,
            )
            q_s[:, h, :LR] = (lat * SCALE).astype(bf16).astype(f32)
            q_s[:, h, LR:] = ropes[j]


def absorb_call(q, keys):
    return pl.pallas_call(
        absorb_kernel,
        out_shape=pltpu.VMEM((B, 16, LR + 128), f32),
        in_specs=[spec(VM)] * 2,
        out_specs=spec(VM),
        name="absorb",
    )(*here(q, keys))


def attend_kernel(slots, q_s, wide, *rest):
    bufs, out = rest[:8], rest[8]
    kv, s_s, p_s, o_s, own_s, place, inv, tsem, sem = rest[9:]
    fetch = pltpu.make_async_copy(slots, inv, tsem)
    fetch.start()
    s, y, c = place_of()
    for i in range(8):
        pltpu.make_async_copy(bufs[i], kv.at[pl.ds(8 * i, 8)], sem.at[i // 2]).start()

    lane = lax.broadcasted_iota(jnp.int32, (B, BP), 1)
    fetch.wait()

    def scores(g, _):
        here = kv.at[pl.ds(16 * g, 16)]
        pltpu.make_async_copy(here, here, sem.at[g]).wait()
        for dc in range(2):
            cs = c if dc == 0 else 1 - c
            alpha = 3 - 2 * cs
            dy = jnp.where(g == 0, 0, jnp.where(g == 1, alpha, jnp.where(g == 2, 2, 4 - alpha)))
            first = (lax.rem(y + dy, 4) * 2 + cs) * 8
            for k in range(8):
                at = g * 16 + dc * 8 + k
                e = inv[first + k]
                place[e] = at
                qb = q_s[e // 4].astype(bf16)
                keys = kv[at, :BP, :]
                rope = jnp.concatenate([kv[at, BP:, 128 * n : 128 * n + 128] for n in range(4)], axis=0)
                sc = lax.dot_general(qb[:, :LR], keys, (((1,), (1,)), ((), ())), preferred_element_type=f32)
                s_s[e] = sc + jnp.dot(qb[:, LR : LR + ROT], rope, preferred_element_type=f32)
        return 0

    lax.fori_loop(0, 4, scores, 0)

    def softmax(bh, r):
        b = bh * 8 + r
        room = inv[64 + b]
        new = jnp.sum(q_s[b] * wide[pl.ds(b, 1), :], axis=1, keepdims=True)
        mine = jnp.full((B, 1), s, jnp.int32) == 0
        live = [lane < room - j * BP for j in range(4)]
        sc = [jnp.where(live[j], s_s[b * 4 + j], FLOOR) for j in range(4)]
        m = jnp.maximum(jnp.maximum(sc[0], sc[1]), jnp.maximum(sc[2], sc[3]))
        m = jnp.maximum(jnp.max(m, axis=1, keepdims=True), jnp.where(mine, new, FLOOR))
        p = [jnp.where(live[j], jnp.exp(sc[j] - m), 0.0) for j in range(4)]
        new = jnp.where(mine, jnp.exp(new - m), 0.0)
        l = jnp.sum((p[0] + p[1]) + (p[2] + p[3]), axis=1, keepdims=True) + new
        m1 = m.astype(bf16).astype(f32)
        m2 = (m - m1).astype(bf16).astype(f32)
        m3 = m - m1 - m2
        l1 = l.astype(bf16).astype(f32)
        l2 = (l - l1).astype(bf16).astype(f32)
        l3 = l - l1 - l2
        stats = jnp.zeros((B, 128), f32)
        for n, v in enumerate((m1, m2, m3, l1, l2, l3)):
            stats = jnp.where(lane == n, v, stats)
        o_s[pl.ds(bh * 16, 16), r, LR:] = stats
        own_s[b] = new.astype(bf16).astype(f32) * wide[pl.ds(b, 1), :LR]
        p_s[b] = jnp.concatenate(p, axis=1).astype(bf16)

    def mixing(bh, r):
        b = bh * 8 + r
        p = p_s[b]
        mix = own_s[b]
        for j in range(4):
            keys = kv[place[b * 4 + j], :BP, :]
            mix = mix + jnp.dot(p[:, 128 * j : 128 * j + 128], keys, preferred_element_type=f32)
        o_s[pl.ds(bh * 16, 16), r, :LR] = mix

    def halves(step):
        def both(bh, _):
            for r in range(8):
                step(bh, r)
            return 0

        lax.fori_loop(0, 2, both, 0)

    halves(softmax)
    halves(mixing)

    def pour(i, _):
        out[i] = o_s[i].astype(bf16)
        return 0

    lax.fori_loop(0, 32, pour, 0, unroll=8)


def attend_call(slots, q, wide, bufs):
    return pl.pallas_call(
        attend_kernel,
        out_shape=pltpu.VMEM((32, 8, LR + 128), bf16),
        in_specs=[spec(HB)] + [spec(VM)] * 2 + [spec(HB)] * 8,
        out_specs=spec(VM),
        scratch_shapes=[
            pltpu.VMEM((64, BP + 16, LR), bf16),
            pltpu.VMEM((64, B, BP), f32),
            pltpu.VMEM((B, B, 4 * BP), bf16),
            pltpu.VMEM((32, 8, LR + 128), f32),
            pltpu.VMEM((B, B, LR), f32),
            pltpu.SMEM((64,), jnp.int32),
            pltpu.SMEM((128,), jnp.int32),
            pltpu.SemaphoreType.DMA,
            pltpu.SemaphoreType.DMA((4,)),
        ],
        name="attend",
    )(*there(slots), *here(q, wide), *there(*bufs))


def value_kernel(parts, value_up, out, vals, sem):
    h = lax.rem(place_of()[0], 16)
    cp = pltpu.make_async_copy(value_up.at[:, pl.ds(pl.multiple_of(h * VD, VD), VD)], vals, sem)
    cp.start()
    tops, tots = [], []
    for i in range(32):
        st = parts[i, :, LR:].astype(f32)
        tops.append(st[:, 0:1] + st[:, 1:2] + st[:, 2:3])
        tots.append(st[:, 3:4] + st[:, 4:5] + st[:, 5:6])
    top = functools.reduce(jnp.maximum, tops)
    total = jnp.zeros((8, 1), f32)
    mix = jnp.zeros((8, LR), f32)
    for i in range(32):
        w = jnp.exp(tops[i] - top)
        total = total + w * tots[i]
        mix = mix + w * parts[i, :, :LR].astype(f32)
    att = (mix / total).astype(bf16)
    cp.wait()
    res = jnp.dot(att, vals[...], preferred_element_type=f32).astype(bf16)
    for i in range(32):
        out[i] = res


def value_call(parts, value_up):
    return pl.pallas_call(
        value_kernel,
        out_shape=pltpu.VMEM((32, 8, VD), bf16),
        in_specs=[spec(VM), spec(HB)],
        out_specs=spec(VM),
        scratch_shapes=[pltpu.VMEM((LR, VD), bf16), pltpu.SemaphoreType.DMA],
        name="value",
    )(*here(parts), value_up)


ALPHA = [(2 * y + c, 2 * ((y + 1 - 2 * c) % 4) + c) for y in range(4) for c in range(2)]
BETA = [(b, a) for a, b in ALPHA]
SWAP = [(0, 1), (1, 0)]


def body(hidden_in, united_down, q_gain, kv_gain, q_up, key_up, value_up, store, rope_pool, lengths, table):
    lane = jnp.arange(128)
    freq = 10000.0 ** (-2.0 * (lane % 32).astype(f32) / ROT)
    angles = lengths.astype(f32)[:, None] * freq
    cos, sin = jnp.cos(angles), jnp.sin(angles)
    mine = pack_call(store, rope_pool)
    alpha = lax.ppermute(mine, T, ALPHA)
    far = lax.ppermute(alpha, T, ALPHA)
    beta = lax.ppermute(mine, T, BETA)
    q_tile = exchange(tiles_call(q_up), S)
    cols = united_call(hidden_in, united_down)
    pair = jnp.stack([cols, lax.ppermute(cols, "c", SWAP)])
    near = lax.ppermute(pair, T, BETA)
    parts = [pair, near, lax.ppermute(near, "c", SWAP), lax.ppermute(near, T, BETA)]
    bufs = []
    for value in (mine, alpha, far, beta):
        bufs += [value, lax.ppermute(value, "c", SWAP)]
    entry, wide, q_copies = query_call(parts, q_gain, kv_gain, cos, sin, q_tile)
    q_all = exchange(q_copies, S)
    q_packs = absorb_call(q_all, keys_call(key_up))
    mixed = attend_call(slots_call(table, lengths), q_packs, wide, bufs)
    spans = exchange(mixed, S)
    res = value_call(spans, value_up)
    res = exchange(res, S)
    res = res.reshape(2, 16, 8, VD).transpose(0, 2, 1, 3).reshape(B, 16 * VD)
    return res, entry


def solution(mesh):
    split = Mesh(mesh.devices.reshape(8, 4, 4, 2), ("z", "x", "y", "c"))
    return jax.shard_map(
        body,
        mesh=split,
        in_specs=(
            P(),
            P(None, T),
            P(),
            P(),
            P(S, T),
            P(None, T),
            P(None, T),
            P(S + T, None, None),
            P(S + T, None, None),
            P(),
            P(None, S),
        ),
        out_specs=(P(None, T), P()),
        check_vma=False,
    )
```

```python
import functools

import jax
import jax.numpy as jnp
from jax import lax
from jax.experimental import pallas as pl
from jax.experimental.pallas import tpu as pltpu
from jax.sharding import Mesh
from jax.sharding import PartitionSpec as P


D = 5120
QR = 1536
LR = 512
ROT = 64
VD = 128
B = 16
BP = 128
QH = 192
SCALE = QH ** (-0.5)
FLOOR = -1e30
S = ("z", "x")
T = ("y", "c")
bf16 = jnp.bfloat16
f32 = jnp.float32
VM = pltpu.MemorySpace.VMEM
SM = pltpu.MemorySpace.SMEM
HB = pltpu.MemorySpace.HBM


def grant(mib):
    return pltpu.CompilerParams(vmem_limit_bytes=mib << 20)


def spec(space):
    return pl.BlockSpec(memory_space=space)


def here(*values):
    return tuple(pltpu.with_memory_space_constraint(v, VM) for v in values)


def there(*values):
    return tuple(pltpu.with_memory_space_constraint(v, HB) for v in values)


def exchange(pieces, axes):
    return lax.all_to_all(pieces, axes, split_axis=0, concat_axis=0, tiled=True)


UK = 5


def united_kernel(hid_hbm, wt, out, hid, wbuf, hsem, wsem):
    step = D // UK
    copies = []
    fetch = pltpu.make_async_copy(hid_hbm, hid, hsem)
    fetch.start()
    for k in range(UK):
        cp = pltpu.make_async_copy(wt.at[:, pl.ds(k * step, step)], wbuf.at[k], wsem.at[k])
        cp.start()
        copies.append(cp)
    acc = jnp.zeros(out.shape, f32)
    fetch.wait()
    for k in range(UK):
        copies[k].wait()
        acc = acc + lax.dot_general(
            hid[:, k * step : (k + 1) * step],
            wbuf[k],
            (((1,), (1,)), ((), ())),
            preferred_element_type=f32,
        )
    out[...] = acc.astype(bf16)


def united_call(hid, down):
    cols = down.shape[1]
    return pl.pallas_call(
        united_kernel,
        out_shape=pltpu.VMEM((B, cols), bf16),
        in_specs=[spec(HB), spec(HB)],
        out_specs=spec(VM),
        scratch_shapes=[
            pltpu.VMEM((B, D), bf16),
            pltpu.VMEM((UK, cols, D // UK), bf16),
            pltpu.SemaphoreType.DMA,
            pltpu.SemaphoreType.DMA((UK,)),
        ],
        name="united",
    )(hid, down.T)


def tiles_kernel(q_up, out):
    for k in range(32):
        j = k % 24
        out[k] = q_up[:, 128 * j : 128 * j + 128]


def tiles_call(q_up):
    return pl.pallas_call(
        tiles_kernel,
        out_shape=pltpu.VMEM((32, 48, 128), bf16),
        in_specs=[spec(VM)],
        out_specs=spec(VM),
        name="tiles",
    )(*here(q_up))


def pack_kernel(lat, rope, out, ropes, sem):
    fetch_rope = pltpu.make_async_copy(rope, ropes, sem.at[0])
    fetch_rope.start()
    fetch = pltpu.make_async_copy(lat, out.at[:, pl.ds(0, BP), :], sem.at[1])
    fetch.start()
    fetch_rope.wait()
    for n in range(8):
        for g in range(4):
            out[n, BP:, 128 * g : 128 * g + 128] = ropes[n, 16 * g : 16 * g + 16, :]
    fetch.wait()


def pack_call(lat, rope):
    return pl.pallas_call(
        pack_kernel,
        out_shape=pltpu.VMEM((8, BP + 16, LR), bf16),
        in_specs=[spec(HB)] * 2,
        out_specs=spec(VM),
        scratch_shapes=[pltpu.VMEM((8, ROT, BP), bf16), pltpu.SemaphoreType.DMA((2,))],
        name="pack",
    )(lat, rope)


def place_of():
    return lax.axis_index("z") * 4 + lax.axis_index("x"), lax.axis_index("y"), lax.axis_index("c")


def swapped(x):
    lane = lax.broadcasted_iota(jnp.int32, x.shape, 1)
    return jnp.where(lane % ROT < ROT // 2, pltpu.roll(x, 96, 1), pltpu.roll(x, 32, 1))


def query_kernel(*refs):
    pairs, (q_gain, kv_gain, cos, sin_part, weights, entry, wide, out, parts) = refs[:4], refs[4:]
    s, y, c = place_of()
    width = 264
    step = 1 - 2 * c
    for ref, dy, core in zip(pairs, (0, step, -step, 2), (c, c, 1 - c, c)):
        at = lax.rem(y + dy + 4, 4) * 2
        parts[at + core] = ref[0].astype(f32)
        parts[at + 1 - core] = ref[1].astype(f32)
    tiles = [None] * 17
    for i in range(8):
        piece = parts[i]
        piece = jnp.concatenate([piece, jnp.zeros((B, 384 - width), f32)], axis=1)
        if i:
            piece = pltpu.roll(piece, 8 * i, 1)
        for k in range(3):
            part = piece[:, 128 * k : 128 * k + 128]
            if 2 * i + k < 17:
                tiles[2 * i + k] = part if tiles[2 * i + k] is None else tiles[2 * i + k] + part
    u = jnp.concatenate(tiles, axis=1)
    uq = u[:, :QR]
    ul = u[:, QR : QR + LR]
    ur = u[:, QR + LR : QR + LR + 128]
    rq = lax.rsqrt(jnp.sum(uq * uq, axis=1, keepdims=True) / QR + 1.0)
    rl = lax.rsqrt(jnp.sum(ul * ul, axis=1, keepdims=True) / LR + 1.0)
    ql = (uq * rq * q_gain[...].reshape(1, QR)).astype(bf16)
    q = jnp.dot(ql, weights[...].reshape(QR, 128), preferred_element_type=f32)
    lane = lax.broadcasted_iota(jnp.int32, (B, 128), 1)
    sin = jnp.where(lane % ROT < ROT // 2, -sin_part[...], sin_part[...])
    kind = lax.rem(s, 3)
    in_rope = ((lane < ROT) & (kind == 1)) | ((lane >= ROT) & (kind == 2))
    res = jnp.where(in_rope, (q * cos[...] + swapped(q) * sin) * SCALE, q).astype(bf16)
    for i in range(32):
        out[i] = res
    lat = (ul * rl * kv_gain[...].reshape(1, LR)).astype(bf16)
    rot = jnp.where(lane < ROT, ur * cos[...] + swapped(ur) * sin, 0.0).astype(bf16)
    entry[:, :LR] = lat
    entry[:, LR:] = rot[:, :ROT]
    wide[:, :LR] = lat.astype(f32)
    wide[:, LR:] = rot.astype(f32)


def query_call(parts, q_gain, kv_gain, cos, sin, weights):
    return pl.pallas_call(
        query_kernel,
        out_shape=(
            jax.ShapeDtypeStruct((B, LR + ROT), bf16),
            pltpu.VMEM((B, LR + 128), f32),
            pltpu.VMEM((32, B, 128), bf16),
        ),
        in_specs=[spec(VM)] * 9,
        out_specs=(spec(VM),) * 3,
        scratch_shapes=[pltpu.VMEM((8, B, 264), f32)],
        name="query",
    )(*here(*parts, q_gain, kv_gain, cos, sin, weights))


def slots_kernel(table, lengths, slots):
    s = place_of()[0]

    def fill(b, _):
        slots[64 + b] = lengths[b] - s * (4 * BP)
        for j in range(4):
            slots[table[j, b] - s * 64] = b * 4 + j
        return 0

    lax.fori_loop(0, B, fill, 0, unroll=4)
    for i in range(80, 128):
        slots[i] = 0


def slots_call(table, lengths):
    return pl.pallas_call(
        slots_kernel,
        out_shape=jax.ShapeDtypeStruct((128,), jnp.int32),
        in_specs=[spec(SM), spec(SM)],
        out_specs=spec(SM),
        name="slots",
    )(table.T, lengths)


def keys_kernel(src, dst, sem):
    cp = pltpu.make_async_copy(src, dst, sem)
    cp.start()
    cp.wait()


def keys_call(key_up):
    return pl.pallas_call(
        keys_kernel,
        out_shape=pltpu.VMEM(key_up.shape, bf16),
        in_specs=[spec(HB)],
        out_specs=spec(VM),
        scratch_shapes=[pltpu.SemaphoreType.DMA],
        name="keys",
        compiler_params=grant(58),
    )(*there(key_up))


def absorb_kernel(q, keys, q_s):
    lane = lax.broadcasted_iota(jnp.int32, (B, 128), 1)
    for p in range(8):
        t0 = q[3 * p].astype(f32)
        r0 = q[3 * p + 1].astype(f32)
        t1 = pltpu.roll(r0, 64, 1)
        t2 = pltpu.roll(q[3 * p + 2].astype(f32), 64, 1)
        nopes = (t0, jnp.where(lane < ROT, t1, t2))
        ropes = (jnp.where(lane < ROT, r0, 0.0), jnp.where(lane < ROT, t2, 0.0))
        for j in range(2):
            h = 2 * p + j
            lat = lax.dot_general(
                nopes[j].astype(bf16),
                keys[:, 128 * h : 128 * h + 128],
                (((1,), (1,)), ((), ())),
                preferred_element_type=f32,
            )
            q_s[:, h, :LR] = (lat * SCALE).astype(bf16).astype(f32)
            q_s[:, h, LR:] = ropes[j]


def absorb_call(q, keys):
    return pl.pallas_call(
        absorb_kernel,
        out_shape=pltpu.VMEM((B, 16, LR + 128), f32),
        in_specs=[spec(VM)] * 2,
        out_specs=spec(VM),
        name="absorb",
        compiler_params=grant(58),
    )(*here(q, keys))


def attend_kernel(slots, q_s, wide, *rest):
    bufs, out = rest[:8], rest[8]
    kv, s_s, p_s, o_s, own_s, place, inv, tsem, sem = rest[9:]
    fetch = pltpu.make_async_copy(slots, inv, tsem)
    fetch.start()
    s, y, c = place_of()
    for i in range(8):
        pltpu.make_async_copy(bufs[i], kv.at[pl.ds(8 * i, 8)], sem.at[i // 2]).start()

    lane = lax.broadcasted_iota(jnp.int32, (B, BP), 1)
    fetch.wait()

    def scores(g, _):
        here = kv.at[pl.ds(16 * g, 16)]
        pltpu.make_async_copy(here, here, sem.at[g]).wait()
        for dc in range(2):
            cs = c if dc == 0 else 1 - c
            alpha = 3 - 2 * cs
            dy = jnp.where(g == 0, 0, jnp.where(g == 1, alpha, jnp.where(g == 2, 2, 4 - alpha)))
            first = (lax.rem(y + dy, 4) * 2 + cs) * 8
            for k in range(8):
                at = g * 16 + dc * 8 + k
                e = inv[first + k]
                place[e] = at
                qb = q_s[e // 4].astype(bf16)
                keys = kv[at, :BP, :]
                rope = jnp.concatenate([kv[at, BP:, 128 * n : 128 * n + 128] for n in range(4)], axis=0)
                sc = lax.dot_general(qb[:, :LR], keys, (((1,), (1,)), ((), ())), preferred_element_type=f32)
                s_s[e] = sc + jnp.dot(qb[:, LR : LR + ROT], rope, preferred_element_type=f32)
        return 0

    lax.fori_loop(0, 4, scores, 0)

    def softmax(bh, r):
        b = bh * 8 + r
        room = inv[64 + b]
        new = jnp.sum(q_s[b] * wide[pl.ds(b, 1), :], axis=1, keepdims=True)
        mine = jnp.full((B, 1), s, jnp.int32) == 0
        live = [lane < room - j * BP for j in range(4)]
        sc = [jnp.where(live[j], s_s[b * 4 + j], FLOOR) for j in range(4)]
        m = jnp.maximum(jnp.maximum(sc[0], sc[1]), jnp.maximum(sc[2], sc[3]))
        m = jnp.maximum(jnp.max(m, axis=1, keepdims=True), jnp.where(mine, new, FLOOR))
        p = [jnp.where(live[j], jnp.exp(sc[j] - m), 0.0) for j in range(4)]
        new = jnp.where(mine, jnp.exp(new - m), 0.0)
        l = jnp.sum((p[0] + p[1]) + (p[2] + p[3]), axis=1, keepdims=True) + new
        m1 = m.astype(bf16).astype(f32)
        m2 = (m - m1).astype(bf16).astype(f32)
        m3 = m - m1 - m2
        l1 = l.astype(bf16).astype(f32)
        l2 = (l - l1).astype(bf16).astype(f32)
        l3 = l - l1 - l2
        stats = jnp.zeros((B, 128), f32)
        for n, v in enumerate((m1, m2, m3, l1, l2, l3)):
            stats = jnp.where(lane == n, v, stats)
        o_s[pl.ds(bh * 16, 16), r, LR:] = stats
        own_s[b] = new.astype(bf16).astype(f32) * wide[pl.ds(b, 1), :LR]
        p_s[b] = jnp.concatenate(p, axis=1).astype(bf16)

    def mixing(bh, r):
        b = bh * 8 + r
        p = p_s[b]
        mix = own_s[b]
        for j in range(4):
            keys = kv[place[b * 4 + j], :BP, :]
            mix = mix + jnp.dot(p[:, 128 * j : 128 * j + 128], keys, preferred_element_type=f32)
        o_s[pl.ds(bh * 16, 16), r, :LR] = mix

    def halves(step):
        def both(bh, _):
            for r in range(8):
                step(bh, r)
            return 0

        lax.fori_loop(0, 2, both, 0)

    halves(softmax)
    halves(mixing)

    def pour(i, _):
        out[i] = o_s[i].astype(bf16)
        return 0

    lax.fori_loop(0, 32, pour, 0, unroll=8)


def attend_call(slots, q, wide, bufs):
    return pl.pallas_call(
        attend_kernel,
        out_shape=pltpu.VMEM((32, 8, LR + 128), bf16),
        in_specs=[spec(HB)] + [spec(VM)] * 2 + [spec(HB)] * 8,
        out_specs=spec(VM),
        scratch_shapes=[
            pltpu.VMEM((64, BP + 16, LR), bf16),
            pltpu.VMEM((64, B, BP), f32),
            pltpu.VMEM((B, B, 4 * BP), bf16),
            pltpu.VMEM((32, 8, LR + 128), f32),
            pltpu.VMEM((B, B, LR), f32),
            pltpu.SMEM((64,), jnp.int32),
            pltpu.SMEM((128,), jnp.int32),
            pltpu.SemaphoreType.DMA,
            pltpu.SemaphoreType.DMA((4,)),
        ],
        name="attend",
        compiler_params=grant(58),
    )(*there(slots), *here(q, wide), *there(*bufs))


def value_kernel(parts, value_up, out, vals, sem):
    h = lax.rem(place_of()[0], 16)
    cp = pltpu.make_async_copy(value_up.at[:, pl.ds(pl.multiple_of(h * VD, VD), VD)], vals, sem)
    cp.start()
    tops, tots = [], []
    for i in range(32):
        st = parts[i, :, LR:].astype(f32)
        tops.append(st[:, 0:1] + st[:, 1:2] + st[:, 2:3])
        tots.append(st[:, 3:4] + st[:, 4:5] + st[:, 5:6])
    top = functools.reduce(jnp.maximum, tops)
    total = jnp.zeros((8, 1), f32)
    mix = jnp.zeros((8, LR), f32)
    for i in range(32):
        w = jnp.exp(tops[i] - top)
        total = total + w * tots[i]
        mix = mix + w * parts[i, :, :LR].astype(f32)
    att = (mix / total).astype(bf16)
    cp.wait()
    res = jnp.dot(att, vals[...], preferred_element_type=f32).astype(bf16)
    for i in range(32):
        out[i] = res


def value_call(parts, value_up):
    return pl.pallas_call(
        value_kernel,
        out_shape=pltpu.VMEM((32, 8, VD), bf16),
        in_specs=[spec(VM), spec(HB)],
        out_specs=spec(VM),
        scratch_shapes=[pltpu.VMEM((LR, VD), bf16), pltpu.SemaphoreType.DMA],
        name="value",
    )(*here(parts), value_up)


ALPHA = [(2 * y + c, 2 * ((y + 1 - 2 * c) % 4) + c) for y in range(4) for c in range(2)]
BETA = [(b, a) for a, b in ALPHA]
SWAP = [(0, 1), (1, 0)]


def body(hidden_in, united_down, q_gain, kv_gain, q_up, key_up, value_up, store, rope_pool, lengths, table):
    lane = jnp.arange(128)
    freq = 10000.0 ** (-2.0 * (lane % 32).astype(f32) / ROT)
    angles = lengths.astype(f32)[:, None] * freq
    cos, sin = jnp.cos(angles), jnp.sin(angles)
    mine = pack_call(store, rope_pool)
    alpha = lax.ppermute(mine, T, ALPHA)
    far = lax.ppermute(alpha, T, ALPHA)
    beta = lax.ppermute(mine, T, BETA)
    q_tile = exchange(tiles_call(q_up), S)
    cols = united_call(hidden_in, united_down)
    pair = jnp.stack([cols, lax.ppermute(cols, "c", SWAP)])
    near = lax.ppermute(pair, T, BETA)
    parts = [pair, near, lax.ppermute(near, "c", SWAP), lax.ppermute(near, T, BETA)]
    bufs = []
    for value in (mine, alpha, far, beta):
        bufs += [value, lax.ppermute(value, "c", SWAP)]
    entry, wide, q_copies = query_call(parts, q_gain, kv_gain, cos, sin, q_tile)
    q_all = exchange(q_copies, S)
    q_packs = absorb_call(q_all, keys_call(key_up))
    mixed = attend_call(slots_call(table, lengths), q_packs, wide, bufs)
    spans = exchange(mixed, S)
    res = value_call(spans, value_up)
    res = exchange(res, S)
    res = res.reshape(2, 16, 8, VD).transpose(0, 2, 1, 3).reshape(B, 16 * VD)
    return res, entry


def solution(mesh):
    split = Mesh(mesh.devices.reshape(8, 4, 4, 2), ("z", "x", "y", "c"))
    return jax.shard_map(
        body,
        mesh=split,
        in_specs=(
            P(),
            P(None, T),
            P(),
            P(),
            P(S, T),
            P(None, T),
            P(None, T),
            P(S + T, None, None),
            P(S + T, None, None),
            P(),
            P(None, S),
        ),
        out_specs=(P(None, T), P()),
        check_vma=False,
    )
```
